32 devices in a mesh: dp: 8 (over y, x, core), tensor: 4 (over z).
Axes of the slice: x: 2, y: 2, z: 4, core: 2. Of those that a mesh axis runs over, the one named last changes fastest.
Arguments:
- tokens: bfloat16 [16384, 1024], P(('dp', 'tensor')), may hold values from -6 to 6
- segment_ids: int32 [8, 2048], P('dp'), may hold values from 0 to 5, never falling along the last dimension, each value on 1 to 800 neighbouring positions
- keep_mask: int32 [8, 2048], P('dp'), may hold values from 0 to 1, as said below
- cotangent: bfloat16 [16384, 1024], P(('dp', 'tensor')), may hold values from -6 to 6
- w_query: bfloat16 [1024, 1024], P('dp', 'tensor'), may hold values from -0.25 to 0.25
- w_key: bfloat16 [1024, 1024], P('dp', 'tensor'), may hold values from -0.1875 to 0.1875
- w_value: bfloat16 [1024, 1024], P('dp', 'tensor'), may hold values from -0.1875 to 0.1875
- w_out: bfloat16 [1024, 1024], P('tensor', 'dp'), may hold values from -1 to 1
- w_in: bfloat16 [1024, 4096], P('dp', 'tensor'), may hold values from -0.1875 to 0.1875
- w_back: bfloat16 [4096, 1024], P('tensor', 'dp'), may hold values from -0.125 to 0.125
- bias_query: bfloat16 [16, 64], P('tensor', 'dp'), may hold values from -3 to 3
- bias_value: bfloat16 [16, 64], P('tensor', 'dp'), may hold values from -3 to 3
- bias_out: bfloat16 [1024], P('dp'), may hold values from -3 to 3
- bias_in: bfloat16 [64, 64], P('tensor', 'dp'), may hold values from -3 to 3
- bias_back: bfloat16 [1024], P('dp'), may hold values from -3 to 3
- gain_first: bfloat16 [1024], P('dp'), may hold values from 0.099609375 to 1.8984375
- shift_first: bfloat16 [1024], P('dp'), may hold values from -3 to 3
- gain_second: bfloat16 [1024], P('dp'), may hold values from 0.099609375 to 1.8984375
- shift_second: bfloat16 [1024], P('dp'), may hold values from -3 to 3
Outputs:
- output: bfloat16 [16384, 1024], P(('dp', 'tensor'))
- grad_tokens: bfloat16 [16384, 1024], P(('dp', 'tensor'))
- grad_w_query: float32 [1024, 1024], P('dp', 'tensor')
- grad_w_key: float32 [1024, 1024], P('dp', 'tensor')
- grad_w_value: float32 [1024, 1024], P('dp', 'tensor')
- grad_w_out: float32 [1024, 1024], P('tensor', 'dp')
- grad_w_in: float32 [1024, 4096], P('dp', 'tensor')
- grad_w_back: float32 [4096, 1024], P('tensor', 'dp')
- grad_bias_query: float32 [16, 64], P('tensor', 'dp')
- grad_bias_value: float32 [16, 64], P('tensor', 'dp')
- grad_bias_out: float32 [1024], P('dp')
- grad_bias_in: float32 [64, 64], P('tensor', 'dp')
- grad_bias_back: float32 [1024], P('dp')
- grad_gain_first: float32 [1024], P('dp')
- grad_shift_first: float32 [1024], P('dp')
- grad_gain_second: float32 [1024], P('dp')
- grad_shift_second: float32 [1024], P('dp')
The draws below stay inside these ranges and needn't reach their ends.
Inputs may be any that keep to these rules, and one draw needn't show every extreme that they name: `segment_ids`: in each sequence the numbers never fall; each of the 6 documents holds 1 to 800 tokens, and some document holds exactly 800. `keep_mask`: in each sequence the zeros are the last 0 to 256 positions; some sequence has exactly 256.
All inputs are finite; a program needn't handle non-finite values.
Results may differ from the reference program's by a relative error of at most 0.023.
Values may be sent and summed in bfloat16 or wider, within the bound.
A program may use at most 192 MiB of HBM per device.

```python
import math
import jax
import jax.numpy as jnp
import numpy as np
from jax import lax

D = 1024
HEADS = 16
HEAD = 64
FF = 4096
LEN = 2048
DOC_MOST = 800
DOC_COUNT = 6
PAD_MOST = 256
QBLOCK = 512
SEQS = 8
TOKENS = 16384


def draw_keep_mask(key, part):
    pad_counts = jax.random.randint(jax.random.fold_in(key, 11), (SEQS,), 0, PAD_MOST + 1)
    longest = jax.random.randint(jax.random.fold_in(key, 12), (), 0, SEQS)
    pad_counts = pad_counts.at[longest].set(PAD_MOST)
    position = jnp.arange(LEN)
    return (position[None, :] < (LEN - pad_counts)[:, None]).astype(jnp.int32)


def shard_levels(rng, dims, pieces, low, largest):
    factor_of = 1.0
    for axis_at, parts in pieces:
        draws = jax.random.uniform(jax.random.fold_in(jax.random.fold_in(rng, 6), axis_at), (parts,), jnp.float32, low / len(pieces), largest / len(pieces))
        factor_of = factor_of * jnp.repeat(jnp.exp(draws), dims[axis_at] // parts).reshape((-1,) + (1,) * (len(dims) - 1 - axis_at))
    return factor_of


def split_up(count, total, reach, slope):
    portions = [(1 << 20) // math.isqrt(grade ** slope) + 1 for grade in range(2, count + 1)]
    surplus, given = total - reach - (count - 1), [1] * (count - 1)
    while surplus > 0:
        movable = [i for i in range(count - 1) if given[i] < reach]
        pool, budget = sum([portions[i] for i in movable]), surplus
        for i in movable:
            extra = min(reach - given[i], max(1, budget * portions[i] // pool), surplus)
            given[i] = given[i] + extra
            surplus = surplus - extra
    return np.array([reach] + given)


def ragged(stream_key, amount, total, most, lean):
    if amount == 2:
        one = jax.random.randint(stream_key, (), max(1, total - most), min(most, total - 1) + 1)
        return jnp.stack([one, total - one])
    sizes = jnp.asarray(split_up(amount, total, most, lean), jnp.int32)
    twos = (amount - 1) // 2
    giver, receiver = sizes[1:1 + 2 * twos:2], sizes[2:2 + 2 * twos:2]
    margin = jnp.minimum(giver - 1, most - receiver)
    passed = jax.random.randint(jax.random.fold_in(stream_key, 1), (twos,), 0, 1 << 20) % (margin + 1)
    sizes = sizes.at[1:1 + 2 * twos:2].set(giver - passed).at[2:2 + 2 * twos:2].set(receiver + passed)
    return sizes[jax.random.permutation(jax.random.fold_in(stream_key, 2), amount)]


def normal_values(stream_key, dims, scale, bound, pieces=(), kind=jnp.bfloat16):
    result = jax.random.normal(stream_key, dims, jnp.float32) * scale
    if len(pieces) > 0:
        result = shard_levels(stream_key, dims, pieces, -0.22, 0.18) * result
    return jnp.clip(result, min=-bound, max=bound).astype(kind)


def setup_inputs(seed: int = 0) -> dict:
    key_of = jax.random.split(jax.random.key(seed), 20)
    return {
        "tokens": normal_values(key_of[0], (TOKENS, D), 1.0, 6.0, ((0, 32),)),
        "segment_ids": jax.vmap(lambda own: jnp.searchsorted(jnp.cumsum(ragged(own, DOC_COUNT, LEN, DOC_MOST, 2)), jnp.arange(LEN), side="right"))(jax.random.split(key_of[1], SEQS)).reshape((SEQS, LEN)).astype(jnp.int32),
        "keep_mask": draw_keep_mask(jax.random.fold_in(key_of[19], 71), 0),
        "cotangent": normal_values(key_of[3], (TOKENS, D), 1.0, 6.0, ((0, 32),)),
        "w_query": normal_values(key_of[4], (D, D), (D // 2) ** -0.5, 0.25, ((0, 8), (1, 4))),
        "w_key": normal_values(key_of[5], (D, D), D ** -0.5, 0.1875, ((0, 8), (1, 4))),
        "w_value": normal_values(key_of[6], (D, D), D ** -0.5, 0.1875, ((0, 8), (1, 4))),
        "w_out": normal_values(key_of[7], (D, D), (D // 32) ** -0.5, 1.0, ((0, 4), (1, 8))),
        "w_in": normal_values(key_of[8], (D, FF), D ** -0.5, 0.1875, ((0, 8), (1, 4))),
        "w_back": normal_values(key_of[9], (FF, D), (FF // 2) ** -0.5, 0.125, ((0, 4), (1, 8))),
        "bias_query": normal_values(key_of[10], (HEADS, HEAD), 0.5, 3.0, ((0, 4), (1, 8))),
        "bias_value": normal_values(key_of[11], (HEADS, HEAD), 0.5, 3.0, ((0, 4), (1, 8))),
        "bias_out": normal_values(key_of[12], (D,), 0.5, 3.0, ((0, 8),)),
        "bias_in": normal_values(key_of[13], (FF // HEAD, HEAD), 0.5, 3.0, ((0, 4), (1, 8))),
        "bias_back": normal_values(key_of[14], (D,), 0.5, 3.0, ((0, 8),)),
        "gain_first": jnp.clip(1.0 + 0.18 * jax.random.normal(key_of[15], (D,), jnp.float32), 0.099609375, 1.8984375).astype(jnp.bfloat16),
        "shift_first": normal_values(key_of[16], (D,), 0.5, 3.0, ((0, 8),)),
        "gain_second": jnp.clip(1.0 + 0.18 * jax.random.normal(key_of[17], (D,), jnp.float32), 0.099609375, 1.8984375).astype(jnp.bfloat16),
        "shift_second": normal_values(key_of[18], (D,), 0.5, 3.0, ((0, 8),)),
    }


@jax.custom_vjp
def low(v):
    return lax.optimization_barrier(v.astype(jnp.bfloat16)).astype(jnp.float32)

@jax.custom_vjp
def low_back(v):
    return v

def low_keep(v):
    return (low(v), None)

def low_pass(kept, grad):
    return (grad,)

def back_keep(v):
    return (v, None)

def back_low(kept, grad):
    return (low(grad),)
low.defvjp(low_keep, low_pass)
low_back.defvjp(back_keep, back_low)

def product(left_side, right_side):
    return jnp.dot(left_side, right_side, precision=lax.Precision.HIGHEST, preferred_element_type=jnp.float32)

def layer_norm(values, gain_vector, shift_vector):
    centred = values - lax.optimization_barrier(jnp.mean(values, axis=-1, keepdims=True))
    scaling = lax.rsqrt(lax.optimization_barrier(jnp.mean(centred * centred, axis=-1, keepdims=True)) + 1e-05)
    return centred * scaling * gain_vector + shift_vector

def attend_block(query_block, key_heads, value_heads, allowed):
    scores = low_back(jnp.einsum('qhd,khd->hqk', query_block, key_heads, precision=lax.Precision.HIGHEST))
    scores = jnp.where(allowed[None], scores, -1e+30)
    highest = lax.optimization_barrier(jnp.max(scores, axis=-1, keepdims=True))
    weights = jnp.exp(scores - highest)
    probabilities = weights / lax.optimization_barrier(jnp.sum(weights, axis=-1, keepdims=True))
    return jnp.einsum('hqk,khd->qhd', low(probabilities), value_heads, precision=lax.Precision.HIGHEST)

def sequence_layer(inputs, weights_all, segment_row, keep_row):
    w_query, w_key, w_value, w_out, w_in, w_back, bias_query, bias_value, bias_out, bias_in, bias_back, gain_first, shift_first, gain_second, shift_second = weights_all
    queries = low_back(low((product(inputs, w_query) + bias_query.reshape(-1)) * 0.125))
    key_rows = low_back(low(product(inputs, w_key)))
    value_rows = low_back(low(product(inputs, w_value) + bias_value.reshape(-1)))
    position = jnp.arange(LEN)
    allowed = (segment_row[:, None] == segment_row[None, :]) & ((keep_row[None, :] == 1) | (position[:, None] == position[None, :]))
    blocks = LEN // QBLOCK
    query_blocks = queries.reshape(blocks, QBLOCK, HEADS, HEAD)
    allowed_blocks = allowed.reshape(blocks, QBLOCK, LEN)
    key_heads = key_rows.reshape(LEN, HEADS, HEAD)
    value_heads = value_rows.reshape(LEN, HEADS, HEAD)
    checked = jax.checkpoint(attend_block)
    mixed_heads = lax.map(lambda block_pair: checked(block_pair[0], key_heads, value_heads, block_pair[1]), (query_blocks, allowed_blocks))
    mixed_heads = low_back(low(mixed_heads.reshape(LEN, D)))
    residual = inputs + low_back(product(mixed_heads, w_out) + bias_out)
    normed = layer_norm(residual, gain_first, shift_first)
    hidden_pre = low_back(product(low(normed), w_in) + bias_in.reshape(-1))
    activated = low(jax.nn.gelu(hidden_pre, approximate=False))
    second = normed + low_back(product(activated, w_back) + bias_back)
    return layer_norm(second, gain_second, shift_second) * keep_row[:, None].astype(jnp.float32)

def reference(tokens, segment_ids, keep_mask, cotangent, w_query, w_key, w_value, w_out, w_in, w_back, bias_query, bias_value, bias_out, bias_in, bias_back, gain_first, shift_first, gain_second, shift_second):
    params = tuple((weight_array.astype(jnp.float32) for weight_array in (w_query, w_key, w_value, w_out, w_in, w_back, bias_query, bias_value, bias_out, bias_in, bias_back, gain_first, shift_first, gain_second, shift_second)))

    def one_sequence(totals, sequence_items):
        seq_tokens, segment_row, keep_row, seq_cotangent = sequence_items
        outputs, pull_back = jax.vjp(lambda inputs, weights_all: sequence_layer(inputs, weights_all, segment_row, keep_row), seq_tokens.astype(jnp.float32), params)
        grad_inputs, grad_params = pull_back(seq_cotangent.astype(jnp.float32))
        totals = jax.tree.map(lambda total_one, new_one: total_one + new_one, totals, grad_params)
        return (totals, (outputs.astype(jnp.bfloat16), grad_inputs.astype(jnp.bfloat16)))
    zeros_all = jax.tree.map(jnp.zeros_like, params)
    totals, (outputs, grad_inputs) = lax.scan(one_sequence, zeros_all, (tokens.reshape(SEQS, LEN, D), segment_ids, keep_mask, cotangent.reshape(SEQS, LEN, D)))
    return (outputs.reshape(TOKENS, D), grad_inputs.reshape(TOKENS, D), totals[0], totals[1], totals[2], totals[3], totals[4], totals[5], totals[6], totals[7], totals[8], totals[9], totals[10], totals[11], totals[12], totals[13], totals[14])
```

```python
import functools

import jax
import jax.numpy as jnp
from jax import lax
from jax.experimental import pallas as pl
from jax.experimental.pallas import tpu as pltpu
from jax.sharding import PartitionSpec as P

HEAD = 64
DOC_MOST = 800
BLOCK = 256
MESH = pl.DeviceIdType.MESH
BF16 = jnp.bfloat16
F32 = jnp.float32
FAR_NEG = -1e30


def dot_nn(left, right):
    return lax.dot_general(left, right, (((1,), (0,)), ((), ())), preferred_element_type=F32)


def dot_nt(left, right):
    return lax.dot_general(left, right, (((1,), (1,)), ((), ())), preferred_element_type=F32)


def dot_tn(left, right):
    return lax.dot_general(left, right, (((0,), (0,)), ((), ())), preferred_element_type=F32)


def bits_of(count):
    found, bit = [], 1
    while bit < count:
        found.append(bit)
        bit *= 2
    return found


def label_of(position, count):
    half = count // 2
    return ((position % half) << 1) | (position // half)


def permute_columns(values, table, ndp):
    rows, width = values.shape
    piece = width // ndp
    if piece % 128:
        return jnp.take(values.reshape(rows, ndp, piece), table, axis=1).reshape(rows, width)

    def body(table_ref, in_ref, out_ref):
        out_ref[...] = in_ref[...]

    return pl.pallas_call(
        body,
        out_shape=jax.ShapeDtypeStruct(values.shape, values.dtype),
        grid_spec=pltpu.PrefetchScalarGridSpec(
            num_scalar_prefetch=1,
            grid=(ndp,),
            in_specs=[pl.BlockSpec((rows, piece), lambda j, t: (0, t[j]))],
            out_specs=pl.BlockSpec((rows, piece), lambda j, t: (0, j)),
        ),
    )(table, values)


def gather_all(messages, tokens, ndp, nz):
    count = len(messages)
    rows, width = messages[0].shape
    local, depth = tokens.shape
    far = -(-(DOC_MOST - 1 - local) // 16) * 16
    window = 5 * local
    own0, l1, r1 = 2 * local, local, 3 * local
    l2, r2 = 2 * local - local - far, 4 * local
    chunks = 2 if rows % 32 == 0 else 1
    piece = rows // chunks
    zbits = bits_of(nz)[::-1]
    dbits = bits_of(ndp)
    xy = dbits[1:]
    half = ndp // 2
    pairs = [(m, c) for c in range(chunks) for m in range(count)]
    zorder, parent = [0], {}
    for bit in zbits:
        for q in list(zorder):
            parent[q ^ bit] = (q, bit)
            zorder.append(q ^ bit)
    total = len(pairs) * (nz - 1) + len(pairs) * nz * half
    stages = len(xy) + 1
    lags = [3 * s for s in range(stages)]

    def kernel(*refs):
        ins, tok = refs[:count], refs[count]
        outs, win = refs[count + 1 : 2 * count + 1], refs[2 * count + 1]
        zeros, ssem, rsem, lsem, hs, hr = refs[2 * count + 2 :]
        d = lax.axis_index("dp")
        z = lax.axis_index("tensor")
        barrier = pltpu.get_barrier_semaphore()
        for step in range(1, nz):
            pl.semaphore_signal(
                barrier, inc=1, device_id=(d, lax.rem(z + step, nz)), device_id_type=MESH
            )
        for bit in dbits:
            pl.semaphore_signal(barrier, inc=1, device_id=(d ^ bit, z), device_id_type=MESH)

        locals_ = []

        def local_copy(src, dst):
            cp = pltpu.make_async_copy(src, dst, lsem.at[len(locals_)])
            locals_.append(cp)
            return cp

        for m in range(count):
            local_copy(ins[m], outs[m].at[0, 0]).start()
        local_copy(tok, win.at[pl.ds(own0, local)]).start()
        zeros[...] = jnp.zeros_like(zeros)
        edge = local - far
        if edge:
            local_copy(zeros.at[pl.ds(0, edge)], win.at[pl.ds(0, edge)]).start()
            local_copy(zeros.at[pl.ds(0, edge)], win.at[pl.ds(window - edge, edge)]).start()
        fills = [
            (z < 1, local_copy(zeros, win.at[pl.ds(l1, local)])),
            (z < 2, local_copy(zeros.at[pl.ds(0, far)], win.at[pl.ds(l2, far)])),
            (z > nz - 2, local_copy(zeros, win.at[pl.ds(r1, local)])),
            (z > nz - 3, local_copy(zeros.at[pl.ds(0, far)], win.at[pl.ds(r2, far)])),
        ]
        fixed = locals_[:-4]
        for when, cp in fills:
            pl.when(when)(cp.start)

        pl.semaphore_wait(barrier, nz - 1 + len(dbits))

        def halo_copy(src, dst, target, index):
            return pltpu.make_async_remote_copy(
                src_ref=src,
                dst_ref=dst,
                send_sem=hs.at[index],
                recv_sem=hr.at[index],
                device_id=(d, target),
                device_id_type=MESH,
            )

        up, down = lax.rem(z + 1, nz), lax.rem(z + nz - 1, nz)
        to_up = halo_copy(tok, win.at[pl.ds(l1, local)], up, 0)
        to_down = halo_copy(tok, win.at[pl.ds(r1, local)], down, 1)
        far_up = halo_copy(
            win.at[pl.ds(l1 + local - far, far)], win.at[pl.ds(l2, far)], up, 2
        )
        far_down = halo_copy(win.at[pl.ds(r1, far)], win.at[pl.ds(r2, far)], down, 3)

        counter, every = [0], []

        def remote(src, dst, device):
            index = counter[0]
            counter[0] += 1
            cp = pltpu.make_async_remote_copy(
                src_ref=src,
                dst_ref=dst,
                send_sem=ssem.at[index],
                recv_sem=rsem.at[index],
                device_id=device,
                device_id_type=MESH,
            )
            every.append(cp)
            return cp

        def block(m, a, p, c):
            return outs[m].at[a, p, pl.ds(c * piece, piece)]

        zcopies = {}
        for q, (par, bit) in parent.items():
            for m, c in pairs:
                src = ins[m].at[pl.ds(c * piece, piece)] if par == 0 else block(m, par, 0, c)
                zcopies[m, c, q] = remote(src, block(m, q, 0, c), (d, z ^ bit))
        items = [(m, c, a) for a in zorder for (m, c) in pairs]
        plan = []
        for i, (m, c, a) in enumerate(items):
            mine, held = [], [0]
            for bit in xy if i % 2 == 0 else xy[::-1]:
                step = []
                for p in held:
                    own = p == 0 and a == 0
                    src = ins[m].at[pl.ds(c * piece, piece)] if own else block(m, a, p, c)
                    step.append(remote(src, block(m, a, p ^ (bit >> 1), c), (d ^ bit, z)))
                mine.append(step)
                held = held + [p ^ (bit >> 1) for p in held]
            part = pl.ds(c * piece, piece)
            mine.append(
                [
                    remote(
                        outs[m].at[a, pl.ds(0, half), part],
                        outs[m].at[a, pl.ds(half, half), part],
                        (d ^ 1, z),
                    )
                ]
            )
            plan.append(mine)

        pl.when(z < nz - 1)(to_up.start)
        pl.when(z > 0)(to_down.start)
        for m, c in pairs:
            for q, (par, _) in parent.items():
                if par == 0:
                    zcopies[m, c, q].start()
        for cp in fixed:
            cp.wait()
        for when, cp in fills:
            pl.when(when)(cp.wait)
        relay_at = 2 * len(pairs)
        for t in range(len(items) + lags[-1]):
            if t == relay_at:
                pl.when(z > 0)(to_up.wait_recv)
                pl.when((z > 0) & (z < nz - 1))(far_up.start)
                pl.when(z < nz - 1)(to_down.wait_recv)
                pl.when((z > 0) & (z < nz - 1))(far_down.start)
            for s in range(stages):
                i = t - lags[s]
                if not 0 <= i < len(items):
                    continue
                m, c, a = items[i]
                if s == 0:
                    if a:
                        zcopies[m, c, a].wait_recv()
                        for q, (par, _) in parent.items():
                            if par == a:
                                zcopies[m, c, q].start()
                else:
                    for cp in plan[i][s - 1]:
                        cp.wait_recv()
                for cp in plan[i][s]:
                    cp.start()
        for mine in plan:
            for cp in mine[-1]:
                cp.wait_recv()
        pl.when(z > 1)(far_up.wait_recv)
        pl.when(z < nz - 2)(far_down.wait_recv)
        for cp in every:
            cp.wait_send()
        pl.when(z < nz - 1)(to_up.wait_send)
        pl.when(z > 0)(to_down.wait_send)
        pl.when((z > 0) & (z < nz - 1))(far_up.wait_send)
        pl.when((z > 0) & (z < nz - 1))(far_down.wait_send)

    any_spec = pl.BlockSpec(memory_space=pl.ANY)
    outs = pl.pallas_call(
        kernel,
        out_shape=[jax.ShapeDtypeStruct((nz, ndp, rows, width), BF16)] * count
        + [jax.ShapeDtypeStruct((window, depth), BF16)],
        in_specs=[pl.BlockSpec(memory_space=pltpu.VMEM)] * (count + 1),
        out_specs=[any_spec] * (count + 1),
        scratch_shapes=[
            pltpu.VMEM((local, depth), BF16),
            pltpu.SemaphoreType.DMA((total,)),
            pltpu.SemaphoreType.DMA((total,)),
            pltpu.SemaphoreType.DMA((count + 7,)),
            pltpu.SemaphoreType.DMA((4,)),
            pltpu.SemaphoreType.DMA((4,)),
        ],
        compiler_params=pltpu.CompilerParams(collective_id=0, has_side_effects=True),
    )(*messages, tokens)
    return [out.reshape(nz, ndp * rows, width) for out in outs[:count]], outs[count]


def project(window_rows, weights, biases, bounds, local):
    nz, depth, _ = weights.shape
    window = window_rows.shape[0]
    own0 = 2 * local
    heads_width = weights.shape[2] // 4

    def body(bounds_ref, x_ref, w_ref, b_ref, q_ref, k_ref, v_ref, kt_ref, vt_ref):
        hw = heads_width
        bias = b_ref[0]
        wq = w_ref[0, :, 0:hw]
        for i in range(local // BLOCK):
            rows = x_ref[pl.ds(own0 + i * BLOCK, BLOCK), :]
            q_ref[0, pl.ds(i * BLOCK, BLOCK), :] = (
                (dot_nn(rows, wq) + bias[:, 0:hw]) * 0.125
            ).astype(BF16)

        def one(j, carry):
            start = pl.multiple_of(j * BLOCK, BLOCK)
            rows = x_ref[pl.ds(start, BLOCK), :]
            kv = dot_nn(rows, w_ref[0, :, hw : 3 * hw])
            key = kv[:, :hw].astype(BF16)
            value = (kv[:, hw:] + bias[:, hw:]).astype(BF16)
            k_ref[0, pl.ds(start, BLOCK), :] = key
            v_ref[0, pl.ds(start, BLOCK), :] = value
            kt_ref[0, :, pl.ds(start, BLOCK)] = key.T
            vt_ref[0, :, pl.ds(start, BLOCK)] = value.T
            return carry

        lax.fori_loop(bounds_ref[0], bounds_ref[1], one, 0)

    hw = heads_width
    return pl.pallas_call(
        body,
        out_shape=[
            jax.ShapeDtypeStruct((nz, local, hw), BF16),
            jax.ShapeDtypeStruct((nz, window, hw), BF16),
            jax.ShapeDtypeStruct((nz, window, hw), BF16),
            jax.ShapeDtypeStruct((nz, hw, window), BF16),
            jax.ShapeDtypeStruct((nz, hw, window), BF16),
        ],
        grid_spec=pltpu.PrefetchScalarGridSpec(
            num_scalar_prefetch=1,
            grid=(nz,),
            in_specs=[
                pl.BlockSpec((window, depth), lambda a, b: (0, 0)),
                pl.BlockSpec((1, depth, 4 * hw), lambda a, b: (a, 0, 0)),
                pl.BlockSpec((1, 1, 2 * hw), lambda a, b: (a, 0, 0)),
            ],
            out_specs=[
                pl.BlockSpec((1, local, hw), lambda a, b: (a, 0, 0)),
                pl.BlockSpec((1, window, hw), lambda a, b: (a, 0, 0)),
                pl.BlockSpec((1, window, hw), lambda a, b: (a, 0, 0)),
                pl.BlockSpec((1, hw, window), lambda a, b: (a, 0, 0)),
                pl.BlockSpec((1, hw, window), lambda a, b: (a, 0, 0)),
            ],
        ),
    )(bounds, window_rows, weights, biases)


def keep_head(values, head):
    lane = lax.broadcasted_iota(jnp.int32, values.shape, 1)
    inside = lane < HEAD if head == 0 else lane >= HEAD
    return jnp.where(inside, values, jnp.zeros_like(values))


def attend(queries, keys, values_t, codes_q, codes_k, bounds):
    nz, local, hw = queries.shape
    window = keys.shape[1]
    pairs = hw // 128

    def body(bounds_ref, q_ref, k_ref, vt_ref, cq_ref, ck_ref, out_ref, lse_ref):
        for i in range(local // BLOCK):
            at = pl.ds(i * BLOCK, BLOCK)
            query = q_ref[0, at, :]
            seg_q = cq_ref[0:1, at]
            pad_q = cq_ref[1:2, at]

            def one(j, carry):
                start = pl.multiple_of(j * BLOCK, BLOCK)
                key = k_ref[0, pl.ds(start, BLOCK), :]
                seg_k = ck_ref[pl.ds(start, BLOCK), 0:1]
                pad_k = ck_ref[pl.ds(start, BLOCK), 1:2]
                allowed = (seg_k == seg_q) | (pad_k == pad_q)
                result = []
                for head in range(2):
                    top, total, acc = carry[head]
                    scores = dot_nt(keep_head(key, head), query)
                    scores = jnp.where(allowed, scores, FAR_NEG)
                    new_top = jnp.maximum(top, jnp.max(scores, axis=0, keepdims=True))
                    shrink = jnp.exp(top - new_top)
                    weights = jnp.exp(scores - new_top)
                    total = total * shrink + jnp.sum(weights, axis=0, keepdims=True)
                    value = vt_ref[0, pl.ds(head * HEAD, HEAD), pl.ds(start, BLOCK)]
                    acc = acc * shrink + dot_nn(value, weights.astype(BF16))
                    result.append((new_top, total, acc))
                return tuple(result)

            fresh = (
                jnp.full((1, BLOCK), FAR_NEG, F32),
                jnp.zeros((1, BLOCK), F32),
                jnp.zeros((HEAD, BLOCK), F32),
            )
            done = lax.fori_loop(bounds_ref[2 * i], bounds_ref[2 * i + 1], one, (fresh, fresh))
            mixed = jnp.concatenate([acc / total for _, total, acc in done], axis=0)
            out_ref[0, at, :] = mixed.T.astype(BF16)
            for head in range(2):
                top, total, _ = done[head]
                lse_ref[0, 0, pl.ds(head, 1), at] = top + jnp.log(total)

    return pl.pallas_call(
        body,
        out_shape=[
            jax.ShapeDtypeStruct((nz, local, hw), BF16),
            jax.ShapeDtypeStruct((nz, pairs, 2, local), F32),
        ],
        grid_spec=pltpu.PrefetchScalarGridSpec(
            num_scalar_prefetch=1,
            grid=(nz, pairs),
            in_specs=[
                pl.BlockSpec((1, local, 128), lambda a, h, b: (a, 0, h)),
                pl.BlockSpec((1, window, 128), lambda a, h, b: (a, 0, h)),
                pl.BlockSpec((1, 128, window), lambda a, h, b: (a, h, 0)),
                pl.BlockSpec((2, local), lambda a, h, b: (0, 0)),
                pl.BlockSpec((window, 2), lambda a, h, b: (0, 0)),
            ],
            out_specs=[
                pl.BlockSpec((1, local, 128), lambda a, h, b: (a, 0, h)),
                pl.BlockSpec((1, 1, 2, local), lambda a, h, b: (a, h, 0, 0)),
            ],
        ),
    )(bounds, queries, keys, values_t, codes_q, codes_k)


def attend_back(queries, keys, keys_t, values, grads, mixed, lse, codes_q, codes_k, bounds):
    nz, local, hw = queries.shape
    window = keys.shape[1]
    pairs = hw // 128
    blocks = local // BLOCK

    def body(
        bounds_ref,
        q_ref,
        k_ref,
        kt_ref,
        v_ref,
        g_ref,
        m_ref,
        lse_ref,
        cq_ref,
        ck_ref,
        dq_ref,
        dk_ref,
        dv_ref,
        dqt,
        inner,
    ):
        dqt[...] = jnp.zeros_like(dqt)
        for i in range(blocks):
            at = pl.ds(i * BLOCK, BLOCK)
            both = (g_ref[0, at, :].astype(F32) * m_ref[0, at, :].astype(F32)).T
            for head in range(2):
                part = both[head * HEAD : (head + 1) * HEAD]
                inner[pl.ds(head, 1), at] = jnp.sum(part, axis=0, keepdims=True)

        lo = bounds_ref[0]
        hi = bounds_ref[2 * blocks - 1]

        def one(j, carry):
            start = pl.multiple_of(j * BLOCK, BLOCK)
            rows = pl.ds(start, BLOCK)
            key = k_ref[0, rows, :]
            value = v_ref[0, rows, :]
            seg_k = ck_ref[rows, 0:1]
            pad_k = ck_ref[rows, 1:2]
            dk_ref[0, rows, :] = jnp.zeros((BLOCK, 128), BF16)
            dv_ref[0, rows, :] = jnp.zeros((BLOCK, 128), BF16)

            def pair(i, gk, gv):
                at = pl.ds(i * BLOCK, BLOCK)
                query = q_ref[0, at, :]
                grad = g_ref[0, at, :]
                allowed = (seg_k == cq_ref[0:1, at]) | (pad_k == cq_ref[1:2, at])
                for head in range(2):
                    scores = dot_nt(keep_head(key, head), query)
                    scores = jnp.where(allowed, scores, FAR_NEG)
                    probs = jnp.exp(scores - lse_ref[0, 0, pl.ds(head, 1), at])
                    slope = dot_nt(keep_head(value, head), grad)
                    change = (probs * (slope - inner[pl.ds(head, 1), at])).astype(BF16)
                    gv = gv + dot_nn(probs.astype(BF16), keep_head(grad, head))
                    gk = gk + dot_nn(change, keep_head(query, head))
                    part = pl.ds(head * HEAD, HEAD)
                    dqt[part, at] += dot_nn(kt_ref[0, part, rows], change)
                return gk, gv

            gk = jnp.zeros((BLOCK, 128), F32)
            gv = jnp.zeros((BLOCK, 128), F32)
            for i in range(blocks):
                inside = (j >= bounds_ref[2 * i]) & (j < bounds_ref[2 * i + 1])
                gk, gv = lax.cond(
                    inside, functools.partial(pair, i), lambda gk, gv: (gk, gv), gk, gv
                )
            dk_ref[0, rows, :] = gk.astype(BF16)
            dv_ref[0, rows, :] = gv.astype(BF16)
            return carry

        lax.fori_loop(lo, hi, one, 0)
        for i in range(blocks):
            at = pl.ds(i * BLOCK, BLOCK)
            dq_ref[0, at, :] = dqt[:, at].T.astype(BF16) * BF16(0.125)

    block_q = pl.BlockSpec((1, local, 128), lambda a, h, b: (a, 0, h))
    block_k = pl.BlockSpec((1, window, 128), lambda a, h, b: (a, 0, h))
    return pl.pallas_call(
        body,
        out_shape=[
            jax.ShapeDtypeStruct((nz, local, hw), BF16),
            jax.ShapeDtypeStruct((nz, window, hw), BF16),
            jax.ShapeDtypeStruct((nz, window, hw), BF16),
        ],
        grid_spec=pltpu.PrefetchScalarGridSpec(
            num_scalar_prefetch=1,
            grid=(nz, pairs),
            in_specs=[
                block_q,
                block_k,
                pl.BlockSpec((1, 128, window), lambda a, h, b: (a, h, 0)),
                block_k,
                block_q,
                block_q,
                pl.BlockSpec((1, 1, 2, local), lambda a, h, b: (a, h, 0, 0)),
                pl.BlockSpec((2, local), lambda a, h, b: (0, 0)),
                pl.BlockSpec((window, 2), lambda a, h, b: (0, 0)),
            ],
            out_specs=[block_q, block_k, block_k],
            scratch_shapes=[pltpu.VMEM((128, local), F32), pltpu.VMEM((2, local), F32)],
        ),
    )(bounds, queries, keys, keys_t, values, grads, mixed, lse, codes_q, codes_k)


def project_back(window_rows, weights, dq, dk, dv, attn_low, mixed, bounds):
    nz, depth, width = weights.shape
    window = window_rows.shape[0]
    local = dq.shape[1]
    own0 = 2 * local
    hw = width // 4

    def body(
        bounds_ref,
        x_ref,
        w_ref,
        dq_ref,
        dk_ref,
        dv_ref,
        g_ref,
        m_ref,
        dw_ref,
        dx_ref,
        bias_ref,
        acc,
        dkv,
    ):
        a = pl.program_id(0)

        @pl.when(a == 0)
        def _():
            acc[...] = jnp.zeros_like(acc)

        own = pl.ds(own0, local)
        grad_q = dq_ref[0]
        dw_ref[0, :, 0:hw] = dot_tn(x_ref[own, :], grad_q).astype(BF16)
        dw_ref[0, :, 3 * hw :] = dot_tn(g_ref[...], m_ref[0]).astype(BF16)
        acc[own, :] += dot_nt(grad_q, w_ref[0, :, 0:hw])
        bias_q = jnp.sum(grad_q.astype(F32), axis=0, keepdims=True)
        dkv[...] = jnp.zeros_like(dkv)

        def one(j, bias_v):
            start = pl.multiple_of(j * BLOCK, BLOCK)
            rows = pl.ds(start, BLOCK)
            both = jnp.concatenate([dk_ref[0, rows, :], dv_ref[0, rows, :]], axis=1)
            dkv[...] += dot_tn(x_ref[rows, :], both)
            acc[rows, :] += dot_nt(both, w_ref[0, :, hw : 3 * hw])
            return bias_v + jnp.sum(both[:, hw:].astype(F32), axis=0, keepdims=True)

        bias_v = lax.fori_loop(bounds_ref[0], bounds_ref[1], one, jnp.zeros((1, hw), F32))
        dw_ref[0, :, hw : 3 * hw] = dkv[...].astype(BF16)
        bias_ref[0] = jnp.concatenate([bias_q, bias_v], axis=1)

        @pl.when(a == nz - 1)
        def _():
            dx_ref[...] = acc[...].astype(BF16)

    def fixed(shape):
        return pl.BlockSpec(shape, lambda a, b: (0,) * len(shape))

    def by_slot(shape):
        return pl.BlockSpec((1,) + shape, lambda a, b: (a,) + (0,) * len(shape))

    return pl.pallas_call(
        body,
        out_shape=[
            jax.ShapeDtypeStruct((nz, depth, width), BF16),
            jax.ShapeDtypeStruct((window, depth), BF16),
            jax.ShapeDtypeStruct((nz, 1, 2 * hw), F32),
        ],
        grid_spec=pltpu.PrefetchScalarGridSpec(
            num_scalar_prefetch=1,
            grid=(nz,),
            in_specs=[
                fixed((window, depth)),
                by_slot((depth, width)),
                by_slot((local, hw)),
                by_slot((window, hw)),
                by_slot((window, hw)),
                fixed((local, depth)),
                by_slot((local, hw)),
            ],
            out_specs=[by_slot((depth, width)), fixed((window, depth)), by_slot((1, 2 * hw))],
            scratch_shapes=[
                pltpu.VMEM((window, depth), F32),
                pltpu.VMEM((depth, 2 * hw), F32),
            ],
        ),
    )(bounds, window_rows, weights, dq, dk, dv, attn_low, mixed)


def swap(values, axis, count, bit):
    return lax.ppermute(values, axis, [(i, i ^ bit) for i in range(count)])


def reduce_shards(values, ndp, nz, flip):
    half = ndp // 2
    held = values.reshape(nz, 2, half, *values.shape[2:])
    got = swap(held[:, 1], "dp", ndp, 1)
    held = (held[:, 0].astype(F32) + got.astype(F32)).astype(BF16)
    order = bits_of(ndp)[1:]
    shape = held.shape
    held = held.reshape((nz,) + (2,) * len(order) + shape[2:])
    axes = {bit: len(order) - k for k, bit in enumerate(order)}
    live = sorted(order)
    for bit in order[::-1] if flip else order:
        axis = axes[bit] - sum(1 for other in order if other not in live and axes[other] < axes[bit])
        keep, send = jnp.take(held, 0, axis=axis), jnp.take(held, 1, axis=axis)
        got = swap(send, "dp", ndp, bit)
        held = (keep.astype(F32) + got.astype(F32)).astype(BF16)
        live.remove(bit)
    held = held.reshape((nz,) + shape[2:])
    for bit in bits_of(nz)[::-1]:
        pass
    zbits = bits_of(nz)
    held = held.reshape((2,) * len(zbits) + shape[2:])
    for bit in zbits:
        keep, send = jnp.take(held, 0, axis=len(zbits) - 1 - zbits.index(bit)), jnp.take(
            held, 1, axis=len(zbits) - 1 - zbits.index(bit)
        )
        got = swap(send, "tensor", nz, bit)
        total = keep.astype(F32) + got.astype(F32)
        held = total if bit == zbits[-1] else total.astype(BF16)
    return held


def reduce_message(values, ndp, nz):
    nz_, depth, width = values.shape
    blocks = values.reshape(nz, ndp, depth // ndp, width)
    left = reduce_shards(blocks[..., : width // 2], ndp, nz, False)
    right = reduce_shards(blocks[..., width // 2 :], ndp, nz, True)
    return jnp.concatenate([left, right], axis=-1)


def return_halo(dx, local, nz):
    far = -(-(DOC_MOST - 1 - local) // 16) * 16
    up = [(i, i + 1) for i in range(nz - 1)]
    down = [(i + 1, i) for i in range(nz - 1)]
    l2, l1, own0, r1, r2 = local - far, local, 2 * local, 3 * local, 4 * local
    from_up = lax.ppermute(dx[l2 : l2 + far], "tensor", down)
    from_down = lax.ppermute(dx[r2 : r2 + far], "tensor", up)
    left = dx[l1 : l1 + local].astype(F32)
    left = left + jnp.pad(from_up.astype(F32), ((local - far, 0), (0, 0)))
    right = dx[r1 : r1 + local].astype(F32)
    right = right + jnp.pad(from_down.astype(F32), ((0, local - far), (0, 0)))
    got_up = lax.ppermute(left.astype(BF16), "tensor", down)
    got_down = lax.ppermute(right.astype(BF16), "tensor", up)
    return dx[own0 : own0 + local].astype(F32) + got_up.astype(F32) + got_down.astype(F32)


def normalize(values, gain_vector, shift_vector):
    centred = values - jnp.mean(values, axis=-1, keepdims=True)
    scaling = lax.rsqrt(jnp.mean(centred * centred, axis=-1, keepdims=True) + 1e-05)
    unit_values = centred * scaling
    return (unit_values * gain_vector + shift_vector, unit_values, scaling)


def normalize_back(grad_values, unit_values, scaling, gain_vector):
    grad_unit = grad_values * gain_vector
    return scaling * (
        grad_unit
        - jnp.mean(grad_unit, axis=-1, keepdims=True)
        - unit_values * jnp.mean(grad_unit * unit_values, axis=-1, keepdims=True)
    )


def gelu_both(values):
    bell = 0.5 * (1.0 + lax.erf(values * 0.7071067811865476))
    slope = bell + values * jnp.exp(-0.5 * values * values) * 0.3989422804014327
    return (values * bell).astype(BF16), slope.astype(BF16)


def on_device(ndp, nz, *arrays):
    (
        tokens,
        segment_ids,
        keep_mask,
        cotangent,
        w_query,
        w_key,
        w_value,
        w_out,
        w_in,
        w_back,
        bias_query,
        bias_value,
        bias_out,
        bias_in,
        bias_back,
        gain_first,
        shift_first,
        gain_second,
        shift_second,
    ) = arrays
    local, depth = tokens.shape
    hw = w_query.shape[1]
    heads_here = hw // HEAD
    hidden_here = w_in.shape[1]
    piece = depth // ndp
    inner_piece = bias_query.shape[1]
    d = lax.axis_index("dp")
    z = lax.axis_index("tensor")
    labels = jnp.array([label_of(p, ndp) for p in range(ndp)], jnp.int32)
    where_label = [0] * ndp
    for p in range(ndp):
        where_label[label_of(p, ndp)] = p
    inverse = jnp.array(where_label, jnp.int32)
    into = labels ^ d
    back = jnp.take(inverse, jnp.arange(ndp, dtype=jnp.int32) ^ d)
    slots = jnp.arange(nz, dtype=jnp.int32) ^ z

    small = jnp.concatenate(
        [
            bias_query.reshape(-1),
            bias_value.reshape(-1),
            bias_in.reshape(-1),
            bias_out,
            bias_back,
            gain_first,
            shift_first,
            gain_second,
            shift_second,
        ]
    )
    every = lax.all_gather(small, ("dp", "tensor"), axis=0, tiled=False)
    every = every.reshape(ndp, nz, -1).astype(F32)
    n_q = heads_here * inner_piece
    n_in = bias_in.shape[0] * inner_piece

    def rows_of_heads(part):
        part = jnp.take(part, slots, axis=1)
        part = part.reshape(ndp, nz, -1, inner_piece).transpose(1, 2, 0, 3)
        return part.reshape(nz, -1)

    bias_q = rows_of_heads(every[:, :, :n_q])
    bias_v = rows_of_heads(every[:, :, n_q : 2 * n_q])
    bias_h = rows_of_heads(every[:, :, 2 * n_q : 2 * n_q + n_in])
    vectors = jnp.take(every[:, 0, 2 * n_q + n_in :], into, axis=0)
    vectors = vectors.reshape(ndp, 6, piece).transpose(1, 0, 2).reshape(6, depth)
    b_out, b_back, g_first, s_first, g_second, s_second = [vectors[i] for i in range(6)]
    bias_qv = jnp.concatenate([bias_q, bias_v], axis=1).reshape(nz, 1, 2 * hw)

    length = segment_ids.shape[1]
    window = 5 * local
    own0 = 2 * local
    seg_pad = jnp.pad(segment_ids[0], (own0, own0), constant_values=-1)
    keep_pad = jnp.pad(keep_mask[0], (own0, own0), constant_values=1)
    seg_win = lax.dynamic_slice(seg_pad, (z * local,), (window,))
    keep_win = lax.dynamic_slice(keep_pad, (z * local,), (window,))
    place = jnp.arange(window, dtype=jnp.int32)
    seg_k = jnp.where(keep_win == 1, seg_win, -7)
    pad_k = jnp.where(keep_win == 1, -1, place)
    codes_k = jnp.stack([seg_k, pad_k], axis=1)
    seg_q = seg_win[own0 : own0 + local]
    keep_q = keep_win[own0 : own0 + local]
    pad_q = jnp.where(keep_q == 1, -2, place[own0 : own0 + local])
    codes_q = jnp.stack([seg_q, pad_q], axis=0)
    blocks = local // BLOCK
    first = seg_q.reshape(blocks, BLOCK)[:, 0]
    last = seg_q.reshape(blocks, BLOCK)[:, -1]
    inside = (seg_win >= 0)[None, :]
    before = jnp.sum((seg_win[None, :] < first[:, None]), axis=1, dtype=jnp.int32)
    outside_after = jnp.sum(
        (seg_win[None, :] <= last[:, None]) & inside, axis=1, dtype=jnp.int32
    )
    lead = jnp.maximum(own0 - z * local, 0)
    trail = jnp.maximum(z * local + window - own0 - length, 0)
    low = (before - trail) // BLOCK
    high = (outside_after + lead + BLOCK - 1) // BLOCK
    bounds = jnp.stack([low, high], axis=1).reshape(-1).astype(jnp.int32)
    whole = jnp.stack([bounds[0], bounds[2 * blocks - 1]])
    keep_local = keep_q.astype(F32)[:, None]

    message_a = jnp.concatenate([w_query, w_key, w_value, w_out.T], axis=1)
    tokens_p = permute_columns(tokens, into, ndp)
    cotangent_p = permute_columns(cotangent, into, ndp)
    (full_a, full_i, full_b), window_rows = gather_all(
        [message_a, w_in, w_back.T], tokens_p, ndp, nz
    )

    queries, keys, values, keys_t, values_t = project(
        window_rows, full_a, bias_qv, whole, local
    )
    mixed, lse = attend(queries, keys, values_t, codes_q, codes_k, bounds)
    out_t = full_a[:, :, 3 * hw :]
    attended = sum(dot_nt(mixed[a], out_t[a]) for a in range(nz))
    residual = tokens_p.astype(F32) + attended + b_out
    normed, unit_first, scale_first = normalize(residual, g_first, s_first)
    normed_low = normed.astype(BF16)
    activated, slopes = [], []
    second = normed + b_back
    for a in range(nz):
        act, slope = gelu_both(dot_nn(normed_low, full_i[a]) + bias_h[a])
        activated.append(act)
        slopes.append(slope)
        second = second + dot_nt(act, full_b[a])
    finished, unit_second, scale_second = normalize(second, g_second, s_second)
    output = permute_columns((finished * keep_local).astype(BF16), back, ndp)

    grad_out = cotangent_p.astype(F32) * keep_local
    d_gain_second = jnp.sum(grad_out * unit_second, axis=0)
    d_shift_second = jnp.sum(grad_out, axis=0)
    grad_second = normalize_back(grad_out, unit_second, scale_second, g_second)
    back_low = grad_second.astype(BF16)
    d_bias_back = jnp.sum(back_low.astype(F32), axis=0)
    d_back = jnp.stack([dot_tn(back_low, activated[a]).astype(BF16) for a in range(nz)])
    shard_b = reduce_message(d_back, ndp, nz)
    grad_normed = grad_second
    d_in, d_bias_in = [], []
    for a in range(nz):
        pre = (dot_nn(back_low, full_b[a]) * slopes[a].astype(F32)).astype(BF16)
        d_bias_in.append(jnp.sum(pre.astype(F32), axis=0))
        d_in.append(dot_tn(normed_low, pre).astype(BF16))
        grad_normed = grad_normed + dot_nt(pre, full_i[a])
    shard_i = reduce_message(jnp.stack(d_in), ndp, nz)
    d_gain_first = jnp.sum(grad_normed * unit_first, axis=0)
    d_shift_first = jnp.sum(grad_normed, axis=0)
    grad_residual = normalize_back(grad_normed, unit_first, scale_first, g_first)
    attn_low = grad_residual.astype(BF16)
    d_bias_out = jnp.sum(attn_low.astype(F32), axis=0)
    grad_mixed = jnp.stack([dot_nn(attn_low, out_t[a]).astype(BF16) for a in range(nz)])
    dq, dk, dv = attend_back(
        queries, keys, keys_t, values, grad_mixed, mixed, lse, codes_q, codes_k, bounds
    )
    d_a, dx, d_bias_qv = project_back(
        window_rows, full_a, dq, dk, dv, attn_low, mixed, whole
    )
    shard_a = reduce_message(d_a, ndp, nz)
    grad_tokens = (grad_residual + return_halo(dx, local, nz)).astype(BF16)
    grad_tokens = permute_columns(grad_tokens, back, ndp)

    stacked = jnp.stack(
        [d_bias_out, d_bias_back, d_gain_first, d_shift_first, d_gain_second, d_shift_second]
    ).reshape(6, ndp, piece)
    stacked = jnp.take(stacked, back, axis=1).reshape(6 * depth)
    d_bias_qv = jnp.take(d_bias_qv.reshape(nz, 2 * hw), slots, axis=0).reshape(-1)
    d_bias_h = jnp.take(jnp.stack(d_bias_in), slots, axis=0).reshape(-1)
    sums = lax.psum(jnp.concatenate([stacked, d_bias_qv, d_bias_h]), ("dp", "tensor"))
    vector_sums = sums[: 6 * depth].reshape(6, depth)
    vector_sums = lax.dynamic_slice(vector_sums, (0, d * piece), (6, piece))
    mine = lax.dynamic_slice(
        sums[6 * depth : 6 * depth + nz * 2 * hw].reshape(nz, 2, heads_here, HEAD),
        (z, 0, 0, d * inner_piece),
        (1, 2, heads_here, inner_piece),
    )
    mine_in = lax.dynamic_slice(
        sums[6 * depth + nz * 2 * hw :].reshape(nz, hidden_here // HEAD, HEAD),
        (z, 0, d * inner_piece),
        (1, hidden_here // HEAD, inner_piece),
    )
    return (
        output,
        grad_tokens,
        shard_a[:, :hw],
        shard_a[:, hw : 2 * hw],
        shard_a[:, 2 * hw : 3 * hw],
        shard_a[:, 3 * hw :].T,
        shard_i,
        shard_b.T,
        mine[0, 0],
        mine[0, 1],
        vector_sums[0],
        mine_in[0],
        vector_sums[1],
        vector_sums[2],
        vector_sums[3],
        vector_sums[4],
        vector_sums[5],
    )


def solution(mesh):
    ndp, nz = mesh.shape["dp"], mesh.shape["tensor"]
    return jax.shard_map(
        functools.partial(on_device, ndp, nz),
        mesh=mesh,
        in_specs=(
            P(("dp", "tensor"), None),
            P("dp", None),
            P("dp", None),
            P(("dp", "tensor"), None),
            P("dp", "tensor"),
            P("dp", "tensor"),
            P("dp", "tensor"),
            P("tensor", "dp"),
            P("dp", "tensor"),
            P("tensor", "dp"),
            P("tensor", "dp"),
            P("tensor", "dp"),
            P("dp"),
            P("tensor", "dp"),
            P("dp"),
            P("dp"),
            P("dp"),
            P("dp"),
            P("dp"),
        ),
        out_specs=(
            P(("dp", "tensor"), None),
            P(("dp", "tensor"), None),
            P("dp", "tensor"),
            P("dp", "tensor"),
            P("dp", "tensor"),
            P("tensor", "dp"),
            P("dp", "tensor"),
            P("tensor", "dp"),
            P("tensor", "dp"),
            P("tensor", "dp"),
            P("dp"),
            P("tensor", "dp"),
            P("dp"),
            P("dp"),
            P("dp"),
            P("dp"),
            P("dp"),
        ),
        check_vma=False,
    )
```

```python
import functools

import jax
import jax.numpy as jnp
from jax import lax
from jax.experimental import pallas as pl
from jax.experimental.pallas import tpu as pltpu
from jax.sharding import PartitionSpec as P

HEAD = 64
DOC_MOST = 800
BLOCK = 256
MESH = pl.DeviceIdType.MESH
BF16 = jnp.bfloat16
F32 = jnp.float32
FAR_NEG = -1e30


def dot_nn(left, right):
    return lax.dot_general(left, right, (((1,), (0,)), ((), ())), preferred_element_type=F32)


def dot_nt(left, right):
    return lax.dot_general(left, right, (((1,), (1,)), ((), ())), preferred_element_type=F32)


def dot_tn(left, right):
    return lax.dot_general(left, right, (((0,), (0,)), ((), ())), preferred_element_type=F32)


def bits_of(count):
    found, bit = [], 1
    while bit < count:
        found.append(bit)
        bit *= 2
    return found


def far_rows(local):
    return -(-(DOC_MOST - 1 - local) // 16) * 16


def bit_at(value, bit):
    return lax.rem(value // bit, 2)


def gather_all(messages, tokens, ndp, nz):
    count = len(messages)
    local, depth = tokens.shape
    far = far_rows(local)
    window = 5 * local
    own0, l1, r1 = 2 * local, local, 3 * local
    l2, r2 = 2 * local - local - far, 4 * local
    zbits = bits_of(nz)[::-1]
    dbits = bits_of(ndp)[::-1]
    xy = dbits[:-1]
    pairs = []
    for c in range(2):
        for m in range(count):
            rows = messages[m].shape[0]
            chunks = 2 if rows % 32 == 0 else 1
            if c < chunks:
                pairs.append((m, c, rows // chunks))
    zorder, parent = [0], {}
    for bit in zbits:
        for q in list(zorder):
            parent[q ^ bit] = (q, bit)
            zorder.append(q ^ bit)
    stages = len(dbits)
    total = len(pairs) * (nz - 1) + len(pairs) * nz * stages
    lags = [3 * s for s in range(stages)]

    def kernel(*refs):
        ins, tok = refs[:count], refs[count]
        outs, win = refs[count + 1 : 2 * count + 1], refs[2 * count + 1]
        zeros, ssem, rsem, lsem, hs, hr = refs[2 * count + 2 :]
        d = lax.axis_index("dp")
        z = lax.axis_index("tensor")
        barrier = pltpu.get_barrier_semaphore()
        for step in range(1, nz):
            pl.semaphore_signal(
                barrier, inc=1, device_id=(d, lax.rem(z + step, nz)), device_id_type=MESH
            )
        for bit in dbits:
            pl.semaphore_signal(barrier, inc=1, device_id=(d ^ bit, z), device_id_type=MESH)

        own = tuple(bit_at(d, bit) for bit in dbits)
        locals_ = []

        def local_copy(src, dst):
            cp = pltpu.make_async_copy(src, dst, lsem.at[len(locals_)])
            locals_.append(cp)
            return cp

        for m in range(count):
            local_copy(ins[m], outs[m].at[(z,) + own]).start()
        local_copy(tok, win.at[pl.ds(own0, local)]).start()
        zeros[...] = jnp.zeros_like(zeros)
        edge = local - far
        if edge:
            local_copy(zeros.at[pl.ds(0, edge)], win.at[pl.ds(0, edge)]).start()
            local_copy(zeros.at[pl.ds(0, edge)], win.at[pl.ds(window - edge, edge)]).start()
        fills = [
            (z < 1, local_copy(zeros, win.at[pl.ds(l1, local)])),
            (z < 2, local_copy(zeros.at[pl.ds(0, far)], win.at[pl.ds(l2, far)])),
            (z > nz - 2, local_copy(zeros, win.at[pl.ds(r1, local)])),
            (z > nz - 3, local_copy(zeros.at[pl.ds(0, far)], win.at[pl.ds(r2, far)])),
        ]
        fixed = locals_[:-4]
        for when, cp in fills:
            pl.when(when)(cp.start)

        pl.semaphore_wait(barrier, nz - 1 + len(dbits))

        def halo_copy(src, dst, target, index):
            return pltpu.make_async_remote_copy(
                src_ref=src,
                dst_ref=dst,
                send_sem=hs.at[index],
                recv_sem=hr.at[index],
                device_id=(d, target),
                device_id_type=MESH,
            )

        up, down = lax.rem(z + 1, nz), lax.rem(z + nz - 1, nz)
        to_up = halo_copy(tok, win.at[pl.ds(l1, local)], up, 0)
        to_down = halo_copy(tok, win.at[pl.ds(r1, local)], down, 1)
        far_up = halo_copy(
            win.at[pl.ds(l1 + local - far, far)], win.at[pl.ds(l2, far)], up, 2
        )
        far_down = halo_copy(win.at[pl.ds(r1, far)], win.at[pl.ds(r2, far)], down, 3)

        counter, every = [0], []

        def remote(ref, index, device, src=None):
            number = counter[0]
            counter[0] += 1
            cp = pltpu.make_async_remote_copy(
                src_ref=ref.at[index] if src is None else src,
                dst_ref=ref.at[index],
                send_sem=ssem.at[number],
                recv_sem=rsem.at[number],
                device_id=device,
                device_id_type=MESH,
            )
            every.append(cp)
            return cp

        zcopies = {}
        for q, (par, bit) in parent.items():
            for m, c, piece in pairs:
                part = pl.ds(c * piece, piece)
                src = ins[m].at[part] if par == 0 else None
                zcopies[m, c, q] = remote(outs[m], (z ^ par,) + own + (part,), (d, z ^ bit), src)
        items = [(m, c, piece, a) for a in zorder for (m, c, piece) in pairs]
        plan = []
        for i, (m, c, piece, a) in enumerate(items):
            mine, held = [], list(own)
            part = pl.ds(c * piece, piece)
            for bit in (xy if i % 2 == 0 else xy[::-1]) + [1]:
                src = ins[m].at[part] if a == 0 and not mine else None
                index = (z ^ a,) + tuple(held) + (part,)
                mine.append(remote(outs[m], index, (d ^ bit, z), src))
                held[dbits.index(bit)] = slice(None)
            plan.append(mine)

        pl.when(z < nz - 1)(to_up.start)
        pl.when(z > 0)(to_down.start)
        for m, c, _ in pairs:
            for q, (par, _) in parent.items():
                if par == 0:
                    zcopies[m, c, q].start()
        for cp in fixed:
            cp.wait()
        for when, cp in fills:
            pl.when(when)(cp.wait)
        relay_at = 2 * len(pairs)
        for t in range(len(items) + lags[-1]):
            if t == relay_at:
                pl.when(z > 0)(to_up.wait_recv)
                pl.when((z > 0) & (z < nz - 1))(far_up.start)
                pl.when(z < nz - 1)(to_down.wait_recv)
                pl.when((z > 0) & (z < nz - 1))(far_down.start)
            for s in range(stages):
                i = t - lags[s]
                if not 0 <= i < len(items):
                    continue
                m, c, _, a = items[i]
                if s == 0:
                    if a:
                        zcopies[m, c, a].wait_recv()
                        for q, (par, _) in parent.items():
                            if par == a:
                                zcopies[m, c, q].start()
                else:
                    plan[i][s - 1].wait_recv()
                plan[i][s].start()
        for mine in plan:
            mine[-1].wait_recv()
        pl.when(z > 1)(far_up.wait_recv)
        pl.when(z < nz - 2)(far_down.wait_recv)
        for cp in every:
            cp.wait_send()
        pl.when(z < nz - 1)(to_up.wait_send)
        pl.when(z > 0)(to_down.wait_send)
        pl.when((z > 0) & (z < nz - 1))(far_up.wait_send)
        pl.when((z > 0) & (z < nz - 1))(far_down.wait_send)

    any_spec = pl.BlockSpec(memory_space=pl.ANY)
    split = (2,) * len(dbits)
    outs = pl.pallas_call(
        kernel,
        out_shape=[jax.ShapeDtypeStruct((nz,) + split + m.shape, BF16) for m in messages]
        + [jax.ShapeDtypeStruct((window, depth), BF16)],
        in_specs=[pl.BlockSpec(memory_space=pltpu.VMEM)] * (count + 1),
        out_specs=[any_spec] * (count + 1),
        scratch_shapes=[
            pltpu.VMEM((local, depth), BF16),
            pltpu.SemaphoreType.DMA((total,)),
            pltpu.SemaphoreType.DMA((total,)),
            pltpu.SemaphoreType.DMA((count + 7,)),
            pltpu.SemaphoreType.DMA((4,)),
            pltpu.SemaphoreType.DMA((4,)),
        ],
        compiler_params=pltpu.CompilerParams(collective_id=0, has_side_effects=True),
    )(*messages, tokens)
    return outs[:count], outs[count]


def sum_all(partials, dx, residual_grad, ndp, nz):
    count = len(partials)
    local, depth = residual_grad.shape
    far = far_rows(local)
    own0, l1, r1 = 2 * local, local, 3 * local
    l2, r2 = local - far, 4 * local
    zbits = bits_of(nz)
    dbits = bits_of(ndp)[::-1]
    xy = dbits[:-1]
    nxy = len(xy)
    stages = len(dbits)
    pairs = []
    for c in range(2):
        for m in range(count):
            rows = partials[m].shape[2]
            chunks = 2 if rows % 32 == 0 else 1
            if c < chunks:
                pairs.append((m, c, rows // chunks))
    zsteps = []
    live = list(range(nz))
    for bit in zbits:
        zsteps.append((bit, [q for q in live if q & bit]))
        live = [q for q in live if not q & bit]
    zorder = [q for _, sent in zsteps for q in sent] + [0]
    items = [(m, c, piece, a) for a in zorder for (m, c, piece) in pairs]
    total = len(items) * stages + len(pairs) * (nz - 1)
    lag = 3
    shapes = [(p.shape[2], p.shape[3], p.dtype) for p in partials]

    def kernel(*refs):
        ins, dxr, res = refs[:count], refs[count], refs[count + 1]
        k = count + 2
        outs, tok = refs[k : k + count], refs[k + count]
        k += count + 1
        acc = refs[k : k + count]
        k += count
        got = [refs[k + s * count : k + (s + 1) * count] for s in range(stages)]
        k += stages * count
        zgot = refs[k : k + count]
        k += count
        hin, hbuf, hnear, ssem, rsem, lsem, hl, hs, hr = refs[k:]
        d = lax.axis_index("dp")
        z = lax.axis_index("tensor")
        barrier = pltpu.get_barrier_semaphore()
        for step in range(1, nz):
            pl.semaphore_signal(
                barrier, inc=1, device_id=(d, lax.rem(z + step, nz)), device_id_type=MESH
            )
        for bit in dbits:
            pl.semaphore_signal(barrier, inc=1, device_id=(d ^ bit, z), device_id_type=MESH)
        own = [bit_at(d, bit) for bit in dbits]
        core = own[-1]

        def remote(src, dst, number, device, send=ssem, recv=rsem):
            return pltpu.make_async_remote_copy(
                src_ref=src,
                dst_ref=dst,
                send_sem=send.at[number],
                recv_sem=recv.at[number],
                device_id=device,
                device_id_type=MESH,
            )

        everything = (slice(None),) * nxy
        plan, loads = [], []
        for i, (m, c, piece, a) in enumerate(items):
            part = pl.ds(c * piece, piece)
            za = z ^ a
            loads.append(
                pltpu.make_async_copy(
                    ins[m].at[(za,) + everything + (core, part)],
                    acc[m].at[(a,) + everything + (part,)],
                    lsem.at[i],
                )
            )
            steps = []
            order = xy if i % 2 == 0 else xy[::-1]
            first = remote(
                ins[m].at[(za,) + everything + (1 - core, part)],
                got[0][m].at[(a,) + everything + (part,)],
                i * stages,
                (d ^ 1, z),
            )
            steps.append((first, None, everything))
            where = list(everything)
            for s, bit in enumerate(order):
                at = xy.index(bit)
                send, keep = list(where), list(where)
                send[at] = 1 - own[at]
                keep[at] = own[at]
                live_count = nxy - 1 - s
                steps.append(
                    (
                        remote(
                            acc[m].at[(a,) + tuple(send) + (part,)],
                            got[s + 1][m].at[(a,) + (slice(None),) * live_count + (part,)],
                            i * stages + s + 1,
                            (d ^ bit, z),
                        ),
                        tuple(where),
                        tuple(keep),
                    )
                )
                where = keep
            plan.append(steps)

        base = len(items) * stages
        zplan = {}
        number = base
        mine = tuple(own[:-1])
        for pi, (m, c, piece) in enumerate(pairs):
            part = pl.ds(c * piece, piece)
            for bit, sent in zsteps:
                for q in sent:
                    zplan[m, c, q] = remote(
                        acc[m].at[(q,) + mine + (part,)],
                        zgot[m].at[q, part],
                        number,
                        (d, z ^ bit),
                    )
                    number += 1

        up, down = lax.rem(z + 1, nz), lax.rem(z + nz - 1, nz)
        own_load = pltpu.make_async_copy(dxr.at[pl.ds(own0, local)], hin.at[0], hl.at[0])
        left_load = pltpu.make_async_copy(dxr.at[pl.ds(l1, local)], hin.at[1], hl.at[1])
        right_load = pltpu.make_async_copy(dxr.at[pl.ds(r1, local)], hin.at[2], hl.at[2])
        far_down = remote(dxr.at[pl.ds(l2, far)], hbuf.at[0], 0, (d, down), hs, hr)
        far_up = remote(dxr.at[pl.ds(r2, far)], hbuf.at[1], 1, (d, up), hs, hr)
        near_down = remote(hin.at[1], hnear.at[0], 2, (d, down), hs, hr)
        near_up = remote(hin.at[2], hnear.at[1], 3, (d, up), hs, hr)
        for cp in (own_load, left_load, right_load):
            cp.start()
        pl.semaphore_wait(barrier, nz - 1 + len(dbits))
        pl.when(z > 1)(far_down.start)
        pl.when(z < nz - 2)(far_up.start)
        for i in range(len(items)):
            plan[i][0][0].start()
            loads[i].start()

        def halo_one():
            left_load.wait()
            right_load.wait()

            @pl.when((z > 0) & (z < nz - 1))
            def _():
                far_down.wait_recv()
                hin[1, pl.ds(local - far, far), :] += hbuf[0]
                far_up.wait_recv()
                hin[2, pl.ds(0, far), :] += hbuf[1]

            pl.when(z > 0)(near_down.start)
            pl.when(z < nz - 1)(near_up.start)

        def add(target, tindex, source, sindex, start, piece):
            step = min(piece, 32)

            def one(j, carry):
                rows = pl.ds(pl.multiple_of(start + j * step, step), step)
                at = tindex + (rows,)
                target[at] = target[at] + source[sindex + (rows,)]
                return carry

            lax.fori_loop(0, piece // step, one, 0)

        def combos(bits_count):
            result = [()]
            for _ in range(bits_count):
                result = [r + (v,) for r in result for v in (0, 1)]
            return result

        def absorb(i, s):
            m, c, piece, a = items[i]
            plan[i][s][0].wait_recv()
            if s == 0:
                loads[i].wait()
            keep = plan[i][s][2]
            free = [k for k in range(nxy) if isinstance(keep[k], slice)]
            for combo in combos(len(free)):
                index = list(keep)
                for k, v in zip(free, combo):
                    index[k] = v
                add(acc[m], (a,) + tuple(index), got[s][m], (a,) + combo, c * piece, piece)

        def zabsorb(m, c, piece, q):
            bit = next(b for b, sent in zsteps if q in sent)
            zplan[m, c, q].wait_recv()
            add(acc[m], (q ^ bit,) + mine, zgot[m], (q,), c * piece, piece)

        for t in range(len(items) + lag * stages):
            if t == 4:
                halo_one()
            for s in range(stages):
                i = t - lag * s
                if not 0 <= i < len(items):
                    continue
                absorb(i, s)
                if s + 1 < stages:
                    plan[i][s + 1][0].start()
                else:
                    m, c, piece, a = items[i]
                    for bit, sent in zsteps:
                        if (a ^ bit) in sent and not a & bit:
                            if bit < (a & -a if a else nz):
                                zabsorb(m, c, piece, a ^ bit)
                    if a:
                        zplan[m, c, a].start()
        for m, c, piece in pairs:
            part = pl.ds(c * piece, piece)
            outs[m][part, :] = acc[m][(0,) + mine + (part,)].astype(F32)
        own_load.wait()

        @pl.when(z < nz - 1)
        def _():
            near_down.wait_recv()

        @pl.when(z > 0)
        def _():
            near_up.wait_recv()

        step = 64

        def finish(j, carry):
            rows = pl.ds(pl.multiple_of(j * step, step), step)
            value = res[rows, :] + hin[0, rows, :].astype(F32)
            value = value + jnp.where(z < nz - 1, hnear[0, rows, :].astype(F32), 0.0)
            value = value + jnp.where(z > 0, hnear[1, rows, :].astype(F32), 0.0)
            tok[rows, :] = value.astype(BF16)
            return carry

        lax.fori_loop(0, local // step, finish, 0)
        for steps in plan:
            for cp, _, _ in steps:
                cp.wait_send()
        for cp in zplan.values():
            cp.wait_send()
        pl.when(z > 1)(far_down.wait_send)
        pl.when(z < nz - 2)(far_up.wait_send)
        pl.when(z > 0)(near_down.wait_send)
        pl.when(z < nz - 1)(near_up.wait_send)

    any_spec = pl.BlockSpec(memory_space=pl.ANY)
    vmem_spec = pl.BlockSpec(memory_space=pltpu.VMEM)
    split = (2,) * len(dbits)
    scratch = [pltpu.VMEM((nz,) + (2,) * nxy + s[:2], s[2]) for s in shapes]
    for stage in range(stages):
        left = nxy if stage == 0 else nxy - stage
        scratch += [pltpu.VMEM((nz,) + (2,) * left + s[:2], s[2]) for s in shapes]
    scratch += [pltpu.VMEM((nz,) + s[:2], s[2]) for s in shapes]
    scratch += [
        pltpu.VMEM((3, local, depth), BF16),
        pltpu.VMEM((2, far, depth), BF16),
        pltpu.VMEM((2, local, depth), BF16),
        pltpu.SemaphoreType.DMA((total,)),
        pltpu.SemaphoreType.DMA((total,)),
        pltpu.SemaphoreType.DMA((len(items),)),
        pltpu.SemaphoreType.DMA((3,)),
        pltpu.SemaphoreType.DMA((4,)),
        pltpu.SemaphoreType.DMA((4,)),
    ]
    result = pl.pallas_call(
        kernel,
        out_shape=[jax.ShapeDtypeStruct(s[:2], F32) for s in shapes]
        + [jax.ShapeDtypeStruct((local, depth), BF16)],
        in_specs=[any_spec] * (count + 1) + [vmem_spec],
        out_specs=[vmem_spec] * (count + 1),
        scratch_shapes=scratch,
        compiler_params=pltpu.CompilerParams(
            collective_id=1, has_side_effects=True, vmem_limit_bytes=63 * 1024 * 1024
        ),
    )(*[p.reshape((nz,) + split + p.shape[2:]) for p in partials], dx, residual_grad)
    return result[:count], result[count]


def project(window_rows, weights, biases, bounds, local):
    nz, depth, _ = weights.shape
    window = window_rows.shape[0]
    own0 = 2 * local
    heads_width = weights.shape[2] // 4

    def body(bounds_ref, x_ref, w_ref, b_ref, q_ref, k_ref, v_ref, kt_ref, vt_ref):
        hw = heads_width
        bias = b_ref[0]
        wq = w_ref[0, :, 0:hw]
        for i in range(local // BLOCK):
            rows = x_ref[pl.ds(own0 + i * BLOCK, BLOCK), :]
            q_ref[0, pl.ds(i * BLOCK, BLOCK), :] = (
                (dot_nn(rows, wq) + bias[:, 0:hw]) * 0.125
            ).astype(BF16)

        def one(j, carry):
            start = pl.multiple_of(j * BLOCK, BLOCK)
            rows = x_ref[pl.ds(start, BLOCK), :]
            kv = dot_nn(rows, w_ref[0, :, hw : 3 * hw])
            key = kv[:, :hw].astype(BF16)
            value = (kv[:, hw:] + bias[:, hw:]).astype(BF16)
            k_ref[0, pl.ds(start, BLOCK), :] = key
            v_ref[0, pl.ds(start, BLOCK), :] = value
            kt_ref[0, :, pl.ds(start, BLOCK)] = key.T
            vt_ref[0, :, pl.ds(start, BLOCK)] = value.T
            return carry

        lax.fori_loop(bounds_ref[0], bounds_ref[1], one, 0)

    hw = heads_width
    return pl.pallas_call(
        body,
        out_shape=[
            jax.ShapeDtypeStruct((nz, local, hw), BF16),
            jax.ShapeDtypeStruct((nz, window, hw), BF16),
            jax.ShapeDtypeStruct((nz, window, hw), BF16),
            jax.ShapeDtypeStruct((nz, hw, window), BF16),
            jax.ShapeDtypeStruct((nz, hw, window), BF16),
        ],
        grid_spec=pltpu.PrefetchScalarGridSpec(
            num_scalar_prefetch=1,
            grid=(nz,),
            in_specs=[
                pl.BlockSpec((window, depth), lambda a, b: (0, 0)),
                pl.BlockSpec((1, depth, 4 * hw), lambda a, b: (a, 0, 0)),
                pl.BlockSpec((1, 1, 2 * hw), lambda a, b: (a, 0, 0)),
            ],
            out_specs=[
                pl.BlockSpec((1, local, hw), lambda a, b: (a, 0, 0)),
                pl.BlockSpec((1, window, hw), lambda a, b: (a, 0, 0)),
                pl.BlockSpec((1, window, hw), lambda a, b: (a, 0, 0)),
                pl.BlockSpec((1, hw, window), lambda a, b: (a, 0, 0)),
                pl.BlockSpec((1, hw, window), lambda a, b: (a, 0, 0)),
            ],
        ),
    )(bounds, window_rows, weights, biases)


def keep_head(values, head):
    lane = lax.broadcasted_iota(jnp.int32, values.shape, 1)
    inside = lane < HEAD if head == 0 else lane >= HEAD
    return jnp.where(inside, values, jnp.zeros_like(values))


def attend(queries, keys, values_t, codes_q, codes_k, bounds):
    nz, local, hw = queries.shape
    window = keys.shape[1]
    pairs = hw // 128

    def body(bounds_ref, q_ref, k_ref, vt_ref, cq_ref, ck_ref, out_ref, lse_ref):
        for i in range(local // BLOCK):
            at = pl.ds(i * BLOCK, BLOCK)
            query = q_ref[0, at, :]
            seg_q = cq_ref[0:1, at]
            pad_q = cq_ref[1:2, at]

            def one(j, carry):
                start = pl.multiple_of(j * BLOCK, BLOCK)
                key = k_ref[0, pl.ds(start, BLOCK), :]
                seg_k = ck_ref[pl.ds(start, BLOCK), 0:1]
                pad_k = ck_ref[pl.ds(start, BLOCK), 1:2]
                allowed = (seg_k == seg_q) | (pad_k == pad_q)
                result = []
                for head in range(2):
                    top, total, acc = carry[head]
                    scores = dot_nt(keep_head(key, head), query)
                    scores = jnp.where(allowed, scores, FAR_NEG)
                    new_top = jnp.maximum(top, jnp.max(scores, axis=0, keepdims=True))
                    shrink = jnp.exp(top - new_top)
                    weights = jnp.exp(scores - new_top)
                    total = total * shrink + jnp.sum(weights, axis=0, keepdims=True)
                    value = vt_ref[0, pl.ds(head * HEAD, HEAD), pl.ds(start, BLOCK)]
                    acc = acc * shrink + dot_nn(value, weights.astype(BF16))
                    result.append((new_top, total, acc))
                return tuple(result)

            fresh = (
                jnp.full((1, BLOCK), FAR_NEG, F32),
                jnp.zeros((1, BLOCK), F32),
                jnp.zeros((HEAD, BLOCK), F32),
            )
            done = lax.fori_loop(bounds_ref[2 * i], bounds_ref[2 * i + 1], one, (fresh, fresh))
            mixed = jnp.concatenate([acc / total for _, total, acc in done], axis=0)
            out_ref[0, at, :] = mixed.T.astype(BF16)
            for head in range(2):
                top, total, _ = done[head]
                lse_ref[0, 0, pl.ds(head, 1), at] = top + jnp.log(total)

    return pl.pallas_call(
        body,
        out_shape=[
            jax.ShapeDtypeStruct((nz, local, hw), BF16),
            jax.ShapeDtypeStruct((nz, pairs, 2, local), F32),
        ],
        grid_spec=pltpu.PrefetchScalarGridSpec(
            num_scalar_prefetch=1,
            grid=(nz, pairs),
            in_specs=[
                pl.BlockSpec((1, local, 128), lambda a, h, b: (a, 0, h)),
                pl.BlockSpec((1, window, 128), lambda a, h, b: (a, 0, h)),
                pl.BlockSpec((1, 128, window), lambda a, h, b: (a, h, 0)),
                pl.BlockSpec((2, local), lambda a, h, b: (0, 0)),
                pl.BlockSpec((window, 2), lambda a, h, b: (0, 0)),
            ],
            out_specs=[
                pl.BlockSpec((1, local, 128), lambda a, h, b: (a, 0, h)),
                pl.BlockSpec((1, 1, 2, local), lambda a, h, b: (a, h, 0, 0)),
            ],
        ),
    )(bounds, queries, keys, values_t, codes_q, codes_k)


def attend_back(queries, keys, keys_t, values, grads, mixed, lse, codes_q, codes_k, bounds):
    nz, local, hw = queries.shape
    window = keys.shape[1]
    pairs = hw // 128
    blocks = local // BLOCK

    def body(
        bounds_ref,
        q_ref,
        k_ref,
        kt_ref,
        v_ref,
        g_ref,
        m_ref,
        lse_ref,
        cq_ref,
        ck_ref,
        dq_ref,
        dk_ref,
        dv_ref,
        dqt,
        inner,
    ):
        dqt[...] = jnp.zeros_like(dqt)
        for i in range(blocks):
            at = pl.ds(i * BLOCK, BLOCK)
            both = (g_ref[0, at, :].astype(F32) * m_ref[0, at, :].astype(F32)).T
            for head in range(2):
                part = both[head * HEAD : (head + 1) * HEAD]
                inner[pl.ds(head, 1), at] = jnp.sum(part, axis=0, keepdims=True)

        lo = bounds_ref[0]
        hi = bounds_ref[2 * blocks - 1]

        def one(j, carry):
            start = pl.multiple_of(j * BLOCK, BLOCK)
            rows = pl.ds(start, BLOCK)
            key = k_ref[0, rows, :]
            value = v_ref[0, rows, :]
            seg_k = ck_ref[rows, 0:1]
            pad_k = ck_ref[rows, 1:2]
            dk_ref[0, rows, :] = jnp.zeros((BLOCK, 128), BF16)
            dv_ref[0, rows, :] = jnp.zeros((BLOCK, 128), BF16)

            def pair(i, gk, gv):
                at = pl.ds(i * BLOCK, BLOCK)
                query = q_ref[0, at, :]
                grad = g_ref[0, at, :]
                allowed = (seg_k == cq_ref[0:1, at]) | (pad_k == cq_ref[1:2, at])
                for head in range(2):
                    scores = dot_nt(keep_head(key, head), query)
                    scores = jnp.where(allowed, scores, FAR_NEG)
                    probs = jnp.exp(scores - lse_ref[0, 0, pl.ds(head, 1), at])
                    slope = dot_nt(keep_head(value, head), grad)
                    change = (probs * (slope - inner[pl.ds(head, 1), at])).astype(BF16)
                    gv = gv + dot_nn(probs.astype(BF16), keep_head(grad, head))
                    gk = gk + dot_nn(change, keep_head(query, head))
                    part = pl.ds(head * HEAD, HEAD)
                    dqt[part, at] += dot_nn(kt_ref[0, part, rows], change)
                return gk, gv

            gk = jnp.zeros((BLOCK, 128), F32)
            gv = jnp.zeros((BLOCK, 128), F32)
            for i in range(blocks):
                inside = (j >= bounds_ref[2 * i]) & (j < bounds_ref[2 * i + 1])
                gk, gv = lax.cond(
                    inside, functools.partial(pair, i), lambda gk, gv: (gk, gv), gk, gv
                )
            dk_ref[0, rows, :] = gk.astype(BF16)
            dv_ref[0, rows, :] = gv.astype(BF16)
            return carry

        lax.fori_loop(lo, hi, one, 0)
        for i in range(blocks):
            at = pl.ds(i * BLOCK, BLOCK)
            dq_ref[0, at, :] = dqt[:, at].T.astype(BF16) * BF16(0.125)

    block_q = pl.BlockSpec((1, local, 128), lambda a, h, b: (a, 0, h))
    block_k = pl.BlockSpec((1, window, 128), lambda a, h, b: (a, 0, h))
    return pl.pallas_call(
        body,
        out_shape=[
            jax.ShapeDtypeStruct((nz, local, hw), BF16),
            jax.ShapeDtypeStruct((nz, window, hw), BF16),
            jax.ShapeDtypeStruct((nz, window, hw), BF16),
        ],
        grid_spec=pltpu.PrefetchScalarGridSpec(
            num_scalar_prefetch=1,
            grid=(nz, pairs),
            in_specs=[
                block_q,
                block_k,
                pl.BlockSpec((1, 128, window), lambda a, h, b: (a, h, 0)),
                block_k,
                block_q,
                block_q,
                pl.BlockSpec((1, 1, 2, local), lambda a, h, b: (a, h, 0, 0)),
                pl.BlockSpec((2, local), lambda a, h, b: (0, 0)),
                pl.BlockSpec((window, 2), lambda a, h, b: (0, 0)),
            ],
            out_specs=[block_q, block_k, block_k],
            scratch_shapes=[pltpu.VMEM((128, local), F32), pltpu.VMEM((2, local), F32)],
        ),
    )(bounds, queries, keys, keys_t, values, grads, mixed, lse, codes_q, codes_k)


def project_back(window_rows, weights, dq, dk, dv, attn_low, mixed, bounds):
    nz, depth, width = weights.shape
    window = window_rows.shape[0]
    local = dq.shape[1]
    own0 = 2 * local
    hw = width // 4

    def body(
        bounds_ref,
        x_ref,
        w_ref,
        dq_ref,
        dk_ref,
        dv_ref,
        g_ref,
        m_ref,
        dw_ref,
        dx_ref,
        bias_ref,
        acc,
        dkv,
    ):
        a = pl.program_id(0)

        @pl.when(a == 0)
        def _():
            acc[...] = jnp.zeros_like(acc)

        own = pl.ds(own0, local)
        grad_q = dq_ref[0]
        dw_ref[0, :, 0:hw] = dot_tn(x_ref[own, :], grad_q).astype(BF16)
        dw_ref[0, :, 3 * hw :] = dot_tn(g_ref[...], m_ref[0]).astype(BF16)
        acc[own, :] += dot_nt(grad_q, w_ref[0, :, 0:hw])
        bias_q = jnp.sum(grad_q.astype(F32), axis=0, keepdims=True)
        dkv[...] = jnp.zeros_like(dkv)

        def one(j, bias_v):
            start = pl.multiple_of(j * BLOCK, BLOCK)
            rows = pl.ds(start, BLOCK)
            both = jnp.concatenate([dk_ref[0, rows, :], dv_ref[0, rows, :]], axis=1)
            dkv[...] += dot_tn(x_ref[rows, :], both)
            acc[rows, :] += dot_nt(both, w_ref[0, :, hw : 3 * hw])
            return bias_v + jnp.sum(both[:, hw:].astype(F32), axis=0, keepdims=True)

        bias_v = lax.fori_loop(bounds_ref[0], bounds_ref[1], one, jnp.zeros((1, hw), F32))
        dw_ref[0, :, hw : 3 * hw] = dkv[...].astype(BF16)
        bias_ref[0] = jnp.concatenate([bias_q, bias_v], axis=1)

        @pl.when(a == nz - 1)
        def _():
            dx_ref[...] = acc[...].astype(BF16)

    def fixed(shape):
        return pl.BlockSpec(shape, lambda a, b: (0,) * len(shape))

    def by_slot(shape):
        return pl.BlockSpec((1,) + shape, lambda a, b: (a,) + (0,) * len(shape))

    return pl.pallas_call(
        body,
        out_shape=[
            jax.ShapeDtypeStruct((nz, depth, width), BF16),
            jax.ShapeDtypeStruct((window, depth), BF16),
            jax.ShapeDtypeStruct((nz, 1, 2 * hw), F32),
        ],
        grid_spec=pltpu.PrefetchScalarGridSpec(
            num_scalar_prefetch=1,
            grid=(nz,),
            in_specs=[
                fixed((window, depth)),
                by_slot((depth, width)),
                by_slot((local, hw)),
                by_slot((window, hw)),
                by_slot((window, hw)),
                fixed((local, depth)),
                by_slot((local, hw)),
            ],
            out_specs=[by_slot((depth, width)), fixed((window, depth)), by_slot((1, 2 * hw))],
            scratch_shapes=[
                pltpu.VMEM((window, depth), F32),
                pltpu.VMEM((depth, 2 * hw), F32),
            ],
        ),
    )(bounds, window_rows, weights, dq, dk, dv, attn_low, mixed)


def normalize(values, gain_vector, shift_vector):
    centred = values - jnp.mean(values, axis=-1, keepdims=True)
    scaling = lax.rsqrt(jnp.mean(centred * centred, axis=-1, keepdims=True) + 1e-05)
    unit_values = centred * scaling
    return (unit_values * gain_vector + shift_vector, unit_values, scaling)


def normalize_back(grad_values, unit_values, scaling, gain_vector):
    grad_unit = grad_values * gain_vector
    return scaling * (
        grad_unit
        - jnp.mean(grad_unit, axis=-1, keepdims=True)
        - unit_values * jnp.mean(grad_unit * unit_values, axis=-1, keepdims=True)
    )


def gelu_both(values):
    bell = 0.5 * (1.0 + lax.erf(values * 0.7071067811865476))
    slope = bell + values * jnp.exp(-0.5 * values * values) * 0.3989422804014327
    return (values * bell).astype(BF16), slope.astype(BF16)


def on_device(ndp, nz, *arrays):
    (
        tokens,
        segment_ids,
        keep_mask,
        cotangent,
        w_query,
        w_key,
        w_value,
        w_out,
        w_in,
        w_back,
        bias_query,
        bias_value,
        bias_out,
        bias_in,
        bias_back,
        gain_first,
        shift_first,
        gain_second,
        shift_second,
    ) = arrays
    local, depth = tokens.shape
    hw = w_query.shape[1]
    heads_here = hw // HEAD
    hidden_here = w_in.shape[1]
    piece = depth // ndp
    inner = bias_query.shape[1]
    z = lax.axis_index("tensor")

    small = jnp.concatenate(
        [
            bias_query.reshape(-1),
            bias_value.reshape(-1),
            bias_in.reshape(-1),
            bias_out,
            bias_back,
            gain_first,
            shift_first,
            gain_second,
            shift_second,
        ]
    )
    small = jnp.pad(small, (0, 2048 - small.shape[0])).reshape(16, 128)
    message_a = jnp.concatenate([w_query, w_key, w_value, w_out.T], axis=1)
    (full_a, full_i, full_b, every), window_rows = gather_all(
        [message_a, w_in, w_back.T, small], tokens, ndp, nz
    )
    full_a = full_a.reshape(nz, depth, -1)
    full_i = full_i.reshape(nz, depth, -1)
    full_b = full_b.reshape(nz, depth, -1)
    every = every.reshape(nz, ndp, 2048).astype(F32)
    n_q = heads_here * inner
    n_in = bias_in.shape[0] * inner

    def rows_of_heads(part):
        part = part.reshape(nz, ndp, -1, inner).transpose(0, 2, 1, 3)
        return part.reshape(nz, -1)

    bias_q = rows_of_heads(every[:, :, :n_q])
    bias_v = rows_of_heads(every[:, :, n_q : 2 * n_q])
    bias_h = rows_of_heads(every[:, :, 2 * n_q : 2 * n_q + n_in])
    n_v = 2 * n_q + n_in
    vectors = every[0, :, n_v : n_v + 6 * piece]
    vectors = vectors.reshape(ndp, 6, piece).transpose(1, 0, 2).reshape(6, depth)
    b_out, b_back, g_first, s_first, g_second, s_second = [vectors[i] for i in range(6)]
    bias_qv = jnp.concatenate([bias_q, bias_v], axis=1).reshape(nz, 1, 2 * hw)

    length = segment_ids.shape[1]
    window = 5 * local
    own0 = 2 * local
    seg_pad = jnp.pad(segment_ids[0], (own0, own0), constant_values=-1)
    keep_pad = jnp.pad(keep_mask[0], (own0, own0), constant_values=1)
    seg_win = lax.dynamic_slice(seg_pad, (z * local,), (window,))
    keep_win = lax.dynamic_slice(keep_pad, (z * local,), (window,))
    place = jnp.arange(window, dtype=jnp.int32)
    seg_k = jnp.where(keep_win == 1, seg_win, -7)
    pad_k = jnp.where(keep_win == 1, -1, place)
    codes_k = jnp.stack([seg_k, pad_k], axis=1)
    seg_q = seg_win[own0 : own0 + local]
    keep_q = keep_win[own0 : own0 + local]
    pad_q = jnp.where(keep_q == 1, -2, place[own0 : own0 + local])
    codes_q = jnp.stack([seg_q, pad_q], axis=0)
    blocks = local // BLOCK
    first = seg_q.reshape(blocks, BLOCK)[:, 0]
    last = seg_q.reshape(blocks, BLOCK)[:, -1]
    inside = (seg_win >= 0)[None, :]
    before = jnp.sum((seg_win[None, :] < first[:, None]), axis=1, dtype=jnp.int32)
    outside_after = jnp.sum(
        (seg_win[None, :] <= last[:, None]) & inside, axis=1, dtype=jnp.int32
    )
    lead = jnp.maximum(own0 - z * local, 0)
    trail = jnp.maximum(z * local + window - own0 - length, 0)
    low = (before - trail) // BLOCK
    high = (outside_after + lead + BLOCK - 1) // BLOCK
    bounds = jnp.stack([low, high], axis=1).reshape(-1).astype(jnp.int32)
    whole = jnp.stack([bounds[0], bounds[2 * blocks - 1]])
    keep_local = keep_q.astype(F32)[:, None]

    queries, keys, values, keys_t, values_t = project(
        window_rows, full_a, bias_qv, whole, local
    )
    mixed, lse = attend(queries, keys, values_t, codes_q, codes_k, bounds)
    out_t = full_a[:, :, 3 * hw :]
    attended = sum(dot_nt(mixed[a], out_t[a]) for a in range(nz))
    residual = tokens.astype(F32) + attended + b_out
    normed, unit_first, scale_first = normalize(residual, g_first, s_first)
    normed_low = normed.astype(BF16)
    activated, slopes = [], []
    second = normed + b_back
    for a in range(nz):
        act, slope = gelu_both(dot_nn(normed_low, full_i[a]) + bias_h[a])
        activated.append(act)
        slopes.append(slope)
        second = second + dot_nt(act, full_b[a])
    finished, unit_second, scale_second = normalize(second, g_second, s_second)
    output = (finished * keep_local).astype(BF16)

    grad_out = cotangent.astype(F32) * keep_local
    d_gain_second = jnp.sum(grad_out * unit_second, axis=0)
    d_shift_second = jnp.sum(grad_out, axis=0)
    grad_second = normalize_back(grad_out, unit_second, scale_second, g_second)
    back_low = grad_second.astype(BF16)
    d_bias_back = jnp.sum(back_low.astype(F32), axis=0)
    d_back = jnp.stack([dot_tn(back_low, activated[a]).astype(BF16) for a in range(nz)])
    grad_normed = grad_second
    d_in, d_bias_in = [], []
    for a in range(nz):
        pre = (dot_nn(back_low, full_b[a]) * slopes[a].astype(F32)).astype(BF16)
        d_bias_in.append(jnp.sum(pre.astype(F32), axis=0))
        d_in.append(dot_tn(normed_low, pre).astype(BF16))
        grad_normed = grad_normed + dot_nt(pre, full_i[a])
    d_gain_first = jnp.sum(grad_normed * unit_first, axis=0)
    d_shift_first = jnp.sum(grad_normed, axis=0)
    grad_residual = normalize_back(grad_normed, unit_first, scale_first, g_first)
    attn_low = grad_residual.astype(BF16)
    d_bias_out = jnp.sum(attn_low.astype(F32), axis=0)
    grad_mixed = jnp.stack([dot_nn(attn_low, out_t[a]).astype(BF16) for a in range(nz)])
    dq, dk, dv = attend_back(
        queries, keys, keys_t, values, grad_mixed, mixed, lse, codes_q, codes_k, bounds
    )
    d_a, dx, d_bias_qv = project_back(
        window_rows, full_a, dq, dk, dv, attn_low, mixed, whole
    )
    def by_device(part):
        part = part.reshape(nz, -1, ndp, inner).transpose(0, 2, 1, 3)
        return part.reshape(nz, ndp, -1)

    stacked = jnp.stack(
        [d_bias_out, d_bias_back, d_gain_first, d_shift_first, d_gain_second, d_shift_second]
    )
    stacked = stacked.reshape(6, ndp, piece).transpose(1, 0, 2).reshape(1, ndp, 6 * piece)
    d_small = jnp.concatenate(
        [
            by_device(d_bias_qv[:, 0, :hw]),
            by_device(d_bias_qv[:, 0, hw:]),
            by_device(jnp.stack(d_bias_in)),
            jnp.broadcast_to(stacked, (nz, ndp, 6 * piece)),
        ],
        axis=2,
    )
    d_small = jnp.pad(d_small, ((0, 0), (0, 0), (0, 2048 - d_small.shape[2])))

    def blocks_of(values):
        return values.reshape(nz, ndp, piece, values.shape[2])

    (shard_a, shard_i, shard_b, sums), grad_tokens = sum_all(
        [
            blocks_of(d_a),
            blocks_of(jnp.stack(d_in)),
            blocks_of(d_back),
            d_small.reshape(nz, ndp, 16, 128),
        ],
        dx,
        grad_residual,
        ndp,
        nz,
    )
    sums = sums.reshape(2048)
    d_bias_q = sums[:n_q].reshape(heads_here, inner)
    d_bias_v = sums[n_q : 2 * n_q].reshape(heads_here, inner)
    d_bias_h = sums[2 * n_q : n_v].reshape(-1, inner)
    vector_sums = sums[n_v : n_v + 6 * piece].reshape(6, piece)
    return (
        output,
        grad_tokens,
        shard_a[:, :hw],
        shard_a[:, hw : 2 * hw],
        shard_a[:, 2 * hw : 3 * hw],
        shard_a[:, 3 * hw :].T,
        shard_i,
        shard_b.T,
        d_bias_q,
        d_bias_v,
        vector_sums[0],
        d_bias_h,
        vector_sums[1],
        vector_sums[2],
        vector_sums[3],
        vector_sums[4],
        vector_sums[5],
    )


def solution(mesh):
    ndp, nz = mesh.shape["dp"], mesh.shape["tensor"]
    return jax.shard_map(
        functools.partial(on_device, ndp, nz),
        mesh=mesh,
        in_specs=(
            P(("dp", "tensor"), None),
            P("dp", None),
            P("dp", None),
            P(("dp", "tensor"), None),
            P("dp", "tensor"),
            P("dp", "tensor"),
            P("dp", "tensor"),
            P("tensor", "dp"),
            P("dp", "tensor"),
            P("tensor", "dp"),
            P("tensor", "dp"),
            P("tensor", "dp"),
            P("dp"),
            P("tensor", "dp"),
            P("dp"),
            P("dp"),
            P("dp"),
            P("dp"),
            P("dp"),
        ),
        out_specs=(
            P(("dp", "tensor"), None),
            P(("dp", "tensor"), None),
            P("dp", "tensor"),
            P("dp", "tensor"),
            P("dp", "tensor"),
            P("tensor", "dp"),
            P("dp", "tensor"),
            P("tensor", "dp"),
            P("tensor", "dp"),
            P("tensor", "dp"),
            P("dp"),
            P("tensor", "dp"),
            P("dp"),
            P("dp"),
            P("dp"),
            P("dp"),
            P("dp"),
        ),
        check_vma=False,
    )
```

```python
import functools

import jax
import jax.numpy as jnp
from jax import lax
from jax.experimental import pallas as pl
from jax.experimental.pallas import tpu as pltpu
from jax.sharding import PartitionSpec as P

HEAD = 64
DOC_MOST = 800
BLOCK = 256
GATHER_LAG = 3
SUM_LAG = 3
HALO_AT = 1.5
RELAY_AT = 3
MESH = pl.DeviceIdType.MESH
BF16 = jnp.bfloat16
F32 = jnp.float32
FAR_NEG = -1e30


def dot_nn(left, right):
    return lax.dot_general(left, right, (((1,), (0,)), ((), ())), preferred_element_type=F32)


def dot_nt(left, right):
    return lax.dot_general(left, right, (((1,), (1,)), ((), ())), preferred_element_type=F32)


def dot_tn(left, right):
    return lax.dot_general(left, right, (((0,), (0,)), ((), ())), preferred_element_type=F32)


def bits_of(count):
    found, bit = [], 1
    while bit < count:
        found.append(bit)
        bit *= 2
    return found


def far_rows(local):
    return -(-(DOC_MOST - 1 - local) // 16) * 16


def bit_at(value, bit):
    return lax.rem(value // bit, 2)


def gather_all(messages, tokens, ndp, nz):
    count = len(messages)
    local, depth = tokens.shape
    far = far_rows(local)
    window = 5 * local
    own0, l1, r1 = 2 * local, local, 3 * local
    l2, r2 = 2 * local - local - far, 4 * local
    zbits = bits_of(nz)[::-1]
    dbits = bits_of(ndp)[::-1]
    xy = dbits[:-1]
    pairs = []
    for c in range(2):
        for m in range(count):
            rows = messages[m].shape[0]
            chunks = 2 if rows % 32 == 0 else 1
            if c < chunks:
                pairs.append((m, c, rows // chunks))
    zorder, parent = [0], {}
    for bit in zbits:
        for q in list(zorder):
            parent[q ^ bit] = (q, bit)
            zorder.append(q ^ bit)
    stages = len(dbits)
    total = len(pairs) * (nz - 1) + len(pairs) * nz * stages
    lags = [GATHER_LAG * s for s in range(stages)]

    def kernel(*refs):
        ins, tok = refs[:count], refs[count]
        outs, win = refs[count + 1 : 2 * count + 1], refs[2 * count + 1]
        zeros, ssem, rsem, lsem, hs, hr = refs[2 * count + 2 :]
        d = lax.axis_index("dp")
        z = lax.axis_index("tensor")
        barrier = pltpu.get_barrier_semaphore()
        for step in range(1, nz):
            pl.semaphore_signal(
                barrier, inc=1, device_id=(d, lax.rem(z + step, nz)), device_id_type=MESH
            )
        for bit in dbits:
            pl.semaphore_signal(barrier, inc=1, device_id=(d ^ bit, z), device_id_type=MESH)

        own = tuple(bit_at(d, bit) for bit in dbits)
        locals_ = []

        def local_copy(src, dst):
            cp = pltpu.make_async_copy(src, dst, lsem.at[len(locals_)])
            locals_.append(cp)
            return cp

        for m in range(count):
            local_copy(ins[m], outs[m].at[(z,) + own]).start()
        local_copy(tok, win.at[pl.ds(own0, local)]).start()
        zeros[...] = jnp.zeros_like(zeros)
        edge = local - far
        if edge:
            local_copy(zeros.at[pl.ds(0, edge)], win.at[pl.ds(0, edge)]).start()
            local_copy(zeros.at[pl.ds(0, edge)], win.at[pl.ds(window - edge, edge)]).start()
        fills = [
            (z < 1, local_copy(zeros, win.at[pl.ds(l1, local)])),
            (z < 2, local_copy(zeros.at[pl.ds(0, far)], win.at[pl.ds(l2, far)])),
            (z > nz - 2, local_copy(zeros, win.at[pl.ds(r1, local)])),
            (z > nz - 3, local_copy(zeros.at[pl.ds(0, far)], win.at[pl.ds(r2, far)])),
        ]
        fixed = locals_[:-4]
        for when, cp in fills:
            pl.when(when)(cp.start)

        pl.semaphore_wait(barrier, nz - 1 + len(dbits))

        def halo_copy(src, dst, target, index):
            return pltpu.make_async_remote_copy(
                src_ref=src,
                dst_ref=dst,
                send_sem=hs.at[index],
                recv_sem=hr.at[index],
                device_id=(d, target),
                device_id_type=MESH,
            )

        up, down = lax.rem(z + 1, nz), lax.rem(z + nz - 1, nz)
        to_up = halo_copy(tok, win.at[pl.ds(l1, local)], up, 0)
        to_down = halo_copy(tok, win.at[pl.ds(r1, local)], down, 1)
        far_up = halo_copy(
            win.at[pl.ds(l1 + local - far, far)], win.at[pl.ds(l2, far)], up, 2
        )
        far_down = halo_copy(win.at[pl.ds(r1, far)], win.at[pl.ds(r2, far)], down, 3)

        counter, every = [0], []

        def remote(ref, index, device, src=None):
            number = counter[0]
            counter[0] += 1
            cp = pltpu.make_async_remote_copy(
                src_ref=ref.at[index] if src is None else src,
                dst_ref=ref.at[index],
                send_sem=ssem.at[number],
                recv_sem=rsem.at[number],
                device_id=device,
                device_id_type=MESH,
            )
            every.append(cp)
            return cp

        zcopies = {}
        for q, (par, bit) in parent.items():
            for m, c, piece in pairs:
                part = pl.ds(c * piece, piece)
                src = ins[m].at[part] if par == 0 else None
                zcopies[m, c, q] = remote(outs[m], (z ^ par,) + own + (part,), (d, z ^ bit), src)
        items = [(m, c, piece, a) for a in zorder for (m, c, piece) in pairs]
        plan = []
        for i, (m, c, piece, a) in enumerate(items):
            mine, held = [], list(own)
            part = pl.ds(c * piece, piece)
            for bit in (xy if i % 2 == 0 else xy[::-1]) + [1]:
                src = ins[m].at[part] if a == 0 and not mine else None
                index = (z ^ a,) + tuple(held) + (part,)
                mine.append(remote(outs[m], index, (d ^ bit, z), src))
                held[dbits.index(bit)] = slice(None)
            plan.append(mine)

        for m, c, _ in pairs:
            for q, (par, _) in parent.items():
                if par == 0:
                    zcopies[m, c, q].start()
        for cp in fixed:
            cp.wait()
        for when, cp in fills:
            pl.when(when)(cp.wait)
        for t in range(len(items) + lags[-1]):
            if t == int(HALO_AT * len(pairs)):
                pl.when(z < nz - 1)(to_up.start)
                pl.when(z > 0)(to_down.start)
            if t == int(RELAY_AT * len(pairs)):
                pl.when(z > 0)(to_up.wait_recv)
                pl.when((z > 0) & (z < nz - 1))(far_up.start)
                pl.when(z < nz - 1)(to_down.wait_recv)
                pl.when((z > 0) & (z < nz - 1))(far_down.start)
            for s in range(stages):
                i = t - lags[s]
                if not 0 <= i < len(items):
                    continue
                m, c, _, a = items[i]
                if s == 0:
                    if a:
                        zcopies[m, c, a].wait_recv()
                        for q, (par, _) in parent.items():
                            if par == a:
                                zcopies[m, c, q].start()
                else:
                    plan[i][s - 1].wait_recv()
                plan[i][s].start()
        for mine in plan:
            mine[-1].wait_recv()
        pl.when(z > 1)(far_up.wait_recv)
        pl.when(z < nz - 2)(far_down.wait_recv)
        for cp in every:
            cp.wait_send()
        pl.when(z < nz - 1)(to_up.wait_send)
        pl.when(z > 0)(to_down.wait_send)
        pl.when((z > 0) & (z < nz - 1))(far_up.wait_send)
        pl.when((z > 0) & (z < nz - 1))(far_down.wait_send)

    any_spec = pl.BlockSpec(memory_space=pl.ANY)
    split = (2,) * len(dbits)
    outs = pl.pallas_call(
        kernel,
        out_shape=[jax.ShapeDtypeStruct((nz,) + split + m.shape, BF16) for m in messages]
        + [jax.ShapeDtypeStruct((window, depth), BF16)],
        in_specs=[pl.BlockSpec(memory_space=pltpu.VMEM)] * (count + 1),
        out_specs=[any_spec] * (count + 1),
        scratch_shapes=[
            pltpu.VMEM((local, depth), BF16),
            pltpu.SemaphoreType.DMA((total,)),
            pltpu.SemaphoreType.DMA((total,)),
            pltpu.SemaphoreType.DMA((count + 7,)),
            pltpu.SemaphoreType.DMA((4,)),
            pltpu.SemaphoreType.DMA((4,)),
        ],
        compiler_params=pltpu.CompilerParams(collective_id=0, has_side_effects=True),
    )(*messages, tokens)
    return outs[:count], outs[count]


def sum_all(partials, dx, residual_grad, ndp, nz):
    count = len(partials)
    local, depth = residual_grad.shape
    far = far_rows(local)
    own0, l1, r1 = 2 * local, local, 3 * local
    l2, r2 = local - far, 4 * local
    zbits = bits_of(nz)
    dbits = bits_of(ndp)[::-1]
    xy = dbits[:-1]
    nxy = len(xy)
    stages = len(dbits)
    pairs = []
    for c in range(2):
        for m in range(count):
            rows = partials[m].shape[2]
            chunks = 2 if rows % 32 == 0 else 1
            if c < chunks:
                pairs.append((m, c, rows // chunks))
    zsteps = []
    live = list(range(nz))
    for bit in zbits:
        zsteps.append((bit, [q for q in live if q & bit]))
        live = [q for q in live if not q & bit]
    zorder = [q for _, sent in zsteps for q in sent] + [0]
    items = [(m, c, piece, a) for a in zorder for (m, c, piece) in pairs]
    total = len(items) * stages + len(pairs) * (nz - 1)
    lag = SUM_LAG
    shapes = [(p.shape[2], p.shape[3], p.dtype) for p in partials]

    def kernel(*refs):
        ins, dxr, res = refs[:count], refs[count], refs[count + 1]
        k = count + 2
        outs, tok = refs[k : k + count], refs[k + count]
        k += count + 1
        acc = refs[k : k + count]
        k += count
        got = [refs[k + s * count : k + (s + 1) * count] for s in range(stages)]
        k += stages * count
        zgot = refs[k : k + count]
        k += count
        hin, hbuf, hnear, ssem, rsem, lsem, hl, hs, hr = refs[k:]
        d = lax.axis_index("dp")
        z = lax.axis_index("tensor")
        barrier = pltpu.get_barrier_semaphore()
        for step in range(1, nz):
            pl.semaphore_signal(
                barrier, inc=1, device_id=(d, lax.rem(z + step, nz)), device_id_type=MESH
            )
        for bit in dbits:
            pl.semaphore_signal(barrier, inc=1, device_id=(d ^ bit, z), device_id_type=MESH)
        own = [bit_at(d, bit) for bit in dbits]
        core = own[-1]

        def remote(src, dst, number, device, send=ssem, recv=rsem):
            return pltpu.make_async_remote_copy(
                src_ref=src,
                dst_ref=dst,
                send_sem=send.at[number],
                recv_sem=recv.at[number],
                device_id=device,
                device_id_type=MESH,
            )

        everything = (slice(None),) * nxy
        plan, loads = [], []
        for i, (m, c, piece, a) in enumerate(items):
            part = pl.ds(c * piece, piece)
            za = z ^ a
            loads.append(
                pltpu.make_async_copy(
                    ins[m].at[(za,) + everything + (core, part)],
                    acc[m].at[(a,) + everything + (part,)],
                    lsem.at[i],
                )
            )
            steps = []
            order = xy if i % 2 == 0 else xy[::-1]
            first = remote(
                ins[m].at[(za,) + everything + (1 - core, part)],
                got[0][m].at[(a,) + everything + (part,)],
                i * stages,
                (d ^ 1, z),
            )
            steps.append((first, None, everything))
            where = list(everything)
            for s, bit in enumerate(order):
                at = xy.index(bit)
                send, keep = list(where), list(where)
                send[at] = 1 - own[at]
                keep[at] = own[at]
                live_count = nxy - 1 - s
                steps.append(
                    (
                        remote(
                            acc[m].at[(a,) + tuple(send) + (part,)],
                            got[s + 1][m].at[(a,) + (slice(None),) * live_count + (part,)],
                            i * stages + s + 1,
                            (d ^ bit, z),
                        ),
                        tuple(where),
                        tuple(keep),
                    )
                )
                where = keep
            plan.append(steps)

        base = len(items) * stages
        zplan = {}
        number = base
        mine = tuple(own[:-1])
        for pi, (m, c, piece) in enumerate(pairs):
            part = pl.ds(c * piece, piece)
            for bit, sent in zsteps:
                for q in sent:
                    zplan[m, c, q] = remote(
                        acc[m].at[(q,) + mine + (part,)],
                        zgot[m].at[q, part],
                        number,
                        (d, z ^ bit),
                    )
                    number += 1

        up, down = lax.rem(z + 1, nz), lax.rem(z + nz - 1, nz)
        own_load = pltpu.make_async_copy(dxr.at[pl.ds(own0, local)], hin.at[0], hl.at[0])
        left_load = pltpu.make_async_copy(dxr.at[pl.ds(l1, local)], hin.at[1], hl.at[1])
        right_load = pltpu.make_async_copy(dxr.at[pl.ds(r1, local)], hin.at[2], hl.at[2])
        far_down = remote(dxr.at[pl.ds(l2, far)], hbuf.at[0], 0, (d, down), hs, hr)
        far_up = remote(dxr.at[pl.ds(r2, far)], hbuf.at[1], 1, (d, up), hs, hr)
        near_down = remote(hin.at[1], hnear.at[0], 2, (d, down), hs, hr)
        near_up = remote(hin.at[2], hnear.at[1], 3, (d, up), hs, hr)
        for cp in (own_load, left_load, right_load):
            cp.start()
        pl.semaphore_wait(barrier, nz - 1 + len(dbits))
        pl.when(z > 1)(far_down.start)
        pl.when(z < nz - 2)(far_up.start)
        for i in range(len(items)):
            plan[i][0][0].start()
            loads[i].start()

        def halo_one():
            left_load.wait()
            right_load.wait()

            @pl.when((z > 0) & (z < nz - 1))
            def _():
                far_down.wait_recv()
                hin[1, pl.ds(local - far, far), :] += hbuf[0]
                far_up.wait_recv()
                hin[2, pl.ds(0, far), :] += hbuf[1]

            pl.when(z > 0)(near_down.start)
            pl.when(z < nz - 1)(near_up.start)

        def add(target, tindex, source, sindex, start, piece):
            step = min(piece, 32)

            def one(j, carry):
                rows = pl.ds(pl.multiple_of(start + j * step, step), step)
                at = tindex + (rows,)
                target[at] = target[at] + source[sindex + (rows,)]
                return carry

            lax.fori_loop(0, piece // step, one, 0)

        def combos(bits_count):
            result = [()]
            for _ in range(bits_count):
                result = [r + (v,) for r in result for v in (0, 1)]
            return result

        def absorb(i, s):
            m, c, piece, a = items[i]
            plan[i][s][0].wait_recv()
            if s == 0:
                loads[i].wait()
            keep = plan[i][s][2]
            free = [k for k in range(nxy) if isinstance(keep[k], slice)]
            for combo in combos(len(free)):
                index = list(keep)
                for k, v in zip(free, combo):
                    index[k] = v
                add(acc[m], (a,) + tuple(index), got[s][m], (a,) + combo, c * piece, piece)

        def zabsorb(m, c, piece, q):
            bit = next(b for b, sent in zsteps if q in sent)
            zplan[m, c, q].wait_recv()
            add(acc[m], (q ^ bit,) + mine, zgot[m], (q,), c * piece, piece)

        for t in range(len(items) + lag * stages):
            if t == 4:
                halo_one()
            for s in range(stages):
                i = t - lag * s
                if not 0 <= i < len(items):
                    continue
                absorb(i, s)
                if s + 1 < stages:
                    plan[i][s + 1][0].start()
                else:
                    m, c, piece, a = items[i]
                    for bit, sent in zsteps:
                        if (a ^ bit) in sent and not a & bit:
                            if bit < (a & -a if a else nz):
                                zabsorb(m, c, piece, a ^ bit)
                    if a:
                        zplan[m, c, a].start()
        for m, c, piece in pairs:
            part = pl.ds(c * piece, piece)
            outs[m][part, :] = acc[m][(0,) + mine + (part,)].astype(F32)
        own_load.wait()

        @pl.when(z < nz - 1)
        def _():
            near_down.wait_recv()

        @pl.when(z > 0)
        def _():
            near_up.wait_recv()

        step = 64

        def finish(j, carry):
            rows = pl.ds(pl.multiple_of(j * step, step), step)
            value = res[rows, :] + hin[0, rows, :].astype(F32)
            value = value + jnp.where(z < nz - 1, hnear[0, rows, :].astype(F32), 0.0)
            value = value + jnp.where(z > 0, hnear[1, rows, :].astype(F32), 0.0)
            tok[rows, :] = value.astype(BF16)
            return carry

        lax.fori_loop(0, local // step, finish, 0)
        for steps in plan:
            for cp, _, _ in steps:
                cp.wait_send()
        for cp in zplan.values():
            cp.wait_send()
        pl.when(z > 1)(far_down.wait_send)
        pl.when(z < nz - 2)(far_up.wait_send)
        pl.when(z > 0)(near_down.wait_send)
        pl.when(z < nz - 1)(near_up.wait_send)

    any_spec = pl.BlockSpec(memory_space=pl.ANY)
    vmem_spec = pl.BlockSpec(memory_space=pltpu.VMEM)
    split = (2,) * len(dbits)
    scratch = [pltpu.VMEM((nz,) + (2,) * nxy + s[:2], s[2]) for s in shapes]
    for stage in range(stages):
        left = nxy if stage == 0 else nxy - stage
        scratch += [pltpu.VMEM((nz,) + (2,) * left + s[:2], s[2]) for s in shapes]
    scratch += [pltpu.VMEM((nz,) + s[:2], s[2]) for s in shapes]
    scratch += [
        pltpu.VMEM((3, local, depth), BF16),
        pltpu.VMEM((2, far, depth), BF16),
        pltpu.VMEM((2, local, depth), BF16),
        pltpu.SemaphoreType.DMA((total,)),
        pltpu.SemaphoreType.DMA((total,)),
        pltpu.SemaphoreType.DMA((len(items),)),
        pltpu.SemaphoreType.DMA((3,)),
        pltpu.SemaphoreType.DMA((4,)),
        pltpu.SemaphoreType.DMA((4,)),
    ]
    result = pl.pallas_call(
        kernel,
        out_shape=[jax.ShapeDtypeStruct(s[:2], F32) for s in shapes]
        + [jax.ShapeDtypeStruct((local, depth), BF16)],
        in_specs=[any_spec] * (count + 1) + [vmem_spec],
        out_specs=[vmem_spec] * (count + 1),
        scratch_shapes=scratch,
        compiler_params=pltpu.CompilerParams(
            collective_id=1, has_side_effects=True, vmem_limit_bytes=63 * 1024 * 1024
        ),
    )(*[p.reshape((nz,) + split + p.shape[2:]) for p in partials], dx, residual_grad)
    return result[:count], result[count]


def project(window_rows, weights, biases, bounds, local):
    nz, depth, _ = weights.shape
    window = window_rows.shape[0]
    own0 = 2 * local
    heads_width = weights.shape[2] // 4

    def body(bounds_ref, x_ref, w_ref, b_ref, q_ref, k_ref, v_ref, kt_ref, vt_ref):
        hw = heads_width
        bias = b_ref[0]
        wq = w_ref[0, :, 0:hw]
        for i in range(local // BLOCK):
            rows = x_ref[pl.ds(own0 + i * BLOCK, BLOCK), :]
            q_ref[0, pl.ds(i * BLOCK, BLOCK), :] = (
                (dot_nn(rows, wq) + bias[:, 0:hw]) * 0.125
            ).astype(BF16)

        def one(j, carry):
            start = pl.multiple_of(j * BLOCK, BLOCK)
            rows = x_ref[pl.ds(start, BLOCK), :]
            kv = dot_nn(rows, w_ref[0, :, hw : 3 * hw])
            key = kv[:, :hw].astype(BF16)
            value = (kv[:, hw:] + bias[:, hw:]).astype(BF16)
            k_ref[0, pl.ds(start, BLOCK), :] = key
            v_ref[0, pl.ds(start, BLOCK), :] = value
            kt_ref[0, :, pl.ds(start, BLOCK)] = key.T
            vt_ref[0, :, pl.ds(start, BLOCK)] = value.T
            return carry

        lax.fori_loop(bounds_ref[0], bounds_ref[1], one, 0)

    hw = heads_width
    return pl.pallas_call(
        body,
        out_shape=[
            jax.ShapeDtypeStruct((nz, local, hw), BF16),
            jax.ShapeDtypeStruct((nz, window, hw), BF16),
            jax.ShapeDtypeStruct((nz, window, hw), BF16),
            jax.ShapeDtypeStruct((nz, hw, window), BF16),
            jax.ShapeDtypeStruct((nz, hw, window), BF16),
        ],
        grid_spec=pltpu.PrefetchScalarGridSpec(
            num_scalar_prefetch=1,
            grid=(nz,),
            in_specs=[
                pl.BlockSpec((window, depth), lambda a, b: (0, 0)),
                pl.BlockSpec((1, depth, 4 * hw), lambda a, b: (a, 0, 0)),
                pl.BlockSpec((1, 1, 2 * hw), lambda a, b: (a, 0, 0)),
            ],
            out_specs=[
                pl.BlockSpec((1, local, hw), lambda a, b: (a, 0, 0)),
                pl.BlockSpec((1, window, hw), lambda a, b: (a, 0, 0)),
                pl.BlockSpec((1, window, hw), lambda a, b: (a, 0, 0)),
                pl.BlockSpec((1, hw, window), lambda a, b: (a, 0, 0)),
                pl.BlockSpec((1, hw, window), lambda a, b: (a, 0, 0)),
            ],
        ),
    )(bounds, window_rows, weights, biases)


def only_head(values, head):
    lane = lax.broadcasted_iota(jnp.int32, values.shape, 1)
    return jnp.where(lane // HEAD == head, values, jnp.zeros_like(values))


def pair_lanes(head):
    return slice(128 * (head // 2), 128 * (head // 2) + 128)


def fill_bias(bounds_ref, cq_ref, ck_ref, bias, blocks):
    for i in range(blocks):
        at = pl.ds(i * BLOCK, BLOCK)

        def fill(j, carry):
            rows = pl.ds(pl.multiple_of(j * BLOCK, BLOCK), BLOCK)
            allowed = (ck_ref[rows, 0:1] == cq_ref[0:1, at]) | (
                ck_ref[rows, 1:2] == cq_ref[1:2, at]
            )
            bias[rows, at] = jnp.where(allowed, 0.0, FAR_NEG)
            return carry

        lax.fori_loop(bounds_ref[2 * i], bounds_ref[2 * i + 1], fill, 0)


def attend(queries, keys, values_t, codes_q, codes_k, bounds):
    nz, local, hw = queries.shape
    window = keys.shape[1]
    heads = hw // HEAD
    blocks = local // BLOCK

    def body(
        bounds_ref, q_ref, k_ref, vt_ref, cq_ref, ck_ref, out_ref, lse_ref, bias, masked, held
    ):
        @pl.when(pl.program_id(0) == 0)
        def _():
            fill_bias(bounds_ref, cq_ref, ck_ref, bias, blocks)

        for i in range(blocks):
            at = pl.ds(i * BLOCK, BLOCK)
            for h in range(heads):
                masked[h] = only_head(q_ref[0, at, pair_lanes(h)], h % 2)

            def first(j, carry):
                rows = pl.ds(pl.multiple_of(j * BLOCK, BLOCK), BLOCK)
                result = []
                for h in range(heads):
                    key = k_ref[0, rows, pair_lanes(h)]
                    scores = dot_nt(key, masked[h]) + bias[rows, at]
                    held[h, rows, :] = scores
                    part = jnp.max(scores.reshape(BLOCK // 8, 8, BLOCK), axis=0)
                    result.append(jnp.maximum(carry[h], part))
                return tuple(result)

            low, high = bounds_ref[2 * i], bounds_ref[2 * i + 1]
            tops = lax.fori_loop(
                low, high, first, (jnp.full((8, BLOCK), FAR_NEG, F32),) * heads
            )
            tops = [jnp.max(top, axis=0, keepdims=True) for top in tops]

            def second(j, carry):
                rows = pl.ds(pl.multiple_of(j * BLOCK, BLOCK), BLOCK)
                result = []
                for h in range(heads):
                    total, acc = carry[h]
                    weights = jnp.exp(held[h, rows, :] - tops[h])
                    total = total + jnp.sum(weights.reshape(BLOCK // 8, 8, BLOCK), axis=0)
                    value = vt_ref[0, pl.ds(h * HEAD, HEAD), rows]
                    acc = acc + dot_nn(value, weights.astype(BF16))
                    result.append((total, acc))
                return tuple(result)

            fresh = (jnp.zeros((8, BLOCK), F32), jnp.zeros((HEAD, BLOCK), F32))
            done = lax.fori_loop(low, high, second, (fresh,) * heads)
            totals = [jnp.sum(total, axis=0, keepdims=True) for total, _ in done]
            mixed = jnp.concatenate([done[h][1] / totals[h] for h in range(heads)], axis=0)
            out_ref[0, at, :] = mixed.T.astype(BF16)
            for h in range(heads):
                lse_ref[0, pl.ds(h, 1), at] = tops[h] + jnp.log(totals[h])

    def by_slot(shape):
        return pl.BlockSpec((1,) + shape, lambda a, b: (a, 0, 0))

    return pl.pallas_call(
        body,
        out_shape=[
            jax.ShapeDtypeStruct((nz, local, hw), BF16),
            jax.ShapeDtypeStruct((nz, heads, local), F32),
        ],
        grid_spec=pltpu.PrefetchScalarGridSpec(
            num_scalar_prefetch=1,
            grid=(nz,),
            in_specs=[
                by_slot((local, hw)),
                by_slot((window, hw)),
                by_slot((hw, window)),
                pl.BlockSpec((2, local), lambda a, b: (0, 0)),
                pl.BlockSpec((window, 2), lambda a, b: (0, 0)),
            ],
            out_specs=[by_slot((local, hw)), by_slot((heads, local))],
            scratch_shapes=[
                pltpu.VMEM((window, local), F32),
                pltpu.VMEM((heads, BLOCK, 128), BF16),
                pltpu.VMEM((heads, window, BLOCK), F32),
            ],
        ),
    )(bounds, queries, keys, values_t, codes_q, codes_k)


def attend_back(queries, keys, keys_t, values, grads, mixed, lse, codes_q, codes_k, bounds):
    nz, local, hw = queries.shape
    window = keys.shape[1]
    pairs = hw // 128
    blocks = local // BLOCK

    def body(
        bounds_ref,
        q_ref,
        k_ref,
        kt_ref,
        v_ref,
        g_ref,
        m_ref,
        lse_ref,
        cq_ref,
        ck_ref,
        dq_ref,
        dk_ref,
        dv_ref,
        bias,
        masked_q,
        masked_g,
        dqt,
        inner,
        dk_acc,
        dv_acc,
    ):
        @pl.when((pl.program_id(0) == 0) & (pl.program_id(1) == 0))
        def _():
            fill_bias(bounds_ref, cq_ref, ck_ref, bias, blocks)

        dqt[...] = jnp.zeros_like(dqt)
        for i in range(blocks):
            at = pl.ds(i * BLOCK, BLOCK)
            query = q_ref[0, at, :]
            grad = g_ref[0, at, :]
            both = (grad.astype(F32) * m_ref[0, at, :].astype(F32)).T
            for h in range(2):
                masked_q[h, at, :] = only_head(query, h)
                masked_g[h, at, :] = only_head(grad, h)
                part = both[h * HEAD : (h + 1) * HEAD]
                inner[pl.ds(h, 1), at] = jnp.sum(part, axis=0, keepdims=True)

        def unit(i, rows):
            at = pl.ds(i * BLOCK, BLOCK)
            key = k_ref[0, rows, :]
            value = v_ref[0, rows, :]
            scores = [dot_nt(key, masked_q[h, at, :]) for h in range(2)]
            slopes = [dot_nt(value, masked_g[h, at, :]) for h in range(2)]
            lows, changes = [], []
            for h in range(2):
                probs = jnp.exp(scores[h] + bias[rows, at] - lse_ref[0, 0, pl.ds(h, 1), at])
                lows.append(probs.astype(BF16))
                changes.append((probs * (slopes[h] - inner[pl.ds(h, 1), at])).astype(BF16))
            dk_acc[...] += sum(dot_nn(changes[h], masked_q[h, at, :]) for h in range(2))
            dv_acc[...] += sum(dot_nn(lows[h], masked_g[h, at, :]) for h in range(2))
            for h in range(2):
                part = pl.ds(h * HEAD, HEAD)
                dqt[part, at] += dot_nn(kt_ref[0, part, rows], changes[h])

        def one(j, carry):
            rows = pl.ds(pl.multiple_of(j * BLOCK, BLOCK), BLOCK)
            dk_acc[...] = jnp.zeros_like(dk_acc)
            dv_acc[...] = jnp.zeros_like(dv_acc)
            for i in range(blocks):
                inside = (j >= bounds_ref[2 * i]) & (j < bounds_ref[2 * i + 1])
                pl.when(inside)(functools.partial(unit, i, rows))
            dk_ref[0, rows, :] = dk_acc[...].astype(BF16)
            dv_ref[0, rows, :] = dv_acc[...].astype(BF16)
            return carry

        lax.fori_loop(bounds_ref[0], bounds_ref[2 * blocks - 1], one, 0)
        for i in range(blocks):
            at = pl.ds(i * BLOCK, BLOCK)
            dq_ref[0, at, :] = dqt[:, at].T.astype(BF16) * BF16(0.125)

    block_q = pl.BlockSpec((1, local, 128), lambda a, h, b: (a, 0, h))
    block_k = pl.BlockSpec((1, window, 128), lambda a, h, b: (a, 0, h))
    return pl.pallas_call(
        body,
        out_shape=[
            jax.ShapeDtypeStruct((nz, local, hw), BF16),
            jax.ShapeDtypeStruct((nz, window, hw), BF16),
            jax.ShapeDtypeStruct((nz, window, hw), BF16),
        ],
        grid_spec=pltpu.PrefetchScalarGridSpec(
            num_scalar_prefetch=1,
            grid=(nz, pairs),
            in_specs=[
                block_q,
                block_k,
                pl.BlockSpec((1, 128, window), lambda a, h, b: (a, h, 0)),
                block_k,
                block_q,
                block_q,
                pl.BlockSpec((1, 1, 2, local), lambda a, h, b: (a, h, 0, 0)),
                pl.BlockSpec((2, local), lambda a, h, b: (0, 0)),
                pl.BlockSpec((window, 2), lambda a, h, b: (0, 0)),
            ],
            out_specs=[block_q, block_k, block_k],
            scratch_shapes=[
                pltpu.VMEM((window, local), F32),
                pltpu.VMEM((2, local, 128), BF16),
                pltpu.VMEM((2, local, 128), BF16),
                pltpu.VMEM((128, local), F32),
                pltpu.VMEM((2, local), F32),
                pltpu.VMEM((BLOCK, 128), F32),
                pltpu.VMEM((BLOCK, 128), F32),
            ],
        ),
    )(bounds, queries, keys, keys_t, values, grads, mixed, lse, codes_q, codes_k)


def project_back(window_rows, weights, dq, dk, dv, attn_low, mixed, bounds):
    nz, depth, width = weights.shape
    window = window_rows.shape[0]
    local = dq.shape[1]
    own0 = 2 * local
    hw = width // 4

    def body(
        bounds_ref,
        x_ref,
        w_ref,
        dq_ref,
        dk_ref,
        dv_ref,
        g_ref,
        m_ref,
        dw_ref,
        dx_ref,
        bias_ref,
        acc,
        dkv,
    ):
        a = pl.program_id(0)

        @pl.when(a == 0)
        def _():
            acc[...] = jnp.zeros_like(acc)

        own = pl.ds(own0, local)
        grad_q = dq_ref[0]
        dw_ref[0, :, 0:hw] = dot_tn(x_ref[own, :], grad_q).astype(BF16)
        dw_ref[0, :, 3 * hw :] = dot_tn(g_ref[...], m_ref[0]).astype(BF16)
        acc[own, :] += dot_nt(grad_q, w_ref[0, :, 0:hw])
        bias_q = jnp.sum(grad_q.astype(F32), axis=0, keepdims=True)
        dkv[...] = jnp.zeros_like(dkv)

        def one(j, bias_v):
            start = pl.multiple_of(j * BLOCK, BLOCK)
            rows = pl.ds(start, BLOCK)
            both = jnp.concatenate([dk_ref[0, rows, :], dv_ref[0, rows, :]], axis=1)
            dkv[...] += dot_tn(x_ref[rows, :], both)
            acc[rows, :] += dot_nt(both, w_ref[0, :, hw : 3 * hw])
            return bias_v + jnp.sum(both[:, hw:].astype(F32), axis=0, keepdims=True)

        bias_v = lax.fori_loop(bounds_ref[0], bounds_ref[1], one, jnp.zeros((1, hw), F32))
        dw_ref[0, :, hw : 3 * hw] = dkv[...].astype(BF16)
        bias_ref[0] = jnp.concatenate([bias_q, bias_v], axis=1)

        @pl.when(a == nz - 1)
        def _():
            dx_ref[...] = acc[...].astype(BF16)

    def fixed(shape):
        return pl.BlockSpec(shape, lambda a, b: (0,) * len(shape))

    def by_slot(shape):
        return pl.BlockSpec((1,) + shape, lambda a, b: (a,) + (0,) * len(shape))

    return pl.pallas_call(
        body,
        out_shape=[
            jax.ShapeDtypeStruct((nz, depth, width), BF16),
            jax.ShapeDtypeStruct((window, depth), BF16),
            jax.ShapeDtypeStruct((nz, 1, 2 * hw), F32),
        ],
        grid_spec=pltpu.PrefetchScalarGridSpec(
            num_scalar_prefetch=1,
            grid=(nz,),
            in_specs=[
                fixed((window, depth)),
                by_slot((depth, width)),
                by_slot((local, hw)),
                by_slot((window, hw)),
                by_slot((window, hw)),
                fixed((local, depth)),
                by_slot((local, hw)),
            ],
            out_specs=[by_slot((depth, width)), fixed((window, depth)), by_slot((1, 2 * hw))],
            scratch_shapes=[
                pltpu.VMEM((window, depth), F32),
                pltpu.VMEM((depth, 2 * hw), F32),
            ],
        ),
    )(bounds, window_rows, weights, dq, dk, dv, attn_low, mixed)


def row_mean(values):
    return jnp.mean(values, axis=-1, keepdims=True)


def normalize(values):
    centred = values - row_mean(values)
    scaling = lax.rsqrt(row_mean(centred * centred) + 1e-05)
    return centred * scaling, scaling


def normalize_back(grad_values, unit_values, scaling, gain_vector):
    grad_unit = grad_values * gain_vector
    return scaling * (
        grad_unit - row_mean(grad_unit) - unit_values * row_mean(grad_unit * unit_values)
    )


def column_sum(values):
    return jnp.sum(values, axis=0, keepdims=True)


def gelu_both(values):
    bell = 0.5 * (1.0 + lax.erf(values * 0.7071067811865476))
    slope = bell + values * jnp.exp(-0.5 * values * values) * 0.3989422804014327
    return (values * bell).astype(BF16), slope.astype(BF16)


ROWS = 128


def row_parts(local):
    return [pl.ds(i * ROWS, ROWS) for i in range(local // ROWS)]


def whole_spec(shape):
    return pl.BlockSpec(shape, lambda a: (0,) * len(shape))


def slot_spec(shape):
    return pl.BlockSpec((1,) + shape, lambda a: (a,) + (0,) * len(shape))


def feed_forward(tokens, mixed, full_a, full_i, full_b, bias_h, vectors, cotangent, keep):
    local, depth = tokens.shape
    nz, _, hw = mixed.shape
    hidden = full_i.shape[2]

    def body(
        t_ref,
        m_ref,
        a_ref,
        i_ref,
        b_ref,
        bh_ref,
        v_ref,
        c_ref,
        keep_ref,
        act_ref,
        slope_ref,
        out_ref,
        low_ref,
        unit_ref,
        scale_ref,
        back_ref,
        second_ref,
        sums_ref,
        acc,
    ):
        step = pl.program_id(0)
        vec = [v_ref[pl.ds(k, 1), :] for k in range(6)]

        @pl.when(step == 0)
        def _():
            for at in row_parts(local):
                total = t_ref[at, :].astype(F32) + vec[0]
                for a in range(nz):
                    total = total + dot_nt(m_ref[a, at, :], a_ref[a])
                unit, scale = normalize(total)
                normed = unit * vec[2] + vec[3]
                unit_ref[at, :] = unit
                scale_ref[at, :] = scale
                low_ref[at, :] = normed.astype(BF16)
                acc[at, :] = normed + vec[1]

        w_in = i_ref[0]
        w_back = b_ref[0]
        for at in row_parts(local):
            act, slope = gelu_both(dot_nn(low_ref[at, :], w_in) + bh_ref[0])
            act_ref[0, at, :] = act
            slope_ref[0, at, :] = slope
            acc[at, :] += dot_nt(act, w_back)

        @pl.when(step == nz - 1)
        def _():
            d_gain = jnp.zeros((1, depth), F32)
            d_shift = jnp.zeros((1, depth), F32)
            d_bias = jnp.zeros((1, depth), F32)
            for at in row_parts(local):
                unit, scale = normalize(acc[at, :])
                kept = keep_ref[at, :]
                out_ref[at, :] = ((unit * vec[4] + vec[5]) * kept).astype(BF16)
                grad = c_ref[at, :].astype(F32) * kept
                d_gain = d_gain + column_sum(grad * unit)
                d_shift = d_shift + column_sum(grad)
                second = normalize_back(grad, unit, scale, vec[4])
                second_ref[at, :] = second
                low = second.astype(BF16)
                back_ref[at, :] = low
                d_bias = d_bias + column_sum(low.astype(F32))
            sums_ref[...] = jnp.concatenate([d_bias, d_gain, d_shift], axis=0)

    flat = (local, depth)
    return pl.pallas_call(
        body,
        out_shape=[
            jax.ShapeDtypeStruct((nz, local, hidden), BF16),
            jax.ShapeDtypeStruct((nz, local, hidden), BF16),
            jax.ShapeDtypeStruct(flat, BF16),
            jax.ShapeDtypeStruct(flat, BF16),
            jax.ShapeDtypeStruct(flat, F32),
            jax.ShapeDtypeStruct((local, 1), F32),
            jax.ShapeDtypeStruct(flat, BF16),
            jax.ShapeDtypeStruct(flat, F32),
            jax.ShapeDtypeStruct((3, depth), F32),
        ],
        grid=(nz,),
        in_specs=[
            whole_spec(flat),
            whole_spec((nz, local, hw)),
            pl.BlockSpec((nz, depth, hw), lambda a: (0, 0, 3)),
            slot_spec((depth, hidden)),
            slot_spec((depth, hidden)),
            slot_spec((1, hidden)),
            whole_spec((6, depth)),
            whole_spec(flat),
            whole_spec((local, 1)),
        ],
        out_specs=[
            slot_spec((local, hidden)),
            slot_spec((local, hidden)),
            whole_spec(flat),
            whole_spec(flat),
            whole_spec(flat),
            whole_spec((local, 1)),
            whole_spec(flat),
            whole_spec(flat),
            whole_spec((3, depth)),
        ],
        scratch_shapes=[pltpu.VMEM(flat, F32)],
    )(tokens, mixed, full_a, full_i, full_b, bias_h, vectors, cotangent, keep)


def grad_of_back(back_low, activated):
    nz, local, hidden = activated.shape
    depth = back_low.shape[1]

    def body(g_ref, act_ref, out_ref, turned):
        @pl.when(pl.program_id(0) == 0)
        def _():
            turned[...] = g_ref[...].T

        for p in range(depth // ROWS):
            at = pl.ds(p * ROWS, ROWS)
            out_ref[0, at, :] = dot_nn(turned[at, :], act_ref[0]).astype(BF16)

    return pl.pallas_call(
        body,
        out_shape=jax.ShapeDtypeStruct((nz, depth, hidden), BF16),
        grid=(nz,),
        in_specs=[whole_spec((local, depth)), slot_spec((local, hidden))],
        out_specs=slot_spec((depth, hidden)),
        scratch_shapes=[pltpu.VMEM((depth, local), BF16)],
    )(back_low, activated)


def feed_back(back_low, slopes, normed_low, full_i, full_b, second, unit, scale, vectors, full_a):
    local, depth = back_low.shape
    nz, _, hidden = slopes.shape
    hw = full_a.shape[2] // 4

    def body(
        g_ref,
        slope_ref,
        low_ref,
        i_ref,
        b_ref,
        second_ref,
        unit_ref,
        scale_ref,
        v_ref,
        a_ref,
        di_ref,
        bias_ref,
        res_ref,
        attn_ref,
        mixed_ref,
        sums_ref,
        acc,
        turned,
        pre_ref,
    ):
        step = pl.program_id(0)

        @pl.when(step == 0)
        def _():
            acc[...] = second_ref[...]
            turned[...] = low_ref[...].T

        w_in = i_ref[0]
        w_back = b_ref[0]
        d_bias = jnp.zeros((1, hidden), F32)
        for at in row_parts(local):
            pre = dot_nn(g_ref[at, :], w_back) * slope_ref[0, at, :].astype(F32)
            pre = pre.astype(BF16)
            pre_ref[at, :] = pre
            d_bias = d_bias + column_sum(pre.astype(F32))
            acc[at, :] += dot_nt(pre, w_in)
        bias_ref[0] = d_bias
        for p in range(depth // ROWS):
            at = pl.ds(p * ROWS, ROWS)
            di_ref[0, at, :] = dot_nn(turned[at, :], pre_ref[...]).astype(BF16)

        @pl.when(step == nz - 1)
        def _():
            d_gain = jnp.zeros((1, depth), F32)
            d_shift = jnp.zeros((1, depth), F32)
            d_out = jnp.zeros((1, depth), F32)
            for at in row_parts(local):
                grad = acc[at, :]
                unit_here = unit_ref[at, :]
                d_gain = d_gain + column_sum(grad * unit_here)
                d_shift = d_shift + column_sum(grad)
                res = normalize_back(grad, unit_here, scale_ref[at, :], v_ref[2:3, :])
                res_ref[at, :] = res
                low = res.astype(BF16)
                attn_ref[at, :] = low
                d_out = d_out + column_sum(low.astype(F32))
                for a in range(nz):
                    mixed_ref[a, at, :] = dot_nn(low, a_ref[a]).astype(BF16)
            sums_ref[...] = jnp.concatenate([d_out, d_gain, d_shift], axis=0)

    flat = (local, depth)
    return pl.pallas_call(
        body,
        out_shape=[
            jax.ShapeDtypeStruct((nz, depth, hidden), BF16),
            jax.ShapeDtypeStruct((nz, 1, hidden), F32),
            jax.ShapeDtypeStruct(flat, F32),
            jax.ShapeDtypeStruct(flat, BF16),
            jax.ShapeDtypeStruct((nz, local, hw), BF16),
            jax.ShapeDtypeStruct((3, depth), F32),
        ],
        grid=(nz,),
        in_specs=[
            whole_spec(flat),
            slot_spec((local, hidden)),
            whole_spec(flat),
            slot_spec((depth, hidden)),
            slot_spec((depth, hidden)),
            whole_spec(flat),
            whole_spec(flat),
            whole_spec((local, 1)),
            whole_spec((6, depth)),
            pl.BlockSpec((nz, depth, hw), lambda a: (0, 0, 3)),
        ],
        out_specs=[
            slot_spec((depth, hidden)),
            slot_spec((1, hidden)),
            whole_spec(flat),
            whole_spec(flat),
            whole_spec((nz, local, hw)),
            whole_spec((3, depth)),
        ],
        scratch_shapes=[
            pltpu.VMEM(flat, F32),
            pltpu.VMEM((depth, local), BF16),
            pltpu.VMEM((local, hidden), BF16),
        ],
    )(back_low, slopes, normed_low, full_i, full_b, second, unit, scale, vectors, full_a)


def on_device(ndp, nz, *arrays):
    (
        tokens,
        segment_ids,
        keep_mask,
        cotangent,
        w_query,
        w_key,
        w_value,
        w_out,
        w_in,
        w_back,
        bias_query,
        bias_value,
        bias_out,
        bias_in,
        bias_back,
        gain_first,
        shift_first,
        gain_second,
        shift_second,
    ) = arrays
    local, depth = tokens.shape
    hw = w_query.shape[1]
    heads_here = hw // HEAD
    hidden_here = w_in.shape[1]
    piece = depth // ndp
    inner = bias_query.shape[1]
    z = lax.axis_index("tensor")

    d = lax.axis_index("dp")

    def spread(part):
        rows, width = part.shape
        lane = lax.broadcasted_iota(jnp.int32, (rows, ndp * width), 1)
        return jnp.where(lane // width == d, jnp.tile(part, (1, ndp)), BF16(0)).reshape(-1)

    vectors = jnp.stack([bias_out, bias_back, gain_first, shift_first, gain_second, shift_second])
    small = jnp.concatenate([spread(vectors)] + [spread(p) for p in (bias_query, bias_value, bias_in)])
    small_rows = -(-small.shape[0] // 4096) * 32
    small = jnp.pad(small, (0, small_rows * 128 - small.shape[0])).reshape(small_rows, 128)
    message_a = jnp.concatenate([w_query, w_key, w_value, w_out.T], axis=1)
    (full_a, full_i, full_b, every), window_rows = gather_all(
        [message_a, w_in, w_back.T, small], tokens, ndp, nz
    )
    full_a = full_a.reshape(nz, depth, -1)
    full_i = full_i.reshape(nz, depth, -1)
    full_b = full_b.reshape(nz, depth, -1)
    every = jnp.sum(every.reshape(nz, ndp, small_rows, 128).astype(F32), axis=1)
    n_q = heads_here * inner
    n_v = 2 * n_q + bias_in.shape[0] * inner
    top = 6 * depth // 128
    vectors = every[0, :top].reshape(6, depth)
    bias_qv = every[:, top : top + 2 * hw // 128].reshape(nz, 1, 2 * hw)
    bias_h = every[:, top + 2 * hw // 128 : top + (2 * hw + hidden_here) // 128]
    bias_h = bias_h.reshape(nz, 1, hidden_here)

    length = segment_ids.shape[1]
    window = 5 * local
    own0 = 2 * local
    seg_pad = jnp.pad(segment_ids[0], (own0, own0), constant_values=-1)
    keep_pad = jnp.pad(keep_mask[0], (own0, own0), constant_values=1)
    seg_win = lax.dynamic_slice(seg_pad, (z * local,), (window,))
    keep_win = lax.dynamic_slice(keep_pad, (z * local,), (window,))
    place = jnp.arange(window, dtype=jnp.int32)
    seg_k = jnp.where(keep_win == 1, seg_win, -7)
    pad_k = jnp.where(keep_win == 1, -1, place)
    codes_k = jnp.stack([seg_k, pad_k], axis=1)
    seg_q = seg_win[own0 : own0 + local]
    keep_q = keep_win[own0 : own0 + local]
    pad_q = jnp.where(keep_q == 1, -2, place[own0 : own0 + local])
    codes_q = jnp.stack([seg_q, pad_q], axis=0)
    blocks = local // BLOCK
    first = seg_q.reshape(blocks, BLOCK)[:, 0]
    last = seg_q.reshape(blocks, BLOCK)[:, -1]
    inside = (seg_win >= 0)[None, :]
    before = jnp.sum((seg_win[None, :] < first[:, None]), axis=1, dtype=jnp.int32)
    outside_after = jnp.sum(
        (seg_win[None, :] <= last[:, None]) & inside, axis=1, dtype=jnp.int32
    )
    lead = jnp.maximum(own0 - z * local, 0)
    trail = jnp.maximum(z * local + window - own0 - length, 0)
    low = (before - trail) // BLOCK
    high = (outside_after + lead + BLOCK - 1) // BLOCK
    bounds = jnp.stack([low, high], axis=1).reshape(-1).astype(jnp.int32)
    whole = jnp.stack([bounds[0], bounds[2 * blocks - 1]])
    keep_local = keep_q.astype(F32)[:, None]

    queries, keys, values, keys_t, values_t = project(
        window_rows, full_a, bias_qv, whole, local
    )
    mixed, lse = attend(queries, keys, values_t, codes_q, codes_k, bounds)
    (activated, slopes, output, normed_low, unit, scale, back_low, second, sums_second) = (
        feed_forward(
            tokens,
            mixed,
            full_a,
            full_i,
            full_b,
            bias_h,
            vectors,
            cotangent,
            keep_local,
        )
    )
    d_back = grad_of_back(back_low, activated)
    d_in, d_bias_h, grad_residual, attn_low, grad_mixed, sums_first = feed_back(
        back_low, slopes, normed_low, full_i, full_b, second, unit, scale, vectors, full_a
    )
    dq, dk, dv = attend_back(
        queries,
        keys,
        keys_t,
        values,
        grad_mixed,
        mixed,
        lse.reshape(nz, hw // 128, 2, local),
        codes_q,
        codes_k,
        bounds,
    )
    d_a, dx, d_bias_qv = project_back(
        window_rows, full_a, dq, dk, dv, attn_low, mixed, whole
    )
    def by_device(part):
        part = part.reshape(nz, -1, ndp, inner).transpose(0, 2, 1, 3)
        return part.reshape(nz, ndp, -1)

    stacked = jnp.stack(
        [
            sums_first[0],
            sums_second[0],
            sums_first[1],
            sums_first[2],
            sums_second[1],
            sums_second[2],
        ]
    )
    stacked = stacked.reshape(6, ndp, piece).transpose(1, 0, 2).reshape(1, ndp, 6 * piece)
    d_small = jnp.concatenate(
        [
            by_device(d_bias_qv[:, 0, :hw]),
            by_device(d_bias_qv[:, 0, hw:]),
            by_device(d_bias_h[:, 0]),
            jnp.broadcast_to(stacked, (nz, ndp, 6 * piece)),
        ],
        axis=2,
    )
    d_small = jnp.pad(d_small, ((0, 0), (0, 0), (0, 2048 - d_small.shape[2])))

    def blocks_of(values):
        return values.reshape(nz, ndp, piece, values.shape[2])

    (shard_a, shard_i, shard_b, sums), grad_tokens = sum_all(
        [
            blocks_of(d_a),
            blocks_of(d_in),
            blocks_of(d_back),
            d_small.reshape(nz, ndp, 16, 128),
        ],
        dx,
        grad_residual,
        ndp,
        nz,
    )
    sums = sums.reshape(2048)
    d_bias_q = sums[:n_q].reshape(heads_here, inner)
    d_bias_v = sums[n_q : 2 * n_q].reshape(heads_here, inner)
    d_bias_in = sums[2 * n_q : n_v].reshape(-1, inner)
    vector_sums = sums[n_v : n_v + 6 * piece].reshape(6, piece)
    return (
        output,
        grad_tokens,
        shard_a[:, :hw],
        shard_a[:, hw : 2 * hw],
        shard_a[:, 2 * hw : 3 * hw],
        shard_a[:, 3 * hw :].T,
        shard_i,
        shard_b.T,
        d_bias_q,
        d_bias_v,
        vector_sums[0],
        d_bias_in,
        vector_sums[1],
        vector_sums[2],
        vector_sums[3],
        vector_sums[4],
        vector_sums[5],
    )


def solution(mesh):
    ndp, nz = mesh.shape["dp"], mesh.shape["tensor"]
    return jax.shard_map(
        functools.partial(on_device, ndp, nz),
        mesh=mesh,
        in_specs=(
            P(("dp", "tensor"), None),
            P("dp", None),
            P("dp", None),
            P(("dp", "tensor"), None),
            P("dp", "tensor"),
            P("dp", "tensor"),
            P("dp", "tensor"),
            P("tensor", "dp"),
            P("dp", "tensor"),
            P("tensor", "dp"),
            P("tensor", "dp"),
            P("tensor", "dp"),
            P("dp"),
            P("tensor", "dp"),
            P("dp"),
            P("dp"),
            P("dp"),
            P("dp"),
            P("dp"),
        ),
        out_specs=(
            P(("dp", "tensor"), None),
            P(("dp", "tensor"), None),
            P("dp", "tensor"),
            P("dp", "tensor"),
            P("dp", "tensor"),
            P("tensor", "dp"),
            P("dp", "tensor"),
            P("tensor", "dp"),
            P("tensor", "dp"),
            P("tensor", "dp"),
            P("dp"),
            P("tensor", "dp"),
            P("dp"),
            P("dp"),
            P("dp"),
            P("dp"),
            P("dp"),
        ),
        check_vma=False,
    )
```

```python
import functools

import jax
import jax.numpy as jnp
from jax import lax
from jax.experimental import pallas as pl
from jax.experimental.pallas import tpu as pltpu
from jax.sharding import PartitionSpec as P

HEAD = 64
DOC_MOST = 800
BLOCK = 256
GATHER_LAG = 3
SUM_LAG = 3
HALO_AT = 1.5
RELAY_AT = 3
MESH = pl.DeviceIdType.MESH
BF16 = jnp.bfloat16
F32 = jnp.float32
FAR_NEG = -1e30


def dot_nn(left, right):
    return lax.dot_general(left, right, (((1,), (0,)), ((), ())), preferred_element_type=F32)


def dot_nt(left, right):
    return lax.dot_general(left, right, (((1,), (1,)), ((), ())), preferred_element_type=F32)


def dot_tn(left, right):
    return lax.dot_general(left, right, (((0,), (0,)), ((), ())), preferred_element_type=F32)


def bits_of(count):
    found, bit = [], 1
    while bit < count:
        found.append(bit)
        bit *= 2
    return found


def far_rows(local):
    return -(-(DOC_MOST - 1 - local) // 16) * 16


def bit_at(value, bit):
    return lax.rem(value // bit, 2)


def gather_all(messages, tokens, ndp, nz):
    count = len(messages)
    local, depth = tokens.shape
    far = far_rows(local)
    window = 5 * local
    own0, l1, r1 = 2 * local, local, 3 * local
    l2, r2 = 2 * local - local - far, 4 * local
    zbits = bits_of(nz)[::-1]
    dbits = bits_of(ndp)[::-1]
    xy = dbits[:-1]
    pairs = []
    for c in range(2):
        for m in range(count):
            rows = messages[m].shape[0]
            chunks = 2 if rows % 32 == 0 else 1
            if c < chunks:
                pairs.append((m, c, rows // chunks))
    zorder, parent = [0], {}
    for bit in zbits:
        for q in list(zorder):
            parent[q ^ bit] = (q, bit)
            zorder.append(q ^ bit)
    stages = len(dbits)
    total = len(pairs) * (nz - 1) + len(pairs) * nz * stages
    lags = [GATHER_LAG * s for s in range(stages)]

    def kernel(*refs):
        ins, tok = refs[:count], refs[count]
        outs, win = refs[count + 1 : 2 * count + 1], refs[2 * count + 1]
        zeros, ssem, rsem, lsem, hs, hr = refs[2 * count + 2 :]
        d = lax.axis_index("dp")
        z = lax.axis_index("tensor")
        barrier = pltpu.get_barrier_semaphore()
        for step in range(1, nz):
            pl.semaphore_signal(
                barrier, inc=1, device_id=(d, lax.rem(z + step, nz)), device_id_type=MESH
            )
        for bit in dbits:
            pl.semaphore_signal(barrier, inc=1, device_id=(d ^ bit, z), device_id_type=MESH)

        own = tuple(bit_at(d, bit) for bit in dbits)
        locals_ = []

        def local_copy(src, dst):
            cp = pltpu.make_async_copy(src, dst, lsem.at[len(locals_)])
            locals_.append(cp)
            return cp

        for m in range(count):
            local_copy(ins[m], outs[m].at[(z,) + own]).start()
        local_copy(tok, win.at[pl.ds(own0, local)]).start()
        zeros[...] = jnp.zeros_like(zeros)
        edge = local - far
        if edge:
            local_copy(zeros.at[pl.ds(0, edge)], win.at[pl.ds(0, edge)]).start()
            local_copy(zeros.at[pl.ds(0, edge)], win.at[pl.ds(window - edge, edge)]).start()
        fills = [
            (z < 1, local_copy(zeros, win.at[pl.ds(l1, local)])),
            (z < 2, local_copy(zeros.at[pl.ds(0, far)], win.at[pl.ds(l2, far)])),
            (z > nz - 2, local_copy(zeros, win.at[pl.ds(r1, local)])),
            (z > nz - 3, local_copy(zeros.at[pl.ds(0, far)], win.at[pl.ds(r2, far)])),
        ]
        fixed = locals_[:-4]
        for when, cp in fills:
            pl.when(when)(cp.start)

        pl.semaphore_wait(barrier, nz - 1 + len(dbits))

        def halo_copy(src, dst, target, index):
            return pltpu.make_async_remote_copy(
                src_ref=src,
                dst_ref=dst,
                send_sem=hs.at[index],
                recv_sem=hr.at[index],
                device_id=(d, target),
                device_id_type=MESH,
            )

        up, down = lax.rem(z + 1, nz), lax.rem(z + nz - 1, nz)
        to_up = halo_copy(tok, win.at[pl.ds(l1, local)], up, 0)
        to_down = halo_copy(tok, win.at[pl.ds(r1, local)], down, 1)
        far_up = halo_copy(
            win.at[pl.ds(l1 + local - far, far)], win.at[pl.ds(l2, far)], up, 2
        )
        far_down = halo_copy(win.at[pl.ds(r1, far)], win.at[pl.ds(r2, far)], down, 3)

        counter, every = [0], []

        def remote(ref, index, device, src=None):
            number = counter[0]
            counter[0] += 1
            cp = pltpu.make_async_remote_copy(
                src_ref=ref.at[index] if src is None else src,
                dst_ref=ref.at[index],
                send_sem=ssem.at[number],
                recv_sem=rsem.at[number],
                device_id=device,
                device_id_type=MESH,
            )
            every.append(cp)
            return cp

        zcopies = {}
        for q, (par, bit) in parent.items():
            for m, c, piece in pairs:
                part = pl.ds(c * piece, piece)
                src = ins[m].at[part] if par == 0 else None
                zcopies[m, c, q] = remote(outs[m], (z ^ par,) + own + (part,), (d, z ^ bit), src)
        items = [(m, c, piece, a) for a in zorder for (m, c, piece) in pairs]
        plan = []
        for i, (m, c, piece, a) in enumerate(items):
            mine, held = [], list(own)
            part = pl.ds(c * piece, piece)
            for bit in (xy if i % 2 == 0 else xy[::-1]) + [1]:
                src = ins[m].at[part] if a == 0 and not mine else None
                index = (z ^ a,) + tuple(held) + (part,)
                mine.append(remote(outs[m], index, (d ^ bit, z), src))
                held[dbits.index(bit)] = slice(None)
            plan.append(mine)

        for m, c, _ in pairs:
            for q, (par, _) in parent.items():
                if par == 0:
                    zcopies[m, c, q].start()
        for cp in fixed:
            cp.wait()
        for when, cp in fills:
            pl.when(when)(cp.wait)
        for t in range(len(items) + lags[-1]):
            if t == int(HALO_AT * len(pairs)):
                pl.when(z < nz - 1)(to_up.start)
                pl.when(z > 0)(to_down.start)
            if t == int(RELAY_AT * len(pairs)):
                pl.when(z > 0)(to_up.wait_recv)
                pl.when((z > 0) & (z < nz - 1))(far_up.start)
                pl.when(z < nz - 1)(to_down.wait_recv)
                pl.when((z > 0) & (z < nz - 1))(far_down.start)
            for s in range(stages):
                i = t - lags[s]
                if not 0 <= i < len(items):
                    continue
                m, c, _, a = items[i]
                if s == 0:
                    if a:
                        zcopies[m, c, a].wait_recv()
                        for q, (par, _) in parent.items():
                            if par == a:
                                zcopies[m, c, q].start()
                else:
                    plan[i][s - 1].wait_recv()
                plan[i][s].start()
        for mine in plan:
            mine[-1].wait_recv()
        pl.when(z > 1)(far_up.wait_recv)
        pl.when(z < nz - 2)(far_down.wait_recv)
        for cp in every:
            cp.wait_send()
        pl.when(z < nz - 1)(to_up.wait_send)
        pl.when(z > 0)(to_down.wait_send)
        pl.when((z > 0) & (z < nz - 1))(far_up.wait_send)
        pl.when((z > 0) & (z < nz - 1))(far_down.wait_send)

    any_spec = pl.BlockSpec(memory_space=pl.ANY)
    split = (2,) * len(dbits)
    outs = pl.pallas_call(
        kernel,
        out_shape=[jax.ShapeDtypeStruct((nz,) + split + m.shape, BF16) for m in messages]
        + [jax.ShapeDtypeStruct((window, depth), BF16)],
        in_specs=[pl.BlockSpec(memory_space=pltpu.VMEM)] * (count + 1),
        out_specs=[any_spec] * (count + 1),
        scratch_shapes=[
            pltpu.VMEM((local, depth), BF16),
            pltpu.SemaphoreType.DMA((total,)),
            pltpu.SemaphoreType.DMA((total,)),
            pltpu.SemaphoreType.DMA((count + 7,)),
            pltpu.SemaphoreType.DMA((4,)),
            pltpu.SemaphoreType.DMA((4,)),
        ],
        compiler_params=pltpu.CompilerParams(collective_id=0, has_side_effects=True),
    )(*messages, tokens)
    return outs[:count], outs[count]


def sum_all(partials, dx, residual_grad, ndp, nz):
    count = len(partials)
    local, depth = residual_grad.shape
    far = far_rows(local)
    own0, l1, r1 = 2 * local, local, 3 * local
    l2, r2 = local - far, 4 * local
    zbits = bits_of(nz)
    dbits = bits_of(ndp)[::-1]
    xy = dbits[:-1]
    nxy = len(xy)
    stages = len(dbits)
    pairs = []
    for c in range(2):
        for m in range(count):
            rows = partials[m].shape[2]
            chunks = 2 if rows % 32 == 0 else 1
            if c < chunks:
                pairs.append((m, c, rows // chunks))
    zsteps = []
    live = list(range(nz))
    for bit in zbits:
        zsteps.append((bit, [q for q in live if q & bit]))
        live = [q for q in live if not q & bit]
    zorder = [q for _, sent in zsteps for q in sent] + [0]
    items = [(m, c, piece, a) for a in zorder for (m, c, piece) in pairs]
    total = len(items) * stages + len(pairs) * (nz - 1)
    lag = SUM_LAG
    shapes = [(p.shape[2], p.shape[3], p.dtype) for p in partials]

    def kernel(*refs):
        ins, dxr, res = refs[:count], refs[count], refs[count + 1]
        k = count + 2
        outs, tok = refs[k : k + count], refs[k + count]
        k += count + 1
        acc = refs[k : k + count]
        k += count
        got = [refs[k + s * count : k + (s + 1) * count] for s in range(stages)]
        k += stages * count
        zgot = refs[k : k + count]
        k += count
        hin, hbuf, hnear, ssem, rsem, lsem, hl, hs, hr = refs[k:]
        d = lax.axis_index("dp")
        z = lax.axis_index("tensor")
        barrier = pltpu.get_barrier_semaphore()
        for step in range(1, nz):
            pl.semaphore_signal(
                barrier, inc=1, device_id=(d, lax.rem(z + step, nz)), device_id_type=MESH
            )
        for bit in dbits:
            pl.semaphore_signal(barrier, inc=1, device_id=(d ^ bit, z), device_id_type=MESH)
        own = [bit_at(d, bit) for bit in dbits]
        core = own[-1]

        def remote(src, dst, number, device, send=ssem, recv=rsem):
            return pltpu.make_async_remote_copy(
                src_ref=src,
                dst_ref=dst,
                send_sem=send.at[number],
                recv_sem=recv.at[number],
                device_id=device,
                device_id_type=MESH,
            )

        everything = (slice(None),) * nxy
        plan, loads = [], []
        for i, (m, c, piece, a) in enumerate(items):
            part = pl.ds(c * piece, piece)
            za = z ^ a
            loads.append(
                pltpu.make_async_copy(
                    ins[m].at[(za,) + everything + (core, part)],
                    acc[m].at[(a,) + everything + (part,)],
                    lsem.at[i],
                )
            )
            steps = []
            order = xy if i % 2 == 0 else xy[::-1]
            first = remote(
                ins[m].at[(za,) + everything + (1 - core, part)],
                got[0][m].at[(a,) + everything + (part,)],
                i * stages,
                (d ^ 1, z),
            )
            steps.append((first, None, everything))
            where = list(everything)
            for s, bit in enumerate(order):
                at = xy.index(bit)
                send, keep = list(where), list(where)
                send[at] = 1 - own[at]
                keep[at] = own[at]
                live_count = nxy - 1 - s
                steps.append(
                    (
                        remote(
                            acc[m].at[(a,) + tuple(send) + (part,)],
                            got[s + 1][m].at[(a,) + (slice(None),) * live_count + (part,)],
                            i * stages + s + 1,
                            (d ^ bit, z),
                        ),
                        tuple(where),
                        tuple(keep),
                    )
                )
                where = keep
            plan.append(steps)

        base = len(items) * stages
        zplan = {}
        number = base
        mine = tuple(own[:-1])
        for pi, (m, c, piece) in enumerate(pairs):
            part = pl.ds(c * piece, piece)
            for bit, sent in zsteps:
                for q in sent:
                    zplan[m, c, q] = remote(
                        acc[m].at[(q,) + mine + (part,)],
                        zgot[m].at[q, part],
                        number,
                        (d, z ^ bit),
                    )
                    number += 1

        up, down = lax.rem(z + 1, nz), lax.rem(z + nz - 1, nz)
        own_load = pltpu.make_async_copy(dxr.at[pl.ds(own0, local)], hin.at[0], hl.at[0])
        left_load = pltpu.make_async_copy(dxr.at[pl.ds(l1, local)], hin.at[1], hl.at[1])
        right_load = pltpu.make_async_copy(dxr.at[pl.ds(r1, local)], hin.at[2], hl.at[2])
        far_down = remote(dxr.at[pl.ds(l2, far)], hbuf.at[0], 0, (d, down), hs, hr)
        far_up = remote(dxr.at[pl.ds(r2, far)], hbuf.at[1], 1, (d, up), hs, hr)
        near_down = remote(hin.at[1], hnear.at[0], 2, (d, down), hs, hr)
        near_up = remote(hin.at[2], hnear.at[1], 3, (d, up), hs, hr)
        for cp in (own_load, left_load, right_load):
            cp.start()
        pl.semaphore_wait(barrier, nz - 1 + len(dbits))
        pl.when(z > 1)(far_down.start)
        pl.when(z < nz - 2)(far_up.start)
        for i in range(len(items)):
            plan[i][0][0].start()
            loads[i].start()

        def halo_one():
            left_load.wait()
            right_load.wait()

            @pl.when((z > 0) & (z < nz - 1))
            def _():
                far_down.wait_recv()
                hin[1, pl.ds(local - far, far), :] += hbuf[0]
                far_up.wait_recv()
                hin[2, pl.ds(0, far), :] += hbuf[1]

            pl.when(z > 0)(near_down.start)
            pl.when(z < nz - 1)(near_up.start)

        def add(target, tindex, source, sindex, start, piece):
            step = min(piece, 32)

            def one(j, carry):
                rows = pl.ds(pl.multiple_of(start + j * step, step), step)
                at = tindex + (rows,)
                target[at] = target[at] + source[sindex + (rows,)]
                return carry

            lax.fori_loop(0, piece // step, one, 0)

        def combos(bits_count):
            result = [()]
            for _ in range(bits_count):
                result = [r + (v,) for r in result for v in (0, 1)]
            return result

        def absorb(i, s):
            m, c, piece, a = items[i]
            plan[i][s][0].wait_recv()
            if s == 0:
                loads[i].wait()
            keep = plan[i][s][2]
            free = [k for k in range(nxy) if isinstance(keep[k], slice)]
            for combo in combos(len(free)):
                index = list(keep)
                for k, v in zip(free, combo):
                    index[k] = v
                add(acc[m], (a,) + tuple(index), got[s][m], (a,) + combo, c * piece, piece)

        def zabsorb(m, c, piece, q):
            bit = next(b for b, sent in zsteps if q in sent)
            zplan[m, c, q].wait_recv()
            add(acc[m], (q ^ bit,) + mine, zgot[m], (q,), c * piece, piece)

        for t in range(len(items) + lag * stages):
            if t == 4:
                halo_one()
            for s in range(stages):
                i = t - lag * s
                if not 0 <= i < len(items):
                    continue
                absorb(i, s)
                if s + 1 < stages:
                    plan[i][s + 1][0].start()
                else:
                    m, c, piece, a = items[i]
                    for bit, sent in zsteps:
                        if (a ^ bit) in sent and not a & bit:
                            if bit < (a & -a if a else nz):
                                zabsorb(m, c, piece, a ^ bit)
                    if a:
                        zplan[m, c, a].start()
        for m, c, piece in pairs:
            part = pl.ds(c * piece, piece)
            outs[m][part, :] = acc[m][(0,) + mine + (part,)].astype(F32)
        own_load.wait()

        @pl.when(z < nz - 1)
        def _():
            near_down.wait_recv()

        @pl.when(z > 0)
        def _():
            near_up.wait_recv()

        step = 64

        def finish(j, carry):
            rows = pl.ds(pl.multiple_of(j * step, step), step)
            value = res[rows, :] + hin[0, rows, :].astype(F32)
            value = value + jnp.where(z < nz - 1, hnear[0, rows, :].astype(F32), 0.0)
            value = value + jnp.where(z > 0, hnear[1, rows, :].astype(F32), 0.0)
            tok[rows, :] = value.astype(BF16)
            return carry

        lax.fori_loop(0, local // step, finish, 0)
        for steps in plan:
            for cp, _, _ in steps:
                cp.wait_send()
        for cp in zplan.values():
            cp.wait_send()
        pl.when(z > 1)(far_down.wait_send)
        pl.when(z < nz - 2)(far_up.wait_send)
        pl.when(z > 0)(near_down.wait_send)
        pl.when(z < nz - 1)(near_up.wait_send)

    any_spec = pl.BlockSpec(memory_space=pl.ANY)
    vmem_spec = pl.BlockSpec(memory_space=pltpu.VMEM)
    split = (2,) * len(dbits)
    scratch = [pltpu.VMEM((nz,) + (2,) * nxy + s[:2], s[2]) for s in shapes]
    for stage in range(stages):
        left = nxy if stage == 0 else nxy - stage
        scratch += [pltpu.VMEM((nz,) + (2,) * left + s[:2], s[2]) for s in shapes]
    scratch += [pltpu.VMEM((nz,) + s[:2], s[2]) for s in shapes]
    scratch += [
        pltpu.VMEM((3, local, depth), BF16),
        pltpu.VMEM((2, far, depth), BF16),
        pltpu.VMEM((2, local, depth), BF16),
        pltpu.SemaphoreType.DMA((total,)),
        pltpu.SemaphoreType.DMA((total,)),
        pltpu.SemaphoreType.DMA((len(items),)),
        pltpu.SemaphoreType.DMA((3,)),
        pltpu.SemaphoreType.DMA((4,)),
        pltpu.SemaphoreType.DMA((4,)),
    ]
    result = pl.pallas_call(
        kernel,
        out_shape=[jax.ShapeDtypeStruct(s[:2], F32) for s in shapes]
        + [jax.ShapeDtypeStruct((local, depth), BF16)],
        in_specs=[any_spec] * (count + 1) + [vmem_spec],
        out_specs=[vmem_spec] * (count + 1),
        scratch_shapes=scratch,
        compiler_params=pltpu.CompilerParams(
            collective_id=1, has_side_effects=True, vmem_limit_bytes=63 * 1024 * 1024
        ),
    )(*[p.reshape((nz,) + split + p.shape[2:]) for p in partials], dx, residual_grad)
    return result[:count], result[count]


def in_pairs(low, high, visit):
    pairs = (high - low) // 2

    def two(p, carry):
        visit(low + 2 * p, 2 * BLOCK)
        return carry

    lax.fori_loop(0, pairs, two, 0)

    @pl.when(low + 2 * pairs < high)
    def _():
        visit(high - 1, BLOCK)


def project(window_rows, weights, biases, bounds, local):
    nz, depth, _ = weights.shape
    window = window_rows.shape[0]
    own0 = 2 * local
    heads_width = weights.shape[2] // 4

    def body(bounds_ref, x_ref, w_ref, b_ref, q_ref, k_ref, v_ref, kt_ref, vt_ref):
        hw = heads_width
        bias = b_ref[0]
        wq = w_ref[0, :, 0:hw]
        own = x_ref[pl.ds(own0, local), :]
        q_ref[0] = ((dot_nn(own, wq) + bias[:, 0:hw]) * 0.125).astype(BF16)

        def visit(j, size):
            at = pl.ds(pl.multiple_of(j * BLOCK, BLOCK), size)
            kv = dot_nn(x_ref[at, :], w_ref[0, :, hw : 3 * hw])
            key = kv[:, :hw].astype(BF16)
            value = (kv[:, hw:] + bias[:, hw:]).astype(BF16)
            k_ref[0, at, :] = key
            v_ref[0, at, :] = value
            kt_ref[0, :, at] = key.T
            vt_ref[0, :, at] = value.T

        in_pairs(bounds_ref[0], bounds_ref[1], visit)

    hw = heads_width
    return pl.pallas_call(
        body,
        out_shape=[
            jax.ShapeDtypeStruct((nz, local, hw), BF16),
            jax.ShapeDtypeStruct((nz, window, hw), BF16),
            jax.ShapeDtypeStruct((nz, window, hw), BF16),
            jax.ShapeDtypeStruct((nz, hw, window), BF16),
            jax.ShapeDtypeStruct((nz, hw, window), BF16),
        ],
        grid_spec=pltpu.PrefetchScalarGridSpec(
            num_scalar_prefetch=1,
            grid=(nz,),
            in_specs=[
                pl.BlockSpec((window, depth), lambda a, b: (0, 0)),
                pl.BlockSpec((1, depth, 4 * hw), lambda a, b: (a, 0, 0)),
                pl.BlockSpec((1, 1, 2 * hw), lambda a, b: (a, 0, 0)),
            ],
            out_specs=[
                pl.BlockSpec((1, local, hw), lambda a, b: (a, 0, 0)),
                pl.BlockSpec((1, window, hw), lambda a, b: (a, 0, 0)),
                pl.BlockSpec((1, window, hw), lambda a, b: (a, 0, 0)),
                pl.BlockSpec((1, hw, window), lambda a, b: (a, 0, 0)),
                pl.BlockSpec((1, hw, window), lambda a, b: (a, 0, 0)),
            ],
        ),
    )(bounds, window_rows, weights, biases)


def only_head(values, head):
    lane = lax.broadcasted_iota(jnp.int32, values.shape, 1)
    return jnp.where(lane // HEAD == head, values, jnp.zeros_like(values))


def pair_lanes(head):
    return slice(128 * (head // 2), 128 * (head // 2) + 128)


def fill_bias(bounds_ref, cq_ref, ck_ref, bias, blocks):
    for i in range(blocks):
        at = pl.ds(i * BLOCK, BLOCK)

        def fill(j, carry):
            rows = pl.ds(pl.multiple_of(j * BLOCK, BLOCK), BLOCK)
            allowed = (ck_ref[rows, 0:1] == cq_ref[0:1, at]) | (
                ck_ref[rows, 1:2] == cq_ref[1:2, at]
            )
            bias[rows, at] = jnp.where(allowed, 0.0, FAR_NEG)
            return carry

        lax.fori_loop(bounds_ref[2 * i], bounds_ref[2 * i + 1], fill, 0)


def attend(queries, keys, values_t, codes_q, codes_k, bounds):
    nz, local, hw = queries.shape
    window = keys.shape[1]
    heads = hw // HEAD
    blocks = local // BLOCK

    def body(
        bounds_ref, q_ref, k_ref, vt_ref, cq_ref, ck_ref, out_ref, lse_ref, bias, masked, held,
        top_acc, sum_acc, out_acc
    ):
        @pl.when(pl.program_id(0) == 0)
        def _():
            fill_bias(bounds_ref, cq_ref, ck_ref, bias, blocks)

        for i in range(blocks):
            at = pl.ds(i * BLOCK, BLOCK)
            for h in range(heads):
                masked[h] = only_head(q_ref[0, at, pair_lanes(h)], h % 2)

            top_acc[...] = jnp.full_like(top_acc, FAR_NEG)
            sum_acc[...] = jnp.zeros_like(sum_acc)
            out_acc[...] = jnp.zeros_like(out_acc)

            def first(j, size):
                rows = pl.ds(pl.multiple_of(j * BLOCK, BLOCK), size)
                for h in range(heads):
                    key = k_ref[0, rows, pair_lanes(h)]
                    scores = dot_nt(key, masked[h]) + bias[rows, at]
                    held[h, rows, :] = scores
                    part = jnp.max(scores.reshape(size // 8, 8, BLOCK), axis=0)
                    top_acc[h] = jnp.maximum(top_acc[h], part)

            low, high = bounds_ref[2 * i], bounds_ref[2 * i + 1]
            in_pairs(low, high, first)
            tops = [jnp.max(top_acc[h], axis=0, keepdims=True) for h in range(heads)]

            def second(j, size):
                rows = pl.ds(pl.multiple_of(j * BLOCK, BLOCK), size)
                for h in range(heads):
                    weights = jnp.exp(held[h, rows, :] - tops[h])
                    sum_acc[h] += jnp.sum(weights.reshape(size // 8, 8, BLOCK), axis=0)
                    part = pl.ds(h * HEAD, HEAD)
                    out_acc[part, :] += dot_nn(vt_ref[0, part, rows], weights.astype(BF16))

            in_pairs(low, high, second)
            done = [(sum_acc[h], out_acc[pl.ds(h * HEAD, HEAD), :]) for h in range(heads)]
            totals = [jnp.sum(total, axis=0, keepdims=True) for total, _ in done]
            mixed = jnp.concatenate([done[h][1] / totals[h] for h in range(heads)], axis=0)
            out_ref[0, at, :] = mixed.T.astype(BF16)
            for h in range(heads):
                lse_ref[0, pl.ds(h, 1), at] = tops[h] + jnp.log(totals[h])

    def by_slot(shape):
        return pl.BlockSpec((1,) + shape, lambda a, b: (a, 0, 0))

    return pl.pallas_call(
        body,
        out_shape=[
            jax.ShapeDtypeStruct((nz, local, hw), BF16),
            jax.ShapeDtypeStruct((nz, heads, local), F32),
        ],
        grid_spec=pltpu.PrefetchScalarGridSpec(
            num_scalar_prefetch=1,
            grid=(nz,),
            in_specs=[
                by_slot((local, hw)),
                by_slot((window, hw)),
                by_slot((hw, window)),
                pl.BlockSpec((2, local), lambda a, b: (0, 0)),
                pl.BlockSpec((window, 2), lambda a, b: (0, 0)),
            ],
            out_specs=[by_slot((local, hw)), by_slot((heads, local))],
            scratch_shapes=[
                pltpu.VMEM((window, local), F32),
                pltpu.VMEM((heads, BLOCK, 128), BF16),
                pltpu.VMEM((heads, window, BLOCK), F32),
                pltpu.VMEM((heads, 8, BLOCK), F32),
                pltpu.VMEM((heads, 8, BLOCK), F32),
                pltpu.VMEM((hw, BLOCK), F32),
            ],
        ),
    )(bounds, queries, keys, values_t, codes_q, codes_k)


def attend_back(queries, keys, keys_t, values, grads, mixed, lse, codes_q, codes_k, bounds):
    nz, local, hw = queries.shape
    window = keys.shape[1]
    pairs = hw // 128
    blocks = local // BLOCK

    def body(
        bounds_ref,
        q_ref,
        k_ref,
        kt_ref,
        v_ref,
        g_ref,
        m_ref,
        lse_ref,
        cq_ref,
        ck_ref,
        dq_ref,
        dk_ref,
        dv_ref,
        bias,
        masked_q,
        masked_g,
        dqt,
        inner,
        dk_acc,
        dv_acc,
    ):
        @pl.when((pl.program_id(0) == 0) & (pl.program_id(1) == 0))
        def _():
            fill_bias(bounds_ref, cq_ref, ck_ref, bias, blocks)

        dqt[...] = jnp.zeros_like(dqt)
        for i in range(blocks):
            at = pl.ds(i * BLOCK, BLOCK)
            query = q_ref[0, at, :]
            grad = g_ref[0, at, :]
            both = (grad.astype(F32) * m_ref[0, at, :].astype(F32)).T
            for h in range(2):
                masked_q[h, at, :] = only_head(query, h)
                masked_g[h, at, :] = only_head(grad, h)
                part = both[h * HEAD : (h + 1) * HEAD]
                inner[pl.ds(h, 1), at] = jnp.sum(part, axis=0, keepdims=True)

        def unit(i, j, size):
            at = pl.ds(i * BLOCK, BLOCK)
            rows = pl.ds(pl.multiple_of(j * BLOCK, BLOCK), size)
            key = k_ref[0, rows, :]
            value = v_ref[0, rows, :]
            scores = [dot_nt(key, masked_q[h, at, :]) for h in range(2)]
            slopes = [dot_nt(value, masked_g[h, at, :]) for h in range(2)]
            lows, changes = [], []
            for h in range(2):
                probs = jnp.exp(scores[h] + bias[rows, at] - lse_ref[0, 0, pl.ds(h, 1), at])
                lows.append(probs.astype(BF16))
                changes.append((probs * (slopes[h] - inner[pl.ds(h, 1), at])).astype(BF16))
            dk_acc[rows, :] += sum(dot_nn(changes[h], masked_q[h, at, :]) for h in range(2))
            dv_acc[rows, :] += sum(dot_nn(lows[h], masked_g[h, at, :]) for h in range(2))
            for h in range(2):
                part = pl.ds(h * HEAD, HEAD)
                dqt[part, at] += dot_nn(kt_ref[0, part, rows], changes[h])

        def clear(j, carry):
            rows = pl.ds(pl.multiple_of(j * BLOCK, BLOCK), BLOCK)
            dk_acc[rows, :] = jnp.zeros((BLOCK, 128), F32)
            dv_acc[rows, :] = jnp.zeros((BLOCK, 128), F32)
            return carry

        def store(j, carry):
            rows = pl.ds(pl.multiple_of(j * BLOCK, BLOCK), BLOCK)
            dk_ref[0, rows, :] = dk_acc[rows, :].astype(BF16)
            dv_ref[0, rows, :] = dv_acc[rows, :].astype(BF16)
            return carry

        low, high = bounds_ref[0], bounds_ref[2 * blocks - 1]
        lax.fori_loop(low, high, clear, 0)
        for i in range(blocks):
            in_pairs(bounds_ref[2 * i], bounds_ref[2 * i + 1], functools.partial(unit, i))
        lax.fori_loop(low, high, store, 0)
        for i in range(blocks):
            at = pl.ds(i * BLOCK, BLOCK)
            dq_ref[0, at, :] = dqt[:, at].T.astype(BF16) * BF16(0.125)

    block_q = pl.BlockSpec((1, local, 128), lambda a, h, b: (a, 0, h))
    block_k = pl.BlockSpec((1, window, 128), lambda a, h, b: (a, 0, h))
    return pl.pallas_call(
        body,
        out_shape=[
            jax.ShapeDtypeStruct((nz, local, hw), BF16),
            jax.ShapeDtypeStruct((nz, window, hw), BF16),
            jax.ShapeDtypeStruct((nz, window, hw), BF16),
        ],
        grid_spec=pltpu.PrefetchScalarGridSpec(
            num_scalar_prefetch=1,
            grid=(nz, pairs),
            in_specs=[
                block_q,
                block_k,
                pl.BlockSpec((1, 128, window), lambda a, h, b: (a, h, 0)),
                block_k,
                block_q,
                block_q,
                pl.BlockSpec((1, 1, 2, local), lambda a, h, b: (a, h, 0, 0)),
                pl.BlockSpec((2, local), lambda a, h, b: (0, 0)),
                pl.BlockSpec((window, 2), lambda a, h, b: (0, 0)),
            ],
            out_specs=[block_q, block_k, block_k],
            scratch_shapes=[
                pltpu.VMEM((window, local), F32),
                pltpu.VMEM((2, local, 128), BF16),
                pltpu.VMEM((2, local, 128), BF16),
                pltpu.VMEM((128, local), F32),
                pltpu.VMEM((2, local), F32),
                pltpu.VMEM((window, 128), F32),
                pltpu.VMEM((window, 128), F32),
            ],
        ),
    )(bounds, queries, keys, keys_t, values, grads, mixed, lse, codes_q, codes_k)


def project_back(window_rows, weights, dq, dk, dv, attn_low, mixed, bounds):
    nz, depth, width = weights.shape
    window = window_rows.shape[0]
    local = dq.shape[1]
    own0 = 2 * local
    hw = width // 4

    def body(
        bounds_ref,
        x_ref,
        w_ref,
        dq_ref,
        dk_ref,
        dv_ref,
        g_ref,
        m_ref,
        dw_ref,
        dx_ref,
        bias_ref,
        acc,
        dkv,
    ):
        a = pl.program_id(0)

        @pl.when(a == 0)
        def _():
            acc[...] = jnp.zeros_like(acc)

        own = pl.ds(own0, local)
        grad_q = dq_ref[0]
        dw_ref[0, :, 0:hw] = dot_tn(x_ref[own, :], grad_q).astype(BF16)
        dw_ref[0, :, 3 * hw :] = dot_tn(g_ref[...], m_ref[0]).astype(BF16)
        acc[own, :] += dot_nt(grad_q, w_ref[0, :, 0:hw])
        bias_q = jnp.sum(grad_q.astype(F32), axis=0, keepdims=True)
        dkv[...] = jnp.zeros_like(dkv)
        bias_ref[0] = jnp.concatenate([bias_q, jnp.zeros_like(bias_q)], axis=1)

        def visit(j, size):
            rows = pl.ds(pl.multiple_of(j * BLOCK, BLOCK), size)
            both = jnp.concatenate([dk_ref[0, rows, :], dv_ref[0, rows, :]], axis=1)
            dkv[...] += dot_tn(x_ref[rows, :], both)
            acc[rows, :] += dot_nt(both, w_ref[0, :, hw : 3 * hw])
            bias_ref[0, :, hw:] += jnp.sum(both[:, hw:].astype(F32), axis=0, keepdims=True)

        in_pairs(bounds_ref[0], bounds_ref[1], visit)
        dw_ref[0, :, hw : 3 * hw] = dkv[...].astype(BF16)

        @pl.when(a == nz - 1)
        def _():
            dx_ref[...] = acc[...].astype(BF16)

    def fixed(shape):
        return pl.BlockSpec(shape, lambda a, b: (0,) * len(shape))

    def by_slot(shape):
        return pl.BlockSpec((1,) + shape, lambda a, b: (a,) + (0,) * len(shape))

    return pl.pallas_call(
        body,
        out_shape=[
            jax.ShapeDtypeStruct((nz, depth, width), BF16),
            jax.ShapeDtypeStruct((window, depth), BF16),
            jax.ShapeDtypeStruct((nz, 1, 2 * hw), F32),
        ],
        grid_spec=pltpu.PrefetchScalarGridSpec(
            num_scalar_prefetch=1,
            grid=(nz,),
            in_specs=[
                fixed((window, depth)),
                by_slot((depth, width)),
                by_slot((local, hw)),
                by_slot((window, hw)),
                by_slot((window, hw)),
                fixed((local, depth)),
                by_slot((local, hw)),
            ],
            out_specs=[by_slot((depth, width)), fixed((window, depth)), by_slot((1, 2 * hw))],
            scratch_shapes=[
                pltpu.VMEM((window, depth), F32),
                pltpu.VMEM((depth, 2 * hw), F32),
            ],
        ),
    )(bounds, window_rows, weights, dq, dk, dv, attn_low, mixed)


def row_mean(values):
    return jnp.mean(values, axis=-1, keepdims=True)


def normalize(values):
    centred = values - row_mean(values)
    scaling = lax.rsqrt(row_mean(centred * centred) + 1e-05)
    return centred * scaling, scaling


def normalize_back(grad_values, unit_values, scaling, gain_vector):
    grad_unit = grad_values * gain_vector
    return scaling * (
        grad_unit - row_mean(grad_unit) - unit_values * row_mean(grad_unit * unit_values)
    )


def column_sum(values):
    return jnp.sum(values, axis=0, keepdims=True)


def gelu_both(values):
    bell = 0.5 * (1.0 + lax.erf(values * 0.7071067811865476))
    slope = bell + values * jnp.exp(-0.5 * values * values) * 0.3989422804014327
    return (values * bell).astype(BF16), slope.astype(BF16)


ROWS = 256


def row_parts(local):
    return [pl.ds(i * ROWS, ROWS) for i in range(local // ROWS)]


def whole_spec(shape):
    return pl.BlockSpec(shape, lambda a: (0,) * len(shape))


def slot_spec(shape):
    return pl.BlockSpec((1,) + shape, lambda a: (a,) + (0,) * len(shape))


def feed_forward(tokens, mixed, full_a, full_i, full_b, bias_h, vectors, cotangent, keep):
    local, depth = tokens.shape
    nz, _, hw = mixed.shape
    hidden = full_i.shape[2]

    def body(
        t_ref,
        m_ref,
        a_ref,
        i_ref,
        b_ref,
        bh_ref,
        v_ref,
        c_ref,
        keep_ref,
        act_ref,
        slope_ref,
        out_ref,
        low_ref,
        unit_ref,
        scale_ref,
        back_ref,
        second_ref,
        sums_ref,
        acc,
    ):
        step = pl.program_id(0)
        vec = [v_ref[pl.ds(k, 1), :] for k in range(6)]

        @pl.when(step == 0)
        def _():
            for at in row_parts(local):
                total = t_ref[at, :].astype(F32) + vec[0]
                for a in range(nz):
                    total = total + dot_nt(m_ref[a, at, :], a_ref[a])
                unit, scale = normalize(total)
                normed = unit * vec[2] + vec[3]
                unit_ref[at, :] = unit
                scale_ref[at, :] = scale
                low_ref[at, :] = normed.astype(BF16)
                acc[at, :] = normed + vec[1]

        w_in = i_ref[0]
        w_back = b_ref[0]
        for at in row_parts(local):
            act, slope = gelu_both(dot_nn(low_ref[at, :], w_in) + bh_ref[0])
            act_ref[0, at, :] = act
            slope_ref[0, at, :] = slope
            acc[at, :] += dot_nt(act, w_back)

        @pl.when(step == nz - 1)
        def _():
            d_gain = jnp.zeros((1, depth), F32)
            d_shift = jnp.zeros((1, depth), F32)
            d_bias = jnp.zeros((1, depth), F32)
            for at in row_parts(local):
                unit, scale = normalize(acc[at, :])
                kept = keep_ref[at, :]
                out_ref[at, :] = ((unit * vec[4] + vec[5]) * kept).astype(BF16)
                grad = c_ref[at, :].astype(F32) * kept
                d_gain = d_gain + column_sum(grad * unit)
                d_shift = d_shift + column_sum(grad)
                second = normalize_back(grad, unit, scale, vec[4])
                second_ref[at, :] = second
                low = second.astype(BF16)
                back_ref[at, :] = low
                d_bias = d_bias + column_sum(low.astype(F32))
            sums_ref[...] = jnp.concatenate([d_bias, d_gain, d_shift], axis=0)

    flat = (local, depth)
    return pl.pallas_call(
        body,
        out_shape=[
            jax.ShapeDtypeStruct((nz, local, hidden), BF16),
            jax.ShapeDtypeStruct((nz, local, hidden), BF16),
            jax.ShapeDtypeStruct(flat, BF16),
            jax.ShapeDtypeStruct(flat, BF16),
            jax.ShapeDtypeStruct(flat, F32),
            jax.ShapeDtypeStruct((local, 1), F32),
            jax.ShapeDtypeStruct(flat, BF16),
            jax.ShapeDtypeStruct(flat, F32),
            jax.ShapeDtypeStruct((3, depth), F32),
        ],
        grid=(nz,),
        in_specs=[
            whole_spec(flat),
            whole_spec((nz, local, hw)),
            pl.BlockSpec((nz, depth, hw), lambda a: (0, 0, 3)),
            slot_spec((depth, hidden)),
            slot_spec((depth, hidden)),
            slot_spec((1, hidden)),
            whole_spec((6, depth)),
            whole_spec(flat),
            whole_spec((local, 1)),
        ],
        out_specs=[
            slot_spec((local, hidden)),
            slot_spec((local, hidden)),
            whole_spec(flat),
            whole_spec(flat),
            whole_spec(flat),
            whole_spec((local, 1)),
            whole_spec(flat),
            whole_spec(flat),
            whole_spec((3, depth)),
        ],
        scratch_shapes=[pltpu.VMEM(flat, F32)],
    )(tokens, mixed, full_a, full_i, full_b, bias_h, vectors, cotangent, keep)


def grad_of_back(back_low, activated):
    nz, local, hidden = activated.shape
    depth = back_low.shape[1]

    def body(g_ref, act_ref, out_ref, turned):
        @pl.when(pl.program_id(0) == 0)
        def _():
            turned[...] = g_ref[...].T

        for p in range(depth // ROWS):
            at = pl.ds(p * ROWS, ROWS)
            out_ref[0, at, :] = dot_nn(turned[at, :], act_ref[0]).astype(BF16)

    return pl.pallas_call(
        body,
        out_shape=jax.ShapeDtypeStruct((nz, depth, hidden), BF16),
        grid=(nz,),
        in_specs=[whole_spec((local, depth)), slot_spec((local, hidden))],
        out_specs=slot_spec((depth, hidden)),
        scratch_shapes=[pltpu.VMEM((depth, local), BF16)],
    )(back_low, activated)


def feed_back(back_low, slopes, normed_low, full_i, full_b, second, unit, scale, vectors, full_a):
    local, depth = back_low.shape
    nz, _, hidden = slopes.shape
    hw = full_a.shape[2] // 4

    def body(
        g_ref,
        slope_ref,
        low_ref,
        i_ref,
        b_ref,
        second_ref,
        unit_ref,
        scale_ref,
        v_ref,
        a_ref,
        di_ref,
        bias_ref,
        res_ref,
        attn_ref,
        mixed_ref,
        sums_ref,
        acc,
        turned,
        pre_ref,
    ):
        step = pl.program_id(0)

        @pl.when(step == 0)
        def _():
            acc[...] = second_ref[...]
            turned[...] = low_ref[...].T

        w_in = i_ref[0]
        w_back = b_ref[0]
        d_bias = jnp.zeros((1, hidden), F32)
        for at in row_parts(local):
            pre = dot_nn(g_ref[at, :], w_back) * slope_ref[0, at, :].astype(F32)
            pre = pre.astype(BF16)
            pre_ref[at, :] = pre
            d_bias = d_bias + column_sum(pre.astype(F32))
            acc[at, :] += dot_nt(pre, w_in)
        bias_ref[0] = d_bias
        for p in range(depth // ROWS):
            at = pl.ds(p * ROWS, ROWS)
            di_ref[0, at, :] = dot_nn(turned[at, :], pre_ref[...]).astype(BF16)

        @pl.when(step == nz - 1)
        def _():
            d_gain = jnp.zeros((1, depth), F32)
            d_shift = jnp.zeros((1, depth), F32)
            d_out = jnp.zeros((1, depth), F32)
            for at in row_parts(local):
                grad = acc[at, :]
                unit_here = unit_ref[at, :]
                d_gain = d_gain + column_sum(grad * unit_here)
                d_shift = d_shift + column_sum(grad)
                res = normalize_back(grad, unit_here, scale_ref[at, :], v_ref[2:3, :])
                res_ref[at, :] = res
                low = res.astype(BF16)
                attn_ref[at, :] = low
                d_out = d_out + column_sum(low.astype(F32))
                for a in range(nz):
                    mixed_ref[a, at, :] = dot_nn(low, a_ref[a]).astype(BF16)
            sums_ref[...] = jnp.concatenate([d_out, d_gain, d_shift], axis=0)

    flat = (local, depth)
    return pl.pallas_call(
        body,
        out_shape=[
            jax.ShapeDtypeStruct((nz, depth, hidden), BF16),
            jax.ShapeDtypeStruct((nz, 1, hidden), F32),
            jax.ShapeDtypeStruct(flat, F32),
            jax.ShapeDtypeStruct(flat, BF16),
            jax.ShapeDtypeStruct((nz, local, hw), BF16),
            jax.ShapeDtypeStruct((3, depth), F32),
        ],
        grid=(nz,),
        in_specs=[
            whole_spec(flat),
            slot_spec((local, hidden)),
            whole_spec(flat),
            slot_spec((depth, hidden)),
            slot_spec((depth, hidden)),
            whole_spec(flat),
            whole_spec(flat),
            whole_spec((local, 1)),
            whole_spec((6, depth)),
            pl.BlockSpec((nz, depth, hw), lambda a: (0, 0, 3)),
        ],
        out_specs=[
            slot_spec((depth, hidden)),
            slot_spec((1, hidden)),
            whole_spec(flat),
            whole_spec(flat),
            whole_spec((nz, local, hw)),
            whole_spec((3, depth)),
        ],
        scratch_shapes=[
            pltpu.VMEM(flat, F32),
            pltpu.VMEM((depth, local), BF16),
            pltpu.VMEM((local, hidden), BF16),
        ],
    )(back_low, slopes, normed_low, full_i, full_b, second, unit, scale, vectors, full_a)


def on_device(ndp, nz, *arrays):
    (
        tokens,
        segment_ids,
        keep_mask,
        cotangent,
        w_query,
        w_key,
        w_value,
        w_out,
        w_in,
        w_back,
        bias_query,
        bias_value,
        bias_out,
        bias_in,
        bias_back,
        gain_first,
        shift_first,
        gain_second,
        shift_second,
    ) = arrays
    local, depth = tokens.shape
    hw = w_query.shape[1]
    heads_here = hw // HEAD
    hidden_here = w_in.shape[1]
    piece = depth // ndp
    inner = bias_query.shape[1]
    z = lax.axis_index("tensor")

    d = lax.axis_index("dp")

    def spread(part):
        rows, width = part.shape
        lane = lax.broadcasted_iota(jnp.int32, (rows, ndp * width), 1)
        return jnp.where(lane // width == d, jnp.tile(part, (1, ndp)), BF16(0)).reshape(-1)

    vectors = jnp.stack([bias_out, bias_back, gain_first, shift_first, gain_second, shift_second])
    small = jnp.concatenate([spread(vectors)] + [spread(p) for p in (bias_query, bias_value, bias_in)])
    small_rows = -(-small.shape[0] // 4096) * 32
    small = jnp.pad(small, (0, small_rows * 128 - small.shape[0])).reshape(small_rows, 128)
    message_a = jnp.concatenate([w_query, w_key, w_value, w_out.T], axis=1)
    (full_a, full_i, full_b, every), window_rows = gather_all(
        [message_a, w_in, w_back.T, small], tokens, ndp, nz
    )
    full_a = full_a.reshape(nz, depth, -1)
    full_i = full_i.reshape(nz, depth, -1)
    full_b = full_b.reshape(nz, depth, -1)
    every = jnp.sum(every.reshape(nz, ndp, small_rows, 128).astype(F32), axis=1)
    n_q = heads_here * inner
    n_v = 2 * n_q + bias_in.shape[0] * inner
    top = 6 * depth // 128
    vectors = every[0, :top].reshape(6, depth)
    bias_qv = every[:, top : top + 2 * hw // 128].reshape(nz, 1, 2 * hw)
    bias_h = every[:, top + 2 * hw // 128 : top + (2 * hw + hidden_here) // 128]
    bias_h = bias_h.reshape(nz, 1, hidden_here)

    length = segment_ids.shape[1]
    window = 5 * local
    own0 = 2 * local
    seg_pad = jnp.pad(segment_ids[0], (own0, own0), constant_values=-1)
    keep_pad = jnp.pad(keep_mask[0], (own0, own0), constant_values=1)
    seg_win = lax.dynamic_slice(seg_pad, (z * local,), (window,))
    keep_win = lax.dynamic_slice(keep_pad, (z * local,), (window,))
    place = jnp.arange(window, dtype=jnp.int32)
    seg_k = jnp.where(keep_win == 1, seg_win, -7)
    pad_k = jnp.where(keep_win == 1, -1, place)
    codes_k = jnp.stack([seg_k, pad_k], axis=1)
    seg_q = seg_win[own0 : own0 + local]
    keep_q = keep_win[own0 : own0 + local]
    pad_q = jnp.where(keep_q == 1, -2, place[own0 : own0 + local])
    codes_q = jnp.stack([seg_q, pad_q], axis=0)
    blocks = local // BLOCK
    first = seg_q.reshape(blocks, BLOCK)[:, 0]
    last = seg_q.reshape(blocks, BLOCK)[:, -1]
    inside = (seg_win >= 0)[None, :]
    before = jnp.sum((seg_win[None, :] < first[:, None]), axis=1, dtype=jnp.int32)
    outside_after = jnp.sum(
        (seg_win[None, :] <= last[:, None]) & inside, axis=1, dtype=jnp.int32
    )
    lead = jnp.maximum(own0 - z * local, 0)
    trail = jnp.maximum(z * local + window - own0 - length, 0)
    low = (before - trail) // BLOCK
    high = (outside_after + lead + BLOCK - 1) // BLOCK
    bounds = jnp.stack([low, high], axis=1).reshape(-1).astype(jnp.int32)
    whole = jnp.stack([bounds[0], bounds[2 * blocks - 1]])
    keep_local = keep_q.astype(F32)[:, None]

    queries, keys, values, keys_t, values_t = project(
        window_rows, full_a, bias_qv, whole, local
    )
    mixed, lse = attend(queries, keys, values_t, codes_q, codes_k, bounds)
    (activated, slopes, output, normed_low, unit, scale, back_low, second, sums_second) = (
        feed_forward(
            tokens,
            mixed,
            full_a,
            full_i,
            full_b,
            bias_h,
            vectors,
            cotangent,
            keep_local,
        )
    )
    d_back = grad_of_back(back_low, activated)
    d_in, d_bias_h, grad_residual, attn_low, grad_mixed, sums_first = feed_back(
        back_low, slopes, normed_low, full_i, full_b, second, unit, scale, vectors, full_a
    )
    dq, dk, dv = attend_back(
        queries,
        keys,
        keys_t,
        values,
        grad_mixed,
        mixed,
        lse.reshape(nz, hw // 128, 2, local),
        codes_q,
        codes_k,
        bounds,
    )
    d_a, dx, d_bias_qv = project_back(
        window_rows, full_a, dq, dk, dv, attn_low, mixed, whole
    )
    def by_device(part):
        part = part.reshape(nz, -1, ndp, inner).transpose(0, 2, 1, 3)
        return part.reshape(nz, ndp, -1)

    stacked = jnp.stack(
        [
            sums_first[0],
            sums_second[0],
            sums_first[1],
            sums_first[2],
            sums_second[1],
            sums_second[2],
        ]
    )
    stacked = stacked.reshape(6, ndp, piece).transpose(1, 0, 2).reshape(1, ndp, 6 * piece)
    d_small = jnp.concatenate(
        [
            by_device(d_bias_qv[:, 0, :hw]),
            by_device(d_bias_qv[:, 0, hw:]),
            by_device(d_bias_h[:, 0]),
            jnp.broadcast_to(stacked, (nz, ndp, 6 * piece)),
        ],
        axis=2,
    )
    d_small = jnp.pad(d_small, ((0, 0), (0, 0), (0, 2048 - d_small.shape[2])))

    def blocks_of(values):
        return values.reshape(nz, ndp, piece, values.shape[2])

    (shard_a, shard_i, shard_b, sums), grad_tokens = sum_all(
        [
            blocks_of(d_a),
            blocks_of(d_in),
            blocks_of(d_back),
            d_small.reshape(nz, ndp, 16, 128),
        ],
        dx,
        grad_residual,
        ndp,
        nz,
    )
    sums = sums.reshape(2048)
    d_bias_q = sums[:n_q].reshape(heads_here, inner)
    d_bias_v = sums[n_q : 2 * n_q].reshape(heads_here, inner)
    d_bias_in = sums[2 * n_q : n_v].reshape(-1, inner)
    vector_sums = sums[n_v : n_v + 6 * piece].reshape(6, piece)
    return (
        output,
        grad_tokens,
        shard_a[:, :hw],
        shard_a[:, hw : 2 * hw],
        shard_a[:, 2 * hw : 3 * hw],
        shard_a[:, 3 * hw :].T,
        shard_i,
        shard_b.T,
        d_bias_q,
        d_bias_v,
        vector_sums[0],
        d_bias_in,
        vector_sums[1],
        vector_sums[2],
        vector_sums[3],
        vector_sums[4],
        vector_sums[5],
    )


def solution(mesh):
    ndp, nz = mesh.shape["dp"], mesh.shape["tensor"]
    return jax.shard_map(
        functools.partial(on_device, ndp, nz),
        mesh=mesh,
        in_specs=(
            P(("dp", "tensor"), None),
            P("dp", None),
            P("dp", None),
            P(("dp", "tensor"), None),
            P("dp", "tensor"),
            P("dp", "tensor"),
            P("dp", "tensor"),
            P("tensor", "dp"),
            P("dp", "tensor"),
            P("tensor", "dp"),
            P("tensor", "dp"),
            P("tensor", "dp"),
            P("dp"),
            P("tensor", "dp"),
            P("dp"),
            P("dp"),
            P("dp"),
            P("dp"),
            P("dp"),
        ),
        out_specs=(
            P(("dp", "tensor"), None),
            P(("dp", "tensor"), None),
            P("dp", "tensor"),
            P("dp", "tensor"),
            P("dp", "tensor"),
            P("tensor", "dp"),
            P("dp", "tensor"),
            P("tensor", "dp"),
            P("tensor", "dp"),
            P("tensor", "dp"),
            P("dp"),
            P("tensor", "dp"),
            P("dp"),
            P("dp"),
            P("dp"),
            P("dp"),
            P("dp"),
        ),
        check_vma=False,
    )
```
